8 devices in a mesh: rep: 1 (over z), vocab: 8 (over y, x, core).
Axes of the slice: x: 2, y: 2, z: 1, core: 2. Of those that a mesh axis runs over, the one named last changes fastest.
Arguments:
- hidden: bfloat16 [4096, 1536], P(('rep', 'vocab'))
- w_head: bfloat16 [151936, 1536], P('vocab')
- allowed_ids: int32 [2048], P('rep')
- allowed_valid: int32 [2048], P('rep')
- target_pos: int32 [4096], P(('rep', 'vocab'))
Outputs:
- output 1: float32 [4096, 2048], P(('rep', 'vocab'))
- output 2: float32 [4096], P(('rep', 'vocab'))
All inputs are finite; a program needn't handle non-finite values.
Results may differ from the reference program's by a relative error of at most 0.001.
Values are sent between devices in bfloat16 or wider.
A program may use at most 1 GiB of HBM per device.

```python
import jax
import jax.numpy as jnp
from jax import lax

VOCAB_SIZE = 151936
MODEL_DIM = 1536
LIST_LEN = 2048
BATCH_ROWS = 4096
SHARDS = 8
HEAD_BLOCKS = 128
INV_TEMP = 1.25


def draw_head(key_head):
    block_keys = jax.random.split(key_head, HEAD_BLOCKS)
    row_scale = MODEL_DIM ** -0.5

    def one_block(block_key):
        block_vals = jax.random.normal(block_key, (VOCAB_SIZE // HEAD_BLOCKS, MODEL_DIM), jnp.float32)
        return (block_vals * row_scale).astype(jnp.bfloat16)

    return lax.map(one_block, block_keys).reshape(VOCAB_SIZE, MODEL_DIM)


def draw_list(key_list):
    key_pair, key_move, key_offset, key_order, key_count, key_valid, key_target = jax.random.split(key_list, 7)
    per_shard = LIST_LEN // SHARDS
    slot_cap = 2 * per_shard
    vocab_local = VOCAB_SIZE // SHARDS
    shard_order = jax.random.permutation(key_pair, SHARDS)
    move_sizes = jax.random.randint(key_move, (SHARDS // 2,), 0, per_shard + 1).at[0].set(per_shard)
    shard_gain = jnp.zeros((SHARDS,), jnp.int32).at[shard_order[0::2]].set(move_sizes).at[shard_order[1::2]].set(-move_sizes)
    counts = per_shard + shard_gain
    offset_keys = jax.random.split(key_offset, SHARDS)
    offsets = jax.vmap(lambda one_key: jax.random.permutation(one_key, vocab_local)[:slot_cap])(offset_keys)
    candidates = jnp.arange(SHARDS, dtype=jnp.int32)[:, None] * vocab_local + offsets
    keep_slot = jnp.arange(slot_cap)[None, :] < counts[:, None]
    sort_key = jnp.where(keep_slot, 0, 1) * (SHARDS * slot_cap) + jnp.arange(SHARDS * slot_cap).reshape(SHARDS, slot_cap)
    chosen = jnp.argsort(sort_key.reshape(-1))[:LIST_LEN]
    grouped = candidates.reshape(-1)[chosen]
    allowed_ids = grouped[jax.random.permutation(key_order, LIST_LEN)].astype(jnp.int32)
    valid_count = jax.random.randint(key_count, (), LIST_LEN // 2, LIST_LEN + 1)
    valid_perm = jax.random.permutation(key_valid, LIST_LEN)
    allowed_valid = (valid_perm < valid_count).astype(jnp.int32)
    inverse = jnp.argsort(valid_perm)
    pick_rank = jax.random.randint(key_target, (BATCH_ROWS,), 0, valid_count)
    target_pos = inverse[pick_rank].astype(jnp.int32)
    return allowed_ids, allowed_valid, target_pos


def setup_inputs(seed: int = 0, part: int = 0) -> dict:
    root_key = jax.random.key(seed)
    key_head, key_groups = jax.random.split(root_key)
    key_part = jax.random.fold_in(key_groups, part)
    key_hidden, key_list = jax.random.split(key_part)
    hidden = jax.random.normal(key_hidden, (BATCH_ROWS, MODEL_DIM), jnp.float32).astype(jnp.bfloat16)
    allowed_ids, allowed_valid, target_pos = draw_list(key_list)
    return dict(hidden=hidden, w_head=draw_head(key_head), allowed_ids=allowed_ids, allowed_valid=allowed_valid, target_pos=target_pos)


def reference(hidden, w_head, allowed_ids, allowed_valid, target_pos):
    head_rows = jnp.take(w_head, allowed_ids, axis=0)
    scores = jnp.dot(hidden, head_rows.T, preferred_element_type=jnp.float32) * INV_TEMP
    keep_mask = (allowed_valid > 0)[None, :]
    masked = jnp.where(keep_mask, scores, -jnp.inf)
    log_norm = jax.nn.logsumexp(masked, axis=1)
    token_probs = jnp.where(keep_mask, jnp.exp(masked - log_norm[:, None]), 0.0)
    picked = jnp.take_along_axis(scores, target_pos[:, None], axis=1)[:, 0]
    return token_probs, picked - log_norm
```

```python
import functools

import jax
import jax.numpy as jnp
from jax import lax
from jax.experimental import pallas as pl
from jax.experimental.pallas import tpu as pltpu
from jax.sharding import PartitionSpec as P

INV_TEMP = 1.25
BLOCK = 64
HALF = BLOCK // 2
WINDOW = 4
GROUP = 64
SELECT = 32
RING = 10
FINISH = 32
MIB = 2 ** 20
MESH = pl.DeviceIdType.MESH
BF16, F32, I32 = jnp.bfloat16, jnp.float32, jnp.int32


def iota(shape, dim):
    return lax.broadcasted_iota(I32, shape, dim)


def onehot(mask):
    return jnp.where(mask, 1.0, 0.0).astype(BF16)


def dot(a, b, dims=((1,), (0,))):
    return lax.dot_general(a, b, (dims, ((), ())), preferred_element_type=F32)


def loop(n, f, start=0):
    def body(i, carry):
        f(i)
        return carry
    lax.fori_loop(start, n, body, 0)


def gather_kernel(chips, vocab_local, caps, ids_ref, valid_ref, w_ref, part_ref, code_ref, cap_ref,
                  id_row, table, table_s, pick, stage, table_sem, in_sem):
    me = lax.axis_index("vocab")
    chip, devices = me // 2, 2 * chips
    rows, lanes = ids_ref.shape
    length = rows * lanes
    ids = ids_ref[...]
    valid = valid_ref[...] > 0
    owner = jnp.zeros_like(ids)
    for d in range(1, devices):
        owner += jnp.where(ids >= vocab_local * d, 1, 0)
    keep = [valid & (owner == d) for d in range(devices)]
    marks = jnp.concatenate([jnp.where(k, 1.0, 0.0) for k in keep], axis=0).astype(BF16)
    inside = dot(marks, onehot(iota((lanes, lanes), 0) <= iota((lanes, lanes), 1)))
    total = dot(marks, jnp.ones((lanes, lanes), BF16))
    n = devices * rows
    r, c_ = iota((n, n), 0), iota((n, n), 1)
    before = dot(onehot((r // (2 * rows) == c_ // (2 * rows)) & (c_ < r)), total.astype(BF16))
    rank = inside + before - 1.0
    code = jnp.full((rows, lanes), -1, I32)
    for d in range(devices):
        code = jnp.where(keep[d], d // 2 * length + rank[d * rows:(d + 1) * rows].astype(I32), code)
    own_id = jnp.where(valid, ids - me * vocab_local, -1)
    for k in range(rows):
        code_ref[:, k * lanes:(k + 1) * lanes] = code[k:k + 1]
        id_row[:, k * lanes:(k + 1) * lanes] = own_id[k:k + 1]
    after = before + total
    ours = iota((n, lanes), 0) // rows == me
    most = jnp.max(after).astype(I32)
    low = jnp.min(jnp.where(ours, before, 1e6)).astype(I32)
    high = jnp.max(jnp.where(ours, after, 0.0)).astype(I32)
    which = jnp.int32(0)
    cap = jnp.int32(caps[0])
    for small, large in zip(caps[:-1], caps[1:]):
        which += jnp.where(most > small, 1, 0)
        cap = jnp.where(most > small, large, cap)
    cap_ref[0] = which

    groups = cap // GROUP
    first, last = low // GROUP, (high + GROUP - 1) // GROUP
    last = jnp.where(high > low, last, first)
    local = id_row[...]
    owned = (local >= 0) & (local < vocab_local)
    tile = local >> 3
    sub = iota((8, length), 0)
    digits = jnp.where(sub == 0, tile >> 6, jnp.where(sub == 1, tile & 63, jnp.where(sub == 2, local & 7, 1)))
    digits = jnp.where(owned & (sub < 4), digits, 0).astype(F32).astype(BF16)

    def fill(kb):
        hot = onehot(code_ref[...] == chip * length + kb * lanes + iota((lanes, length), 0))
        found = dot(hot, digits, ((1,), (1,)))
        pick[pl.ds(pl.multiple_of(kb * lanes, lanes), lanes), :] = found
        across = found.T
        table[pl.ds(kb, 1), :] = (across[0:1] * 64.0 + across[1:2]).astype(I32)

    loop((high + lanes - 1) // lanes, fill, low // lanes)
    to_smem = pltpu.make_async_copy(table, table_s, table_sem)
    to_smem.start()
    to_smem.wait()

    def stage_at(g):
        return pl.ds(pl.multiple_of(lax.rem(g, RING) * (8 * GROUP), 8 * GROUP), 8 * GROUP)

    def issue(g):
        per = lanes // GROUP
        line, offset, slot = g // per, lax.rem(g, per) * GROUP, lax.rem(g, RING)
        for i in range(GROUP):
            t = table_s[line, offset + i]
            pltpu.make_async_copy(
                w_ref.at[pl.ds(pl.multiple_of(t * 8, 8), 8), :],
                stage.at[pl.ds(pl.multiple_of(slot * (8 * GROUP) + i * 8, 8), 8), :],
                in_sem.at[slot]).start()

    loop(jnp.minimum(last, first + RING), issue, first)

    def blank(g):
        part_ref[pl.ds(pl.multiple_of(g * GROUP, GROUP), GROUP), :] = jnp.zeros((GROUP, part_ref.shape[1]), BF16)

    loop(first, blank)
    loop(groups, blank, last)

    def step(g):
        slot = lax.rem(g, RING)
        pltpu.make_async_copy(w_ref.at[pl.ds(0, 8 * GROUP), :], stage.at[stage_at(g), :], in_sem.at[slot]).wait()
        for k in range(GROUP // SELECT):
            here = pl.ds(pl.multiple_of(g * GROUP + k * SELECT, SELECT), SELECT)
            found = pick[here, :]
            row = jnp.where(found[:, 3:4] > 0.5, found[:, 2:3], -4096.0).astype(I32)
            sel = onehot(iota((SELECT, 8 * SELECT), 1) - 8 * iota((SELECT, 8 * SELECT), 0) == row)
            tiles = pl.ds(pl.multiple_of(slot * (8 * GROUP) + k * 8 * SELECT, 8 * SELECT), 8 * SELECT)
            part_ref[here, :] = dot(sel, stage[tiles, :]).astype(BF16)

        @pl.when(g + RING < last)
        def _():
            issue(g + RING)

    loop(last, step, first)


def exchange_kernel(cap, length, hid, part, code_ref, acc, inc, rows, split, send, inc_recv, recv, p_recv):
    m = cap // BLOCK
    me = lax.axis_index("vocab")
    chip, core = me // 2, lax.rem(me, 2)
    x, y = lax.rem(chip, 2), chip // 2
    mate = {"vocab": me + 1 - 2 * core}
    x_dev = {"vocab": me + 2 - 4 * x}
    y_dev = {"vocab": me + 4 - 8 * y}
    x_chip, y_chip, d_chip = y * 2 + 1 - x, (1 - y) * 2 + x, (1 - y) * 2 + 1 - x
    mine, other = core * HALF, (1 - core) * HALF

    barrier = pltpu.get_barrier_semaphore()
    for dev in (mate, x_dev, y_dev):
        pl.semaphore_signal(barrier, inc=1, device_id=dev, device_id_type=MESH)
    acc[...] = jnp.broadcast_to(jnp.where(code_ref[...] >= 0, 0.0, -jnp.inf), acc.shape)
    pl.semaphore_wait(barrier, 3)

    def at(block, side):
        return rows.at[pl.ds(pl.multiple_of(block * BLOCK + side, HALF), HALF), :]

    def remote(src, dst, sent, received, dev):
        return pltpu.make_async_remote_copy(src_ref=src, dst_ref=dst, send_sem=sent, recv_sem=received,
                                            device_id=dev, device_id_type=MESH)

    def inc_copy(i):
        return remote(part.at[pl.ds(pl.multiple_of(i * BLOCK + other, HALF), HALF), :],
                      inc.at[pl.ds(pl.multiple_of(i * HALF, HALF), HALF), :],
                      send.at[0], inc_recv.at[i], mate)

    def own_x(i):
        return remote(at(i, mine), at(m + 2 * i, mine), send.at[1], recv.at[2 * i], x_dev)

    def own_y(i):
        j = 2 * (m - 1 - i) + 1
        return remote(at(i, mine), at(m + j, mine), send.at[2], recv.at[j], y_dev)

    def pair(b):
        return remote(at(b, mine), at(b, mine), send.at[3], p_recv.at[b], mate)

    def forward(j, dev):
        return remote(at(m + j, mine), at(3 * m + j, mine), send.at[4], recv.at[2 * m + j], dev)

    inc_copy(0).start()
    inc_copy(m - 1).start()
    loop(m - 1, lambda i: inc_copy(i).start(), 1)

    def merge(i):
        inc_copy(i).wait_recv()
        src = pl.ds(pl.multiple_of(i * BLOCK + mine, HALF), HALF)
        rows[src, :] = part[src, :] + inc[pl.ds(pl.multiple_of(i * HALF, HALF), HALF), :]

    merge(0)
    merge(m - 1)
    own_x(0).start()
    own_y(m - 1).start()
    loop(m - 1, merge, 1)

    def send_own(i):
        own_x(i).start()
        own_y(m - 1 - i).start()

    loop(m, send_own, 1)
    loop(m, lambda i: pair(i).start())

    def arrived(b):
        j = b - m

        @pl.when((b >= m) & (b < 4 * m))
        def _():
            remote(at(b, mine), at(b, mine), send.at[3], recv.at[j], mate).wait_recv()
            pair(b).start()

        @pl.when((b >= m) & (b < 2 * m) & (lax.rem(j + 2 * m, 2) == 0))
        def _():
            forward(j, y_dev).start()

        @pl.when((b >= m) & (b < 2 * m) & (lax.rem(j + 2 * m, 2) == 1))
        def _():
            forward(j, x_dev).start()

    def base(b):
        j = jnp.where(b < m, b, jnp.where(b < 3 * m, b - m, b - 3 * m))
        s, odd = j // 2, lax.rem(j, 2)
        of = jnp.where(b < m, chip, jnp.where(b >= 3 * m, d_chip, jnp.where(odd == 0, x_chip, y_chip)))
        i = jnp.where(b < m, b, jnp.where(odd == 0, s, m - 1 - s))
        return of * length + i * BLOCK

    width = WINDOW * BLOCK
    step_n = length // WINDOW

    def window(w):
        for k in range(WINDOW):
            pair(w * WINDOW + k).wait_recv()
        got = rows[pl.ds(pl.multiple_of(w * width, width), width), :]
        s = dot(hid[...], got, ((1,), (1,))) * INV_TEMP
        high = s.astype(BF16)
        rest = s - high.astype(F32)
        middle = rest.astype(BF16)
        split[:, :width] = high
        split[:, width:2 * width] = middle
        split[:, 2 * width:] = (rest - middle.astype(F32)).astype(BF16)
        slot = jnp.concatenate([base(w * WINDOW + k) + iota((BLOCK, step_n), 0) for k in range(WINDOW)], axis=0)

        def columns(c):
            cols = pl.ds(pl.multiple_of(c * step_n, step_n), step_n)
            hot = onehot(code_ref[:, cols] == slot)
            acc[:, cols] += dot(split[...], jnp.concatenate([hot, hot, hot], axis=0))
            arrived((w + 1) * WINDOW + c)

        loop(WINDOW, columns)

    for k in range(WINDOW):
        arrived(jnp.int32(k))
    loop(m, window)
    sent = lambda n, k: remote(rows.at[pl.ds(0, n), :], rows.at[pl.ds(0, n), :], send.at[k], recv.at[0], mate).wait_send()
    for k, blocks in enumerate((m, m, m, 4 * m, m)):
        sent(blocks * HALF, k)


def finish_kernel(s_ref, target_ref, prob_ref, logp_ref, prob, picked, sem):
    rows, lanes = prob.shape[0], target_ref.shape[1]
    lane = iota((FINISH, prob.shape[1]), 1)

    def block(i):
        target = jnp.broadcast_to(target_ref[pl.ds(i, 1), :].astype(F32), (lanes, lanes)).T[:, :1].astype(I32)
        for k in range(lanes // FINISH):
            here = pl.ds(pl.multiple_of(i * lanes + k * FINISH, FINISH), FINISH)
            s = s_ref[here, :]
            top = jnp.max(s, axis=1, keepdims=True)
            e = jnp.exp(s - top)
            total = jnp.sum(e, axis=1, keepdims=True)
            prob[here, :] = e * (1.0 / total)
            at_target = jnp.sum(jnp.where(lane == target[k * FINISH:(k + 1) * FINISH], s, 0.0), axis=1, keepdims=True)
            picked[k * FINISH:(k + 1) * FINISH, :] = at_target - (top + jnp.log(total))
            pltpu.make_async_copy(prob.at[here, :], prob_ref.at[here, :], sem).start()
        logp_ref[pl.ds(i, 1), :] = jnp.broadcast_to(picked[...], (lanes, lanes)).T[:1]

    loop(rows // lanes, block)
    pltpu.make_async_copy(prob, prob_ref, sem).wait()


def solution(mesh):
    shards = mesh.shape["vocab"]
    chips = shards // 2
    hbm = pl.BlockSpec(memory_space=pl.ANY)
    vmem = pl.BlockSpec(memory_space=pltpu.VMEM)

    def device_step(hidden, w_head, allowed_ids, allowed_valid, target_pos):
        rows_dev, depth = hidden.shape
        length = allowed_ids.shape[0]
        caps = [c for c in CAPS if c < length] + [length]
        lanes = 128
        part, code, which = pl.pallas_call(
            functools.partial(gather_kernel, chips, w_head.shape[0], caps),
            out_shape=(pltpu.VMEM((length, depth), BF16),
                       pltpu.VMEM((1, length), I32),
                       jax.ShapeDtypeStruct((1,), I32)),
            in_specs=[vmem, vmem, hbm],
            out_specs=(vmem, vmem, pl.BlockSpec(memory_space=pltpu.SMEM)),
            scratch_shapes=[
                pltpu.VMEM((1, length), I32),
                pltpu.VMEM((length // lanes, lanes), I32),
                pltpu.SMEM((length // lanes, lanes), I32),
                pltpu.VMEM((length, 8), F32),
                pltpu.VMEM((RING * 8 * GROUP, depth), BF16),
                pltpu.SemaphoreType.DMA,
                pltpu.SemaphoreType.DMA((RING,)),
            ],
            compiler_params=pltpu.CompilerParams(vmem_limit_bytes=28 * MIB),
            name="gather_rows",
        )(allowed_ids.reshape(-1, lanes), allowed_valid.reshape(-1, lanes), w_head)

        tile = 128
        finish = pl.pallas_call(
            finish_kernel,
            out_shape=(jax.ShapeDtypeStruct((rows_dev, length), F32),
                       jax.ShapeDtypeStruct((rows_dev // tile, tile), F32)),
            in_specs=[vmem, vmem],
            out_specs=(hbm, vmem),
            scratch_shapes=[pltpu.VMEM((rows_dev, length), F32), pltpu.VMEM((tile, 1), F32), pltpu.SemaphoreType.DMA],
            compiler_params=pltpu.CompilerParams(vmem_limit_bytes=16 * MIB),
            name="finish",
        )

        def serve(cap, cid):
            m = cap // BLOCK
            dma = lambda n: pltpu.SemaphoreType.DMA((n,))
            exchange = pl.pallas_call(
                functools.partial(exchange_kernel, cap, length),
                out_shape=pltpu.VMEM((rows_dev, length), F32),
                in_specs=[vmem, vmem, vmem],
                out_specs=vmem,
                scratch_shapes=[
                    pltpu.VMEM((cap // 2, depth), BF16),
                    pltpu.VMEM((4 * cap, depth), BF16),
                    pltpu.VMEM((rows_dev, 3 * WINDOW * BLOCK), BF16),
                    dma(5), dma(m), dma(3 * m), dma(4 * m),
                ],
                compiler_params=pltpu.CompilerParams(collective_id=cid, has_side_effects=True,
                                                     vmem_limit_bytes=(8 + 15 * cap // 1024) * MIB),
                name=f"exchange_{cap}",
            )
            return lambda hidden, part, code, target: finish(exchange(hidden, part, code), target)

        probs, logp = lax.switch(which[0], [serve(cap, k) for k, cap in enumerate(caps)],
                                 hidden, part, code, target_pos.reshape(-1, tile))
        return probs, logp.reshape(rows_dev)

    row_spec = P(("rep", "vocab"))
    mat_spec = P(("rep", "vocab"), None)
    return jax.shard_map(device_step, mesh=mesh, in_specs=(mat_spec, P("vocab", None), P("rep"), P("rep"), row_spec),
                         out_specs=(mat_spec, row_spec), check_vma=False)


CAPS = (320, 384, 448, 512, 576, 640, 704, 768, 832, 896, 1024)
```

```python
import functools

import jax
import jax.numpy as jnp
from jax import lax
from jax.experimental import pallas as pl
from jax.experimental.pallas import tpu as pltpu
from jax.sharding import PartitionSpec as P

INV_TEMP = 1.25
BLOCK = 64
HALF = BLOCK // 2
WINDOW = 4
GROUP = 64
SELECT = 32
RING = 10
FINISH = 32
MIB = 2 ** 20
MESH = pl.DeviceIdType.MESH
BF16, F32, I32 = jnp.bfloat16, jnp.float32, jnp.int32


def iota(shape, dim):
    return lax.broadcasted_iota(I32, shape, dim)


def onehot(mask):
    return jnp.where(mask, 1.0, 0.0).astype(BF16)


def dot(a, b, dims=((1,), (0,))):
    return lax.dot_general(a, b, (dims, ((), ())), preferred_element_type=F32)


def loop(n, f, start=0):
    def body(i, carry):
        f(i)
        return carry
    lax.fori_loop(start, n, body, 0)


def gather_kernel(chips, vocab_local, caps, ids_hbm, valid_hbm, w_ref, part_ref, code_ref, cap_ref,
                  ids_ref, valid_ref, id_row, table, table_s, pick, stage, load_sem, table_sem, in_sem):
    me = lax.axis_index("vocab")
    chip, devices = me // 2, 2 * chips
    loads = [pltpu.make_async_copy(ids_hbm, ids_ref, load_sem.at[0]),
             pltpu.make_async_copy(valid_hbm, valid_ref, load_sem.at[1])]
    for load in loads:
        load.start()
    for load in loads:
        load.wait()
    rows, lanes = ids_ref.shape
    length = rows * lanes
    ids = ids_ref[...]
    valid = valid_ref[...] > 0
    owner = jnp.zeros_like(ids)
    for d in range(1, devices):
        owner += jnp.where(ids >= vocab_local * d, 1, 0)
    keep = [valid & (owner == d) for d in range(devices)]
    marks = jnp.concatenate([jnp.where(k, 1.0, 0.0) for k in keep], axis=0).astype(BF16)
    inside = dot(marks, onehot(iota((lanes, lanes), 0) <= iota((lanes, lanes), 1)))
    total = dot(marks, jnp.ones((lanes, lanes), BF16))
    n = devices * rows
    r, c_ = iota((n, n), 0), iota((n, n), 1)
    before = dot(onehot((r // (2 * rows) == c_ // (2 * rows)) & (c_ < r)), total.astype(BF16))
    rank = inside + before - 1.0
    code = jnp.full((rows, lanes), -1, I32)
    for d in range(devices):
        code = jnp.where(keep[d], d // 2 * length + rank[d * rows:(d + 1) * rows].astype(I32), code)
    own_id = jnp.where(valid, ids - me * vocab_local, -1)
    for k in range(rows):
        code_ref[:, k * lanes:(k + 1) * lanes] = code[k:k + 1]
        id_row[:, k * lanes:(k + 1) * lanes] = own_id[k:k + 1]
    after = before + total
    ours = iota((n, lanes), 0) // rows == me
    most = jnp.max(after).astype(I32)
    low = jnp.min(jnp.where(ours, before, 1e6)).astype(I32)
    high = jnp.max(jnp.where(ours, after, 0.0)).astype(I32)
    which = jnp.int32(0)
    cap = jnp.int32(caps[0])
    for small, large in zip(caps[:-1], caps[1:]):
        which += jnp.where(most > small, 1, 0)
        cap = jnp.where(most > small, large, cap)
    cap_ref[0] = which

    groups = cap // GROUP
    first, last = low // GROUP, (high + GROUP - 1) // GROUP
    last = jnp.where(high > low, last, first)
    local = id_row[...]
    owned = (local >= 0) & (local < vocab_local)
    tile = local >> 3
    sub = iota((8, length), 0)
    digits = jnp.where(sub == 0, tile >> 6, jnp.where(sub == 1, tile & 63, jnp.where(sub == 2, local & 7, 1)))
    digits = jnp.where(owned & (sub < 4), digits, 0).astype(F32).astype(BF16)

    def fill(kb):
        hot = onehot(code_ref[...] == chip * length + kb * lanes + iota((lanes, length), 0))
        found = dot(hot, digits, ((1,), (1,)))
        pick[pl.ds(pl.multiple_of(kb * lanes, lanes), lanes), :] = found
        across = found.T
        table[pl.ds(kb, 1), :] = (across[0:1] * 64.0 + across[1:2]).astype(I32)
        to_smem(kb).start()

    def to_smem(kb):
        return pltpu.make_async_copy(table.at[pl.ds(kb, 1), :], table_s.at[pl.ds(kb, 1), :], table_sem.at[kb])

    loop(jnp.where(high > low, (high + lanes - 1) // lanes, 0), fill, low // lanes)

    def issue(g):
        per = lanes // GROUP
        line, offset, slot = g // per, lax.rem(g, per) * GROUP, lax.rem(g, RING)

        @pl.when((offset == 0) | (g == first))
        def _():
            to_smem(line).wait()
        for i in range(GROUP):
            pltpu.make_async_copy(w_ref.at[table_s[line, offset + i]], stage.at[slot, i], in_sem.at[slot]).start()

    loop(jnp.minimum(last, first + RING), issue, first)

    def blank(g):
        part_ref[pl.ds(pl.multiple_of(g * GROUP, GROUP), GROUP), :] = jnp.zeros((GROUP, part_ref.shape[1]), BF16)

    loop(first, blank)
    loop(groups, blank, last)

    def step(g):
        slot = lax.rem(g, RING)
        pltpu.make_async_copy(w_ref.at[pl.ds(0, GROUP)], stage.at[slot], in_sem.at[slot]).wait()
        for k in range(GROUP // SELECT):
            here = pl.ds(pl.multiple_of(g * GROUP + k * SELECT, SELECT), SELECT)
            found = pick[here, :]
            row = jnp.where(found[:, 3:4] > 0.5, found[:, 2:3], -4096.0).astype(I32)
            sel = onehot(iota((SELECT, 8 * SELECT), 1) - 8 * iota((SELECT, 8 * SELECT), 0) == row)
            tiles = stage[slot, k * SELECT:(k + 1) * SELECT].reshape(8 * SELECT, part_ref.shape[1])
            part_ref[here, :] = dot(sel, tiles).astype(BF16)

        @pl.when(g + RING < last)
        def _():
            issue(g + RING)

    loop(last, step, first)


def exchange_kernel(cap, length, hid, part, code_ref, acc, inc, rows, split, send, inc_recv, recv, p_recv):
    m = cap // BLOCK
    me = lax.axis_index("vocab")
    chip, core = me // 2, lax.rem(me, 2)
    x, y = lax.rem(chip, 2), chip // 2
    mate = {"vocab": me + 1 - 2 * core}
    x_dev = {"vocab": me + 2 - 4 * x}
    y_dev = {"vocab": me + 4 - 8 * y}
    x_chip, y_chip, d_chip = y * 2 + 1 - x, (1 - y) * 2 + x, (1 - y) * 2 + 1 - x
    mine, other = core * HALF, (1 - core) * HALF

    barrier = pltpu.get_barrier_semaphore()
    for dev in (mate, x_dev, y_dev):
        pl.semaphore_signal(barrier, inc=1, device_id=dev, device_id_type=MESH)
    acc[...] = jnp.broadcast_to(jnp.where(code_ref[...] >= 0, 0.0, -jnp.inf), acc.shape)
    pl.semaphore_wait(barrier, 3)

    def at(block, side):
        return rows.at[pl.ds(pl.multiple_of(block * BLOCK + side, HALF), HALF), :]

    def remote(src, dst, sent, received, dev):
        return pltpu.make_async_remote_copy(src_ref=src, dst_ref=dst, send_sem=sent, recv_sem=received,
                                            device_id=dev, device_id_type=MESH)

    def inc_copy(i):
        return remote(part.at[pl.ds(pl.multiple_of(i * BLOCK + other, HALF), HALF), :],
                      inc.at[pl.ds(pl.multiple_of(i * HALF, HALF), HALF), :],
                      send.at[0], inc_recv.at[jnp.where(i == 0, 0, jnp.where(i == m - 1, 1, 2))], mate)

    def own_x(i):
        return remote(at(i, mine), at(m + 2 * i, mine), send.at[1], recv.at[i], x_dev)

    def own_y(i):
        return remote(at(i, mine), at(m + 2 * (m - 1 - i) + 1, mine), send.at[2], recv.at[m - 1 - i], y_dev)

    def pair(b):
        return remote(at(b, mine), at(b, mine), send.at[3], p_recv.at[b // WINDOW], mate)

    def forward(j, dev):
        return remote(at(m + j, mine), at(3 * m + j, mine), send.at[4], recv.at[m + j // 2], dev)

    def wait_for(n, sem):
        chunk = rows.at[pl.ds(0, n * HALF), :]
        remote(chunk, chunk, send.at[0], sem, mate).wait_recv()

    loop(m, lambda i: inc_copy(jnp.where(i == 0, 0, jnp.where(i == 1, m - 1, i - 1))).start())

    def merge(i):
        src = pl.ds(pl.multiple_of(i * BLOCK + mine, HALF), HALF)
        rows[src, :] = part[src, :] + inc[pl.ds(pl.multiple_of(i * HALF, HALF), HALF), :]

    wait_for(1, inc_recv.at[0])
    merge(0)
    wait_for(1, inc_recv.at[1])
    merge(m - 1)
    own_x(0).start()
    own_y(m - 1).start()
    wait_for(m - 2, inc_recv.at[2])
    loop(m - 1, merge, 1)

    def send_own(i):
        own_x(i).start()
        own_y(m - 1 - i).start()

    loop(m, send_own, 1)
    loop(m, lambda i: pair(i).start())

    pairs = m + (m + 1) // 2

    def arrived(t):
        j = 2 * t

        @pl.when((t >= 0) & (t < pairs))
        def _():
            alone = (m % 2 == 1) & (t == pairs - 1)

            @pl.when(jnp.logical_not(alone))
            def _():
                wait_for(2, recv.at[t])
                pair(m + j).start()
                pair(m + j + 1).start()

            @pl.when(alone)
            def _():
                wait_for(1, recv.at[t])
                pair(m + j).start()

            @pl.when(j < m)
            def _():
                forward(j, y_dev).start()

            @pl.when(j + 1 < m)
            def _():
                forward(j + 1, x_dev).start()

    def base(b):
        j = jnp.where(b < m, b, jnp.where(b < 3 * m, b - m, b - 3 * m))
        s, odd = j // 2, lax.rem(j, 2)
        of = jnp.where(b < m, chip, jnp.where(b >= 3 * m, d_chip, jnp.where(odd == 0, x_chip, y_chip)))
        i = jnp.where(b < m, b, jnp.where(odd == 0, s, m - 1 - s))
        return of * length + i * BLOCK

    width = WINDOW * BLOCK
    step_n = length // WINDOW

    def window(w):
        wait_for(WINDOW, p_recv.at[w])
        got = rows[pl.ds(pl.multiple_of(w * width, width), width), :]
        s = dot(hid[...], got, ((1,), (1,))) * INV_TEMP
        high = s.astype(BF16)
        rest = s - high.astype(F32)
        middle = rest.astype(BF16)
        split[:, :width] = high
        split[:, width:2 * width] = middle
        split[:, 2 * width:] = (rest - middle.astype(F32)).astype(BF16)
        slot = jnp.concatenate([base(w * WINDOW + k) + iota((BLOCK, step_n), 0) for k in range(WINDOW)], axis=0)

        def columns(c):
            cols = pl.ds(pl.multiple_of(c * step_n, step_n), step_n)
            hot = onehot(code_ref[:, cols] == slot)
            acc[:, cols] += dot(split[...], jnp.concatenate([hot, hot, hot], axis=0))
            need = (w + 2) * WINDOW - m

            @pl.when(c < 2)
            def _():
                lo = jnp.maximum((need - WINDOW + 1) // 2, 0)
                hi = jnp.minimum(jnp.maximum((need + 1) // 2, 0), pairs)

                @pl.when(lo + c < hi)
                def _():
                    arrived(lo + c)

        loop(WINDOW, columns)

    loop(m, window)
    sent = lambda n, k: remote(rows.at[pl.ds(0, n), :], rows.at[pl.ds(0, n), :], send.at[k], recv.at[0], mate).wait_send()
    for k, blocks in enumerate((m, m, m, 4 * m, m)):
        sent(blocks * HALF, k)


def finish_kernel(s_ref, target_ref, prob_ref, logp_ref, prob, picked, sem):
    rows, lanes = prob.shape[0], target_ref.shape[1]
    lane = iota((FINISH, prob.shape[1]), 1)

    def block(i):
        target = jnp.broadcast_to(target_ref[pl.ds(i, 1), :].astype(F32), (lanes, lanes)).T[:, :1].astype(I32)
        for k in range(lanes // FINISH):
            here = pl.ds(pl.multiple_of(i * lanes + k * FINISH, FINISH), FINISH)
            s = s_ref[here, :]
            top = jnp.max(s, axis=1, keepdims=True)
            e = jnp.exp(s - top)
            total = jnp.sum(e, axis=1, keepdims=True)
            prob[here, :] = e * (1.0 / total)
            at_target = jnp.sum(jnp.where(lane == target[k * FINISH:(k + 1) * FINISH], s, 0.0), axis=1, keepdims=True)
            picked[k * FINISH:(k + 1) * FINISH, :] = at_target - (top + jnp.log(total))
            pltpu.make_async_copy(prob.at[here, :], prob_ref.at[here, :], sem).start()
        logp_ref[pl.ds(i, 1), :] = jnp.broadcast_to(picked[...], (lanes, lanes)).T[:1]

    loop(rows // lanes, block)
    pltpu.make_async_copy(prob, prob_ref, sem).wait()


def solution(mesh):
    shards = mesh.shape["vocab"]
    chips = shards // 2
    hbm = pl.BlockSpec(memory_space=pl.ANY)
    vmem = pl.BlockSpec(memory_space=pltpu.VMEM)

    def device_step(hidden, w_head, allowed_ids, allowed_valid, target_pos):
        rows_dev, depth = hidden.shape
        length = allowed_ids.shape[0]
        caps = [c for c in CAPS if c < length] + [length]
        lanes = 128
        part, code, which = pl.pallas_call(
            functools.partial(gather_kernel, chips, w_head.shape[0], caps),
            out_shape=(pltpu.VMEM((length, depth), BF16),
                       pltpu.VMEM((1, length), I32),
                       jax.ShapeDtypeStruct((1,), I32)),
            in_specs=[pl.BlockSpec(memory_space=pltpu.HBM)] * 3,
            out_specs=(vmem, vmem, pl.BlockSpec(memory_space=pltpu.SMEM)),
            scratch_shapes=[
                pltpu.VMEM((length // lanes, lanes), I32),
                pltpu.VMEM((length // lanes, lanes), I32),
                pltpu.VMEM((1, length), I32),
                pltpu.VMEM((length // lanes, lanes), I32),
                pltpu.SMEM((length // lanes, lanes), I32),
                pltpu.VMEM((length, 8), F32),
                pltpu.VMEM((RING, GROUP, 8, depth), BF16),
                pltpu.SemaphoreType.DMA((2,)),
                pltpu.SemaphoreType.DMA((length // lanes,)),
                pltpu.SemaphoreType.DMA((RING,)),
            ],
            compiler_params=pltpu.CompilerParams(vmem_limit_bytes=28 * MIB),
            name="gather_rows",
        )(*(pltpu.with_memory_space_constraint(v, pltpu.HBM) for v in (allowed_ids.reshape(-1, lanes), allowed_valid.reshape(-1, lanes))), w_head.reshape(-1, 8, depth))

        tile = 128
        finish = pl.pallas_call(
            finish_kernel,
            out_shape=(jax.ShapeDtypeStruct((rows_dev, length), F32),
                       jax.ShapeDtypeStruct((rows_dev // tile, tile), F32)),
            in_specs=[vmem, vmem],
            out_specs=(hbm, vmem),
            scratch_shapes=[pltpu.VMEM((rows_dev, length), F32), pltpu.VMEM((tile, 1), F32), pltpu.SemaphoreType.DMA],
            compiler_params=pltpu.CompilerParams(vmem_limit_bytes=16 * MIB),
            name="finish",
        )

        def serve(cap, cid):
            m = cap // BLOCK
            dma = lambda n: pltpu.SemaphoreType.DMA((n,))
            exchange = pl.pallas_call(
                functools.partial(exchange_kernel, cap, length),
                out_shape=pltpu.VMEM((rows_dev, length), F32),
                in_specs=[vmem, vmem, vmem],
                out_specs=vmem,
                scratch_shapes=[
                    pltpu.VMEM((cap // 2, depth), BF16),
                    pltpu.VMEM((4 * cap, depth), BF16),
                    pltpu.VMEM((rows_dev, 3 * WINDOW * BLOCK), BF16),
                    dma(5), dma(3), dma(m + (m + 1) // 2), dma(m),
                ],
                compiler_params=pltpu.CompilerParams(collective_id=cid, has_side_effects=True,
                                                     vmem_limit_bytes=(8 + 15 * cap // 1024) * MIB),
                name=f"exchange_{cap}",
            )
            return lambda hidden, part, code, target: finish(exchange(hidden, part, code), target)

        probs, logp = lax.switch(which[0], [serve(cap, k) for k, cap in enumerate(caps)],
                                 hidden, part, code, target_pos.reshape(-1, tile))
        return probs, logp.reshape(rows_dev)

    row_spec = P(("rep", "vocab"))
    mat_spec = P(("rep", "vocab"), None)
    return jax.shard_map(device_step, mesh=mesh, in_specs=(mat_spec, P("vocab", None), P("rep"), P("rep"), row_spec),
                         out_specs=(mat_spec, row_spec), check_vma=False)


CAPS = (320, 384, 448, 512, 576, 640, 704, 768, 832, 896, 1024)
```

```python
import functools

import jax
import jax.numpy as jnp
from jax import lax
from jax.experimental import pallas as pl
from jax.experimental.pallas import tpu as pltpu
from jax.sharding import PartitionSpec as P

INV_TEMP = 1.25
BLOCK = 64
HALF = BLOCK // 2
WINDOW = 4
GROUP = 64
SELECT = 32
RING = 10
FINISH = 32
MIB = 2 ** 20
MESH = pl.DeviceIdType.MESH
BF16, F32, I32 = jnp.bfloat16, jnp.float32, jnp.int32


def iota(shape, dim):
    return lax.broadcasted_iota(I32, shape, dim)


def onehot(mask):
    return jnp.where(mask, 1.0, 0.0).astype(BF16)


def dot(a, b, dims=((1,), (0,))):
    return lax.dot_general(a, b, (dims, ((), ())), preferred_element_type=F32)


def loop(n, f, start=0):
    def body(i, carry):
        f(i)
        return carry
    lax.fori_loop(start, n, body, 0)


def pick_of(table, index):
    value = jnp.int32(table[0])
    for k in range(1, len(table)):
        if table[k] != table[0]:
            value = jnp.where(index == k, table[k], value)
    return value


def gather_kernel(chips, vocab_local, plans, ids_hbm, valid_hbm, w_ref, part_ref, code_ref, cap_ref,
                  ids_ref, valid_ref, id_row, table, table_s, pick, stage, load_sem, table_sem, in_sem):
    me = lax.axis_index("vocab")
    chip, devices = me // 2, 2 * chips
    loads = [pltpu.make_async_copy(ids_hbm, ids_ref, load_sem.at[0]),
             pltpu.make_async_copy(valid_hbm, valid_ref, load_sem.at[1])]
    for load in loads:
        load.start()
    for load in loads:
        load.wait()
    rows, lanes = ids_ref.shape
    length = rows * lanes
    ids = ids_ref[...]
    valid = valid_ref[...] > 0
    owner = jnp.zeros_like(ids)
    for d in range(1, devices):
        owner += jnp.where(ids >= vocab_local * d, 1, 0)
    keep = [valid & (owner == d) for d in range(devices)]
    marks = jnp.concatenate([jnp.where(k, 1.0, 0.0) for k in keep], axis=0).astype(BF16)
    inside = dot(marks, onehot(iota((lanes, lanes), 0) <= iota((lanes, lanes), 1)))
    total = dot(marks, jnp.ones((lanes, lanes), BF16))
    n = devices * rows
    r, c_ = iota((n, n), 0), iota((n, n), 1)
    before = dot(onehot((r // (2 * rows) == c_ // (2 * rows)) & (c_ < r)), total.astype(BF16))
    rank = inside + before - 1.0
    code = jnp.full((rows, lanes), -1, I32)
    for d in range(devices):
        code = jnp.where(keep[d], d // 2 * length + rank[d * rows:(d + 1) * rows].astype(I32), code)
    own_id = jnp.where(valid, ids - me * vocab_local, -1)
    for k in range(rows):
        code_ref[:, k * lanes:(k + 1) * lanes] = code[k:k + 1]
        id_row[:, k * lanes:(k + 1) * lanes] = own_id[k:k + 1]
    after = before + total
    ours = iota((n, lanes), 0) // rows == me
    low = jnp.min(jnp.where(ours, before, 1e6)).astype(I32)
    high = jnp.max(jnp.where(ours, after, 0.0)).astype(I32)
    counts = [jnp.max(after[c * 2 * rows:(c + 1) * 2 * rows]).astype(I32) for c in range(chips)]
    which = jnp.int32(len(plans) - 1)
    cap = pick_of(plans[-1], chip)
    for v in range(len(plans) - 2, -1, -1):
        fits = counts[0] <= plans[v][0] * BLOCK
        for c in range(1, chips):
            fits &= counts[c] <= plans[v][c] * BLOCK
        which = jnp.where(fits, v, which)
        cap = jnp.where(fits, pick_of(plans[v], chip), cap)
    cap_ref[0] = which

    groups = cap * (BLOCK // GROUP)
    first, last = low // GROUP, (high + GROUP - 1) // GROUP
    last = jnp.where(high > low, last, first)

    local = id_row[...]
    owned = (local >= 0) & (local < vocab_local)
    tile = local >> 3
    sub = iota((8, length), 0)
    digits = jnp.where(sub == 0, tile >> 6, jnp.where(sub == 1, tile & 63, jnp.where(sub == 2, local & 7, 1)))
    digits = jnp.where(owned & (sub < 4), digits, 0).astype(F32).astype(BF16)

    def fill(kb):
        hot = onehot(code_ref[...] == chip * length + kb * lanes + iota((lanes, length), 0))
        found = dot(hot, digits, ((1,), (1,)))
        pick[pl.ds(pl.multiple_of(kb * lanes, lanes), lanes), :] = found
        across = found.T
        table[pl.ds(kb, 1), :] = (across[0:1] * 64.0 + across[1:2]).astype(I32)
        to_smem(kb).start()

    def to_smem(kb):
        return pltpu.make_async_copy(table.at[pl.ds(kb, 1), :], table_s.at[pl.ds(kb, 1), :], table_sem.at[kb])

    loop(jnp.where(high > low, (high + lanes - 1) // lanes, 0), fill, low // lanes)

    def issue(g):
        per = lanes // GROUP
        line, offset, slot = g // per, lax.rem(g, per) * GROUP, lax.rem(g, RING)

        @pl.when((offset == 0) | (g == first))
        def _():
            to_smem(line).wait()
        for i in range(GROUP):
            pltpu.make_async_copy(w_ref.at[table_s[line, offset + i]], stage.at[slot, i], in_sem.at[slot]).start()

    loop(jnp.minimum(last, first + RING), issue, first)

    def blank(g):
        part_ref[pl.ds(pl.multiple_of(g * GROUP, GROUP), GROUP), :] = jnp.zeros((GROUP, part_ref.shape[1]), BF16)

    loop(first, blank)
    loop(groups, blank, last)

    def step(g):
        slot = lax.rem(g, RING)
        pltpu.make_async_copy(w_ref.at[pl.ds(0, GROUP)], stage.at[slot], in_sem.at[slot]).wait()
        for k in range(GROUP // SELECT):
            here = pl.ds(pl.multiple_of(g * GROUP + k * SELECT, SELECT), SELECT)
            found = pick[here, :]
            row = jnp.where(found[:, 3:4] > 0.5, found[:, 2:3], -4096.0).astype(I32)
            sel = onehot(iota((SELECT, 8 * SELECT), 1) - 8 * iota((SELECT, 8 * SELECT), 0) == row)
            tiles = stage[slot, k * SELECT:(k + 1) * SELECT].reshape(8 * SELECT, part_ref.shape[1])
            part_ref[here, :] = dot(sel, tiles).astype(BF16)

        @pl.when(g + RING < last)
        def _():
            issue(g + RING)

    loop(last, step, first)


def cuts_of(ms):
    cuts = []
    for s in range(4):
        through_y, through_x = ms[s ^ 2], ms[s ^ 1]
        cuts.append(min(max((through_y + ms[s] - through_x + 1) // 2, 0), ms[s]))
    return cuts


def link_load(ms):
    cuts = cuts_of(ms)
    return max(max(ms[s ^ 2] + ms[s] - cuts[s], ms[s ^ 1] + cuts[s]) for s in range(4))


def exchange_kernel(ms, length, hid, part, code_ref, acc, inc, rows, split, send, inc_recv, recv, p_recv):
    cuts, total = cuts_of(ms), sum(ms)
    steps = -(-total // WINDOW)
    from_x = [ms[r ^ 1] + ms[r ^ 3] - cuts[r ^ 3] for r in range(4)]
    from_y = [ms[r ^ 2] + cuts[r ^ 3] for r in range(4)]
    both = [min(u, v) for u, v in zip(from_x, from_y)]
    longer = [int(v > u) for u, v in zip(from_x, from_y)]

    me = lax.axis_index("vocab")
    chip, core = me // 2, lax.rem(me, 2)
    x, y = lax.rem(chip, 2), chip // 2
    mate = {"vocab": me + 1 - 2 * core}
    x_dev = {"vocab": me + 2 - 4 * x}
    y_dev = {"vocab": me + 4 - 8 * y}
    x_chip, y_chip, d_chip = y * 2 + 1 - x, (1 - y) * 2 + x, (1 - y) * 2 + 1 - x
    mine, other = core * HALF, (1 - core) * HALF
    m, m_x, m_y, m_d = (pick_of(ms, c) for c in (chip, x_chip, y_chip, d_chip))
    cut_x, cut_y = pick_of(cuts, x_chip), pick_of(cuts, y_chip)
    shared, tail_side = pick_of(both, chip), pick_of(longer, chip)

    barrier = pltpu.get_barrier_semaphore()
    for dev in (mate, x_dev, y_dev):
        pl.semaphore_signal(barrier, inc=1, device_id=dev, device_id_type=MESH)

    def start_value(i):
        start = jnp.where(code_ref[...] >= 0, 0.0, -jnp.inf)
        acc[pl.ds(pl.multiple_of(i * 8, 8), 8), :] = jnp.broadcast_to(start, (8, length))

    loop(acc.shape[0] // 8, start_value)
    if total < steps * WINDOW:
        rows[total * BLOCK:, :] = jnp.zeros((steps * WINDOW * BLOCK - total * BLOCK, rows.shape[1]), BF16)
    pl.semaphore_wait(barrier, 3)

    def at(block, side):
        return rows.at[pl.ds(pl.multiple_of(block * BLOCK + side, HALF), HALF), :]

    def remote(src, dst, sent, received, dev):
        return pltpu.make_async_remote_copy(src_ref=src, dst_ref=dst, send_sem=sent, recv_sem=received,
                                            device_id=dev, device_id_type=MESH)

    def wait_for(n, sem):
        chunk = rows.at[pl.ds(0, n * HALF), :]
        remote(chunk, chunk, send.at[0], sem, mate).wait_recv()

    def inc_copy(i):
        return remote(part.at[pl.ds(pl.multiple_of(i * BLOCK + other, HALF), HALF), :],
                      inc.at[pl.ds(pl.multiple_of(i * HALF, HALF), HALF), :],
                      send.at[0], inc_recv.at[i], mate)

    def to_link(block, side, t, sent):
        there, dev = ((x_chip, x_dev), (y_chip, y_dev))[side]
        pair_up = pick_of(both, there)
        place = jnp.where(t < pair_up, 2 * t + side, pair_up + t)
        return remote(at(block, mine), at(pick_of(ms, there) + place, mine), send.at[sent], recv.at[place], dev)

    def pair(b):
        return remote(at(b, mine), at(b, mine), send.at[3], p_recv.at[b // WINDOW], mate)

    loop(m, lambda i: inc_copy(jnp.where(i == 0, 0, jnp.where(i == 1, m - 1, i - 1))).start())

    def merge(i):
        wait_for(1, inc_recv.at[i])
        src = pl.ds(pl.multiple_of(i * BLOCK + mine, HALF), HALF)
        rows[src, :] = part[src, :] + inc[pl.ds(pl.multiple_of(i * HALF, HALF), HALF), :]

    merge(0)
    merge(m - 1)
    to_link(0, 0, 0, 1).start()
    to_link(m - 1, 1, 0, 2).start()
    loop(m - 1, merge, 1)

    def send_own(t):
        to_link(t, 0, t, 1).start()
        to_link(m - 1 - t, 1, t, 2).start()

    loop(m, send_own, 1)
    loop(m, lambda i: pair(i).start())

    def source(p):
        paired = p < 2 * shared
        return jnp.where(paired, lax.rem(p + 2 * total, 2), tail_side), jnp.where(paired, p // 2, p - shared)

    def arrived(p):
        side, t = source(p)
        wait_for(1, recv.at[p])
        pair(m + p).start()

        @pl.when((side == 0) & (t < cut_x))
        def _():
            to_link(m + p, 1, m + t, 4).start()

        @pl.when((side == 1) & (t < m_y - cut_y))
        def _():
            to_link(m + p, 0, m + t, 4).start()

    def base(b):
        side, t = source(b - m)
        near = t < jnp.where(side == 0, m_x, m_y)
        of = jnp.where(near, jnp.where(side == 0, x_chip, y_chip), d_chip)
        i = jnp.where(side == 0, jnp.where(near, t, m_d - 1 - (t - m_x)), jnp.where(near, m_y - 1 - t, t - m_y))
        of, i = jnp.where(b < m, chip, of), jnp.where(b < m, b, i)
        return jnp.where(b < total, of * length + i * BLOCK, -length)

    width = WINDOW * BLOCK
    step_n = length // WINDOW
    left = total - (steps - 1) * WINDOW

    def window(w):
        if left == WINDOW:
            wait_for(WINDOW, p_recv.at[w])
        else:
            @pl.when(w < steps - 1)
            def _():
                wait_for(WINDOW, p_recv.at[w])

            @pl.when(w == steps - 1)
            def _():
                wait_for(left, p_recv.at[w])
        got = rows[pl.ds(pl.multiple_of(w * width, width), width), :]
        s = dot(hid[...], got, ((1,), (1,))) * INV_TEMP
        high = s.astype(BF16)
        rest = s - high.astype(F32)
        middle = rest.astype(BF16)
        split[:, :width] = high
        split[:, width:2 * width] = middle
        split[:, 2 * width:] = (rest - middle.astype(F32)).astype(BF16)
        slot = jnp.concatenate([base(w * WINDOW + k) + iota((BLOCK, step_n), 0) for k in range(WINDOW)], axis=0)

        def columns(c):
            cols = pl.ds(pl.multiple_of(c * step_n, step_n), step_n)
            hot = onehot(code_ref[:, cols] == slot)
            acc[:, cols] += dot(split[...], jnp.concatenate([hot, hot, hot], axis=0))

            @pl.when(c < 2)
            def _():
                start = (w + 1) * WINDOW - m + 2 * c
                loop(jnp.minimum(start + 2, total - m), arrived, jnp.maximum(start, 0))

        loop(WINDOW, columns)

    loop(WINDOW - m, arrived)
    loop(steps, window)

    def drain(q):
        amounts = (ms[q], ms[q], ms[q], total, cuts[q ^ 1] + ms[q ^ 2] - cuts[q ^ 2])
        for k, blocks in enumerate(amounts):
            if blocks:
                chunk = rows.at[pl.ds(0, blocks * HALF), :]
                remote(chunk, chunk, send.at[k], recv.at[0], mate).wait_send()

    if len(set(ms)) == 1 and len({cuts[q ^ 1] + ms[q ^ 2] - cuts[q ^ 2] for q in range(4)}) == 1:
        drain(0)
    else:
        for q in range(4):
            pl.when(chip == q)(functools.partial(drain, q))


def finish_kernel(s_ref, target_ref, prob_ref, logp_ref, prob, column, sem):
    rows, tile = prob.shape[0], target_ref.shape[1]
    lane = iota((FINISH, prob.shape[1]), 1)

    def turn_in(i):
        target = jnp.broadcast_to(target_ref[pl.ds(i, 1), :].astype(F32), (tile, tile)).T[:, :1]
        column[pl.ds(pl.multiple_of(i * tile, tile), tile), :] = target

    def block(i):
        here = pl.ds(pl.multiple_of(i * FINISH, FINISH), FINISH)
        s = s_ref[here, :]
        top = jnp.max(s, axis=1, keepdims=True)
        e = jnp.exp(s - top)
        total = jnp.sum(e, axis=1, keepdims=True)
        prob[here, :] = e * (1.0 / total)
        picked = jnp.sum(jnp.where(lane == column[here, :].astype(I32), s, 0.0), axis=1, keepdims=True)
        column[here, :] = picked - (top + jnp.log(total))
        pltpu.make_async_copy(prob.at[here, :], prob_ref.at[here, :], sem).start()

    def turn_out(i):
        value = column[pl.ds(pl.multiple_of(i * tile, tile), tile), :]
        logp_ref[pl.ds(i, 1), :] = jnp.broadcast_to(value, (tile, tile)).T[:1]

    loop(rows // tile, turn_in)
    loop(rows // FINISH, block)
    loop(rows // tile, turn_out)
    pltpu.make_async_copy(prob, prob_ref, sem).wait()


def solution(mesh):
    shards = mesh.shape["vocab"]
    chips = shards // 2
    hbm = pl.BlockSpec(memory_space=pl.ANY)
    vmem = pl.BlockSpec(memory_space=pltpu.VMEM)

    def device_step(hidden, w_head, allowed_ids, allowed_valid, target_pos):
        rows_dev, depth = hidden.shape
        length = allowed_ids.shape[0]
        most = length // BLOCK
        plans = sorted({p for p in PLANS if max(p) < most}, key=lambda p: (link_load(p), sum(p))) + [(most,) * chips]
        lanes = 128
        part, code, which = pl.pallas_call(
            functools.partial(gather_kernel, chips, w_head.shape[0], plans),
            out_shape=(pltpu.VMEM((length, depth), BF16),
                       pltpu.VMEM((1, length), I32),
                       jax.ShapeDtypeStruct((1,), I32)),
            in_specs=[pl.BlockSpec(memory_space=pltpu.HBM)] * 3,
            out_specs=(vmem, vmem, pl.BlockSpec(memory_space=pltpu.SMEM)),
            scratch_shapes=[
                pltpu.VMEM((length // lanes, lanes), I32),
                pltpu.VMEM((length // lanes, lanes), I32),
                pltpu.VMEM((1, length), I32),
                pltpu.VMEM((length // lanes, lanes), I32),
                pltpu.SMEM((length // lanes, lanes), I32),
                pltpu.VMEM((length, 8), F32),
                pltpu.VMEM((RING, GROUP, 8, depth), BF16),
                pltpu.SemaphoreType.DMA((2,)),
                pltpu.SemaphoreType.DMA((length // lanes,)),
                pltpu.SemaphoreType.DMA((RING,)),
            ],
            compiler_params=pltpu.CompilerParams(vmem_limit_bytes=28 * MIB),
            name="gather_rows",
        )(*(pltpu.with_memory_space_constraint(v, pltpu.HBM) for v in (allowed_ids.reshape(-1, lanes), allowed_valid.reshape(-1, lanes))), w_head.reshape(-1, 8, depth))

        tile = 128
        finish = pl.pallas_call(
            finish_kernel,
            out_shape=(jax.ShapeDtypeStruct((rows_dev, length), F32),
                       jax.ShapeDtypeStruct((rows_dev // tile, tile), F32)),
            in_specs=[vmem, vmem],
            out_specs=(hbm, vmem),
            scratch_shapes=[pltpu.VMEM((rows_dev, length), F32), pltpu.VMEM((rows_dev, 1), F32), pltpu.SemaphoreType.DMA],
            compiler_params=pltpu.CompilerParams(vmem_limit_bytes=16 * MIB),
            name="finish",
        )

        def serve(ms, cid):
            total, steps = sum(ms), -(-sum(ms) // WINDOW)
            dma = lambda n: pltpu.SemaphoreType.DMA((n,))
            exchange = pl.pallas_call(
                functools.partial(exchange_kernel, ms, length),
                out_shape=pltpu.VMEM((rows_dev, length), F32),
                in_specs=[vmem, vmem, vmem],
                out_specs=vmem,
                scratch_shapes=[
                    pltpu.VMEM((max(ms) * HALF, depth), BF16),
                    pltpu.VMEM((steps * WINDOW * BLOCK, depth), BF16),
                    pltpu.VMEM((rows_dev, 3 * WINDOW * BLOCK), BF16),
                    dma(5), dma(max(ms)), dma(total - min(ms)), dma(steps),
                ],
                compiler_params=pltpu.CompilerParams(collective_id=cid, has_side_effects=True,
                                                     vmem_limit_bytes=(8 + total // 5 + max(ms) // 10) * MIB),
                name="exchange_" + "_".join(map(str, ms)),
            )
            return lambda hidden, part, code, target: finish(exchange(hidden, part, code), target)

        probs, logp = lax.switch(which[0], [serve(ms, k) for k, ms in enumerate(plans)],
                                 hidden, part, code, target_pos.reshape(-1, tile))
        return probs, logp.reshape(rows_dev)

    row_spec = P(("rep", "vocab"))
    mat_spec = P(("rep", "vocab"), None)
    return jax.shard_map(device_step, mesh=mesh, in_specs=(mat_spec, P("vocab", None), P("rep"), P("rep"), row_spec),
                         out_specs=(mat_spec, row_spec), check_vma=False)


PLANS = [(k,) * 4 for k in (6, 7, 8, 9, 10, 11, 12, 14, 16)]
for heavy, others in ((15, 8), (11, 7), (10, 6), (12, 8)):
    PLANS += [tuple(heavy if c == h else others for c in range(4)) for h in range(4)]
```

```python
import functools

import jax
import jax.numpy as jnp
from jax import lax
from jax.experimental import pallas as pl
from jax.experimental.pallas import tpu as pltpu
from jax.sharding import PartitionSpec as P

INV_TEMP = 1.25
BLOCK = 64
HALF = BLOCK // 2
WINDOW = 4
GROUP = 64
SELECT = 32
RING = 10
FINISH = 128
MIB = 2 ** 20
MESH = pl.DeviceIdType.MESH
BF16, F32, I32 = jnp.bfloat16, jnp.float32, jnp.int32


def iota(shape, dim):
    return lax.broadcasted_iota(I32, shape, dim)


def onehot(mask):
    return jnp.where(mask, 1.0, 0.0).astype(BF16)


def dot(a, b, dims=((1,), (0,))):
    return lax.dot_general(a, b, (dims, ((), ())), preferred_element_type=F32)


def loop(n, f, start=0):
    def body(i, carry):
        f(i)
        return carry
    lax.fori_loop(start, n, body, 0)


def pick_of(table, index):
    value = jnp.int32(table[0])
    for k in range(1, len(table)):
        if table[k] != table[0]:
            value = jnp.where(index == k, table[k], value)
    return value


def gather_kernel(chips, vocab_local, plans, ids_hbm, valid_hbm, w_ref, target_hbm, part_ref, code_ref, column_ref, cap_ref,
                  ids_ref, valid_ref, target_ref, id_row, turned, table, table_s, pick, stage, load_sem, table_sem, in_sem):
    me = lax.axis_index("vocab")
    chip, devices = me // 2, 2 * chips
    loads = [pltpu.make_async_copy(ids_hbm, ids_ref, load_sem.at[0]),
             pltpu.make_async_copy(valid_hbm, valid_ref, load_sem.at[1]),
             pltpu.make_async_copy(target_hbm, target_ref, load_sem.at[2])]
    for load in loads:
        load.start()
    for load in loads:
        load.wait()
    rows, lanes = ids_ref.shape
    length = rows * lanes
    ids = ids_ref[...]
    valid = valid_ref[...] > 0
    owner = jnp.zeros_like(ids)
    for d in range(1, devices):
        owner += jnp.where(ids >= vocab_local * d, 1, 0)
    keep = [valid & (owner == d) for d in range(devices)]
    marks = jnp.concatenate([jnp.where(k, 1.0, 0.0) for k in keep], axis=0).astype(BF16)
    inside = dot(marks, onehot(iota((lanes, lanes), 0) <= iota((lanes, lanes), 1)))
    total = dot(marks, jnp.ones((lanes, lanes), BF16))
    n = devices * rows
    r, c_ = iota((n, n), 0), iota((n, n), 1)
    before = dot(onehot((r // (2 * rows) == c_ // (2 * rows)) & (c_ < r)), total.astype(BF16))
    rank = inside + before - 1.0
    code = jnp.full((rows, lanes), -1, I32)
    for d in range(devices):
        code = jnp.where(keep[d], d // 2 * length + rank[d * rows:(d + 1) * rows].astype(I32), code)
    own_id = jnp.where(valid, ids - me * vocab_local, -1)
    for k in range(rows):
        code_ref[:, k * lanes:(k + 1) * lanes] = code[k:k + 1]
        id_row[:, k * lanes:(k + 1) * lanes] = own_id[k:k + 1]
    after = before + total
    ours = iota((n, lanes), 0) // rows == me
    low = jnp.min(jnp.where(ours, before, 1e6)).astype(I32)
    high = jnp.max(jnp.where(ours, after, 0.0)).astype(I32)
    counts = [jnp.max(after[c * 2 * rows:(c + 1) * 2 * rows]).astype(I32) for c in range(chips)]
    which = jnp.int32(len(plans) - 1)
    cap = pick_of(plans[-1], chip)
    for v in range(len(plans) - 2, -1, -1):
        fits = counts[0] <= plans[v][0] * BLOCK
        for c in range(1, chips):
            fits &= counts[c] <= plans[v][c] * BLOCK
        which = jnp.where(fits, v, which)
        cap = jnp.where(fits, pick_of(plans[v], chip), cap)
    cap_ref[0] = which

    groups = cap * (BLOCK // GROUP)
    first, last = low // GROUP, (high + GROUP - 1) // GROUP
    last = jnp.where(high > low, last, first)

    local = id_row[...]
    owned = (local >= 0) & (local < vocab_local)
    tile = local >> 3
    sub = iota((8, length), 0)
    digits = jnp.where(sub == 0, tile >> 6, jnp.where(sub == 1, tile & 63, jnp.where(sub == 2, local & 7, 1)))
    digits = jnp.where(owned & (sub < 4), digits, 0).astype(F32)

    for k in range(rows):
        turned[k * lanes:(k + 1) * lanes, :] = digits[:, k * lanes:(k + 1) * lanes].T.astype(BF16)

    def fill(kb):
        hot = onehot(code_ref[...] == chip * length + kb * lanes + iota((lanes, length), 0))
        found = dot(hot, turned[...])
        pick[pl.ds(pl.multiple_of(kb * lanes, lanes), lanes), :] = found
        across = found.T
        table[pl.ds(kb, 1), :] = (across[0:1] * 64.0 + across[1:2]).astype(I32)
        to_smem(kb).start()

    def to_smem(kb):
        return pltpu.make_async_copy(table.at[pl.ds(kb, 1), :], table_s.at[pl.ds(kb, 1), :], table_sem.at[kb])

    loop(jnp.where(high > low, (high + lanes - 1) // lanes, 0), fill, low // lanes)

    def issue(g):
        per = lanes // GROUP
        line, offset, slot = g // per, lax.rem(g, per) * GROUP, lax.rem(g, RING)

        @pl.when((offset == 0) | (g == first))
        def _():
            to_smem(line).wait()
        for i in range(GROUP):
            pltpu.make_async_copy(w_ref.at[table_s[line, offset + i]], stage.at[slot, i], in_sem.at[slot]).start()

    loop(jnp.minimum(last, first + RING), issue, first)

    tile = target_ref.shape[1]
    for k in range(target_ref.shape[0]):
        target = jnp.broadcast_to(target_ref[k:k + 1, :].astype(F32), (tile, tile)).T
        column_ref[k * tile:(k + 1) * tile, :] = target[:, :1]

    def blank(g):
        part_ref[pl.ds(pl.multiple_of(g * GROUP, GROUP), GROUP), :] = jnp.zeros((GROUP, part_ref.shape[1]), BF16)

    loop(first, blank)
    loop(groups, blank, last)

    def step(g):
        slot = lax.rem(g, RING)
        pltpu.make_async_copy(w_ref.at[pl.ds(0, GROUP)], stage.at[slot], in_sem.at[slot]).wait()
        for k in range(GROUP // SELECT):
            here = pl.ds(pl.multiple_of(g * GROUP + k * SELECT, SELECT), SELECT)
            found = pick[here, :]
            row = jnp.where(found[:, 3:4] > 0.5, found[:, 2:3], -4096.0).astype(I32)
            sel = onehot(iota((SELECT, 8 * SELECT), 1) - 8 * iota((SELECT, 8 * SELECT), 0) == row)
            tiles = stage[slot, k * SELECT:(k + 1) * SELECT].reshape(8 * SELECT, part_ref.shape[1])
            part_ref[here, :] = dot(sel, tiles).astype(BF16)

        @pl.when(g + RING < last)
        def _():
            issue(g + RING)

    loop(last, step, first)


def cuts_of(ms):
    cuts = []
    for s in range(4):
        through_y, through_x = ms[s ^ 2], ms[s ^ 1]
        cuts.append(min(max((through_y + ms[s] - through_x + 1) // 2, 0), ms[s]))
    return cuts


def link_load(ms):
    cuts = cuts_of(ms)
    return max(max(ms[s ^ 2] + ms[s] - cuts[s], ms[s ^ 1] + cuts[s]) for s in range(4))


def exchange_kernel(ms, length, hid, part, code_ref, acc, inc, rows, split, send, inc_recv, recv, p_recv):
    cuts, total = cuts_of(ms), sum(ms)
    steps = -(-total // WINDOW)
    from_x = [ms[r ^ 1] + ms[r ^ 3] - cuts[r ^ 3] for r in range(4)]
    from_y = [ms[r ^ 2] + cuts[r ^ 3] for r in range(4)]
    both = [min(u, v) for u, v in zip(from_x, from_y)]
    longer = [int(v > u) for u, v in zip(from_x, from_y)]

    me = lax.axis_index("vocab")
    chip, core = me // 2, lax.rem(me, 2)
    x, y = lax.rem(chip, 2), chip // 2
    mate = {"vocab": me + 1 - 2 * core}
    x_dev = {"vocab": me + 2 - 4 * x}
    y_dev = {"vocab": me + 4 - 8 * y}
    x_chip, y_chip, d_chip = y * 2 + 1 - x, (1 - y) * 2 + x, (1 - y) * 2 + 1 - x
    mine, other = core * HALF, (1 - core) * HALF
    m, m_x, m_y, m_d = (pick_of(ms, c) for c in (chip, x_chip, y_chip, d_chip))
    cut_x, cut_y = pick_of(cuts, x_chip), pick_of(cuts, y_chip)
    shared, tail_side = pick_of(both, chip), pick_of(longer, chip)

    barrier = pltpu.get_barrier_semaphore()
    for dev in (mate, x_dev, y_dev):
        pl.semaphore_signal(barrier, inc=1, device_id=dev, device_id_type=MESH)

    def start_value(i):
        start = jnp.where(code_ref[...] >= 0, 0.0, -jnp.inf)
        acc[pl.ds(pl.multiple_of(i * 8, 8), 8), :] = jnp.broadcast_to(start, (8, length))

    loop(acc.shape[0] // 8, start_value)
    if total < steps * WINDOW:
        rows[total * BLOCK:, :] = jnp.zeros((steps * WINDOW * BLOCK - total * BLOCK, rows.shape[1]), BF16)
    pl.semaphore_wait(barrier, 3)

    def at(block, side):
        return rows.at[pl.ds(pl.multiple_of(block * BLOCK + side, HALF), HALF), :]

    def remote(src, dst, sent, received, dev):
        return pltpu.make_async_remote_copy(src_ref=src, dst_ref=dst, send_sem=sent, recv_sem=received,
                                            device_id=dev, device_id_type=MESH)

    def wait_for(n, sem):
        chunk = rows.at[pl.ds(0, n * HALF), :]
        remote(chunk, chunk, send.at[0], sem, mate).wait_recv()

    def inc_copy(i):
        return remote(part.at[pl.ds(pl.multiple_of(i * BLOCK + other, HALF), HALF), :],
                      inc.at[pl.ds(pl.multiple_of(i * HALF, HALF), HALF), :],
                      send.at[0], inc_recv.at[i], mate)

    def to_link(block, side, t, sent):
        there, dev = ((x_chip, x_dev), (y_chip, y_dev))[side]
        pair_up = pick_of(both, there)
        place = jnp.where(t < pair_up, 2 * t + side, pair_up + t)
        return remote(at(block, mine), at(pick_of(ms, there) + place, mine), send.at[sent], recv.at[place], dev)

    def pair(b):
        return remote(at(b, mine), at(b, mine), send.at[3], p_recv.at[b // WINDOW], mate)

    loop(m, lambda i: inc_copy(jnp.where(i == 0, 0, jnp.where(i == 1, m - 1, i - 1))).start())

    def merge(i):
        wait_for(1, inc_recv.at[i])
        src = pl.ds(pl.multiple_of(i * BLOCK + mine, HALF), HALF)
        rows[src, :] = part[src, :] + inc[pl.ds(pl.multiple_of(i * HALF, HALF), HALF), :]

    merge(0)
    merge(m - 1)
    to_link(0, 0, 0, 1).start()
    to_link(m - 1, 1, 0, 2).start()
    loop(m - 1, merge, 1)

    def send_own(t):
        to_link(t, 0, t, 1).start()
        to_link(m - 1 - t, 1, t, 2).start()

    loop(m, send_own, 1)
    loop(m, lambda i: pair(i).start())

    def source(p):
        paired = p < 2 * shared
        return jnp.where(paired, lax.rem(p + 2 * total, 2), tail_side), jnp.where(paired, p // 2, p - shared)

    def arrived(p):
        side, t = source(p)
        wait_for(1, recv.at[p])
        pair(m + p).start()

        @pl.when((side == 0) & (t < cut_x))
        def _():
            to_link(m + p, 1, m + t, 4).start()

        @pl.when((side == 1) & (t < m_y - cut_y))
        def _():
            to_link(m + p, 0, m + t, 4).start()

    def base(b):
        side, t = source(b - m)
        near = t < jnp.where(side == 0, m_x, m_y)
        of = jnp.where(near, jnp.where(side == 0, x_chip, y_chip), d_chip)
        i = jnp.where(side == 0, jnp.where(near, t, m_d - 1 - (t - m_x)), jnp.where(near, m_y - 1 - t, t - m_y))
        of, i = jnp.where(b < m, chip, of), jnp.where(b < m, b, i)
        return jnp.where(b < total, of * length + i * BLOCK, -length)

    width = WINDOW * BLOCK
    step_n = length // WINDOW
    left = total - (steps - 1) * WINDOW

    def window(w):
        if left == WINDOW:
            wait_for(WINDOW, p_recv.at[w])
        else:
            @pl.when(w < steps - 1)
            def _():
                wait_for(WINDOW, p_recv.at[w])

            @pl.when(w == steps - 1)
            def _():
                wait_for(left, p_recv.at[w])
        got = rows[pl.ds(pl.multiple_of(w * width, width), width), :]
        s = dot(hid[...], got, ((1,), (1,))) * INV_TEMP
        high = s.astype(BF16)
        rest = s - high.astype(F32)
        middle = rest.astype(BF16)
        split[:, :width] = high
        split[:, width:2 * width] = middle
        split[:, 2 * width:] = (rest - middle.astype(F32)).astype(BF16)
        slot = jnp.concatenate([base(w * WINDOW + k) + iota((BLOCK, step_n), 0) for k in range(WINDOW)], axis=0)

        def columns(c):
            cols = pl.ds(pl.multiple_of(c * step_n, step_n), step_n)
            hot = onehot(code_ref[:, cols] == slot)
            acc[:, cols] += dot(split[...], jnp.concatenate([hot, hot, hot], axis=0))

            @pl.when(c < 2)
            def _():
                start = (w + 1) * WINDOW - m + 2 * c
                loop(jnp.minimum(start + 2, total - m), arrived, jnp.maximum(start, 0))

        loop(WINDOW, columns)

    loop(WINDOW - m, arrived)
    loop(steps, window)

    def drain(q):
        amounts = (ms[q], ms[q], ms[q], total, cuts[q ^ 1] + ms[q ^ 2] - cuts[q ^ 2])
        for k, blocks in enumerate(amounts):
            if blocks:
                chunk = rows.at[pl.ds(0, blocks * HALF), :]
                remote(chunk, chunk, send.at[k], recv.at[0], mate).wait_send()

    if len(set(ms)) == 1 and len({cuts[q ^ 1] + ms[q ^ 2] - cuts[q ^ 2] for q in range(4)}) == 1:
        drain(0)
    else:
        for q in range(4):
            pl.when(chip == q)(functools.partial(drain, q))


def finish_kernel(s_ref, target_ref, prob_ref, logp_ref, prob, column, sem):
    rows, tile = prob.shape[0], logp_ref.shape[1]
    lane = iota((FINISH, prob.shape[1]), 1)

    def block(i):
        here = pl.ds(pl.multiple_of(i * FINISH, FINISH), FINISH)
        s = s_ref[here, :]
        top = jnp.max(s, axis=1, keepdims=True)
        e = jnp.exp(s - top)
        total = jnp.sum(e, axis=1, keepdims=True)
        prob[here, :] = e * (1.0 / total)
        picked = jnp.sum(jnp.where(lane == target_ref[here, :].astype(I32), s, 0.0), axis=1, keepdims=True)
        column[here, :] = picked - (top + jnp.log(total))
        pltpu.make_async_copy(prob.at[here, :], prob_ref.at[here, :], sem).start()

    def turn_out(i):
        value = column[pl.ds(pl.multiple_of(i * tile, tile), tile), :]
        logp_ref[pl.ds(i, 1), :] = jnp.broadcast_to(value, (tile, tile)).T[:1]

    loop(rows // FINISH, block)
    loop(rows // tile, turn_out)
    pltpu.make_async_copy(prob, prob_ref, sem).wait()


def solution(mesh):
    shards = mesh.shape["vocab"]
    chips = shards // 2
    hbm = pl.BlockSpec(memory_space=pl.ANY)
    vmem = pl.BlockSpec(memory_space=pltpu.VMEM)

    def device_step(hidden, w_head, allowed_ids, allowed_valid, target_pos):
        rows_dev, depth = hidden.shape
        length = allowed_ids.shape[0]
        most = length // BLOCK
        plans = sorted({p for p in PLANS if max(p) < most}, key=lambda p: (link_load(p), sum(p))) + [(most,) * chips]
        lanes = 128
        tile = 128
        part, code, column, which = pl.pallas_call(
            functools.partial(gather_kernel, chips, w_head.shape[0], plans),
            out_shape=(pltpu.VMEM((length, depth), BF16),
                       pltpu.VMEM((1, length), I32),
                       pltpu.VMEM((rows_dev, 1), F32),
                       jax.ShapeDtypeStruct((1,), I32)),
            in_specs=[pl.BlockSpec(memory_space=pltpu.HBM)] * 4,
            out_specs=(vmem, vmem, vmem, pl.BlockSpec(memory_space=pltpu.SMEM)),
            scratch_shapes=[
                pltpu.VMEM((length // lanes, lanes), I32),
                pltpu.VMEM((length // lanes, lanes), I32),
                pltpu.VMEM((rows_dev // tile, tile), I32),
                pltpu.VMEM((1, length), I32),
                pltpu.VMEM((length, 8), BF16),
                pltpu.VMEM((length // lanes, lanes), I32),
                pltpu.SMEM((length // lanes, lanes), I32),
                pltpu.VMEM((length, 8), F32),
                pltpu.VMEM((RING, GROUP, 8, depth), BF16),
                pltpu.SemaphoreType.DMA((3,)),
                pltpu.SemaphoreType.DMA((length // lanes,)),
                pltpu.SemaphoreType.DMA((RING,)),
            ],
            compiler_params=pltpu.CompilerParams(vmem_limit_bytes=28 * MIB),
            name="gather_rows",
        )(*(pltpu.with_memory_space_constraint(v, pltpu.HBM) for v in (allowed_ids.reshape(-1, lanes), allowed_valid.reshape(-1, lanes))), w_head.reshape(-1, 8, depth),
          pltpu.with_memory_space_constraint(target_pos.reshape(-1, tile), pltpu.HBM))

        finish = pl.pallas_call(
            finish_kernel,
            out_shape=(jax.ShapeDtypeStruct((rows_dev, length), F32),
                       jax.ShapeDtypeStruct((rows_dev // tile, tile), F32)),
            in_specs=[vmem, vmem],
            out_specs=(hbm, vmem),
            scratch_shapes=[pltpu.VMEM((rows_dev, length), F32), pltpu.VMEM((rows_dev, 1), F32), pltpu.SemaphoreType.DMA],
            compiler_params=pltpu.CompilerParams(vmem_limit_bytes=16 * MIB),
            name="finish",
        )

        def serve(ms, cid):
            total, steps = sum(ms), -(-sum(ms) // WINDOW)
            dma = lambda n: pltpu.SemaphoreType.DMA((n,))
            exchange = pl.pallas_call(
                functools.partial(exchange_kernel, ms, length),
                out_shape=pltpu.VMEM((rows_dev, length), F32),
                in_specs=[vmem, vmem, vmem],
                out_specs=vmem,
                scratch_shapes=[
                    pltpu.VMEM((max(ms) * HALF, depth), BF16),
                    pltpu.VMEM((steps * WINDOW * BLOCK, depth), BF16),
                    pltpu.VMEM((rows_dev, 3 * WINDOW * BLOCK), BF16),
                    dma(5), dma(max(ms)), dma(total - min(ms)), dma(steps),
                ],
                compiler_params=pltpu.CompilerParams(collective_id=cid, has_side_effects=True,
                                                     vmem_limit_bytes=(8 + total // 5 + max(ms) // 10) * MIB),
                name="exchange_" + "_".join(map(str, ms)),
            )
            return lambda hidden, part, code, target: finish(exchange(hidden, part, code), target)

        probs, logp = lax.switch(which[0], [serve(ms, k) for k, ms in enumerate(plans)],
                                 hidden, part, code, column)
        return probs, logp.reshape(rows_dev)

    row_spec = P(("rep", "vocab"))
    mat_spec = P(("rep", "vocab"), None)
    return jax.shard_map(device_step, mesh=mesh, in_specs=(mat_spec, P("vocab", None), P("rep"), P("rep"), row_spec),
                         out_specs=(mat_spec, row_spec), check_vma=False)


PLANS = [(k,) * 4 for k in (6, 7, 8, 9, 10, 11, 12, 14, 16)]
for heavy, others in ((15, 8), (11, 7), (10, 6)):
    PLANS += [tuple(heavy if c == h else others for c in range(4)) for h in range(4)]
```

```python
import functools

import jax
import jax.numpy as jnp
from jax import lax
from jax.experimental import pallas as pl
from jax.experimental.pallas import tpu as pltpu
from jax.sharding import PartitionSpec as P

INV_TEMP = 1.25
BLOCK = 64
HALF = BLOCK // 2
WINDOW = 4
GROUP = 128
SELECT = 32
RING = 5
FINISH = 128
MIB = 2 ** 20
MESH = pl.DeviceIdType.MESH
BF16, F32, I32 = jnp.bfloat16, jnp.float32, jnp.int32


def iota(shape, dim):
    return lax.broadcasted_iota(I32, shape, dim)


def onehot(mask):
    return jnp.where(mask, 1.0, 0.0).astype(BF16)


def dot(a, b, dims=((1,), (0,))):
    return lax.dot_general(a, b, (dims, ((), ())), preferred_element_type=F32)


def loop(n, f, start=0):
    def body(i, carry):
        f(i)
        return carry
    lax.fori_loop(start, n, body, 0)


def pick_of(table, index):
    value = jnp.int32(table[0])
    for k in range(1, len(table)):
        if table[k] != table[0]:
            value = jnp.where(index == k, table[k], value)
    return value


def gather_kernel(chips, vocab_local, plans, ids_hbm, valid_hbm, w_ref, target_hbm, part_ref, code_ref, column_ref, cap_ref,
                  ids_ref, valid_ref, target_ref, id_row, turned, table, table_s, pick, stage, load_sem, table_sem, in_sem):
    me = lax.axis_index("vocab")
    chip, devices = me // 2, 2 * chips
    loads = [pltpu.make_async_copy(ids_hbm, ids_ref, load_sem.at[0]),
             pltpu.make_async_copy(valid_hbm, valid_ref, load_sem.at[1]),
             pltpu.make_async_copy(target_hbm, target_ref, load_sem.at[2])]
    for load in loads:
        load.start()
    for load in loads:
        load.wait()
    rows, lanes = ids_ref.shape
    length = rows * lanes
    ids = ids_ref[...]
    valid = valid_ref[...] > 0
    owner = jnp.zeros_like(ids)
    for d in range(1, devices):
        owner += jnp.where(ids >= vocab_local * d, 1, 0)
    keep = [valid & (owner == d) for d in range(devices)]
    marks = jnp.concatenate([jnp.where(k, 1.0, 0.0) for k in keep], axis=0).astype(BF16)
    inside = dot(marks, onehot(iota((lanes, lanes), 0) <= iota((lanes, lanes), 1)))
    total = dot(marks, jnp.ones((lanes, lanes), BF16))
    n = devices * rows
    r, c_ = iota((n, n), 0), iota((n, n), 1)
    before = dot(onehot((r // (2 * rows) == c_ // (2 * rows)) & (c_ < r)), total.astype(BF16))
    rank = inside + before - 1.0
    code = jnp.full((rows, lanes), -1, I32)
    for d in range(devices):
        code = jnp.where(keep[d], d // 2 * length + rank[d * rows:(d + 1) * rows].astype(I32), code)
    own_id = jnp.where(valid, ids - me * vocab_local, -1)
    for k in range(rows):
        code_ref[:, k * lanes:(k + 1) * lanes] = code[k:k + 1]
        id_row[:, k * lanes:(k + 1) * lanes] = own_id[k:k + 1]
    after = before + total
    ours = iota((n, lanes), 0) // rows == me
    low = jnp.min(jnp.where(ours, before, 1e6)).astype(I32)
    high = jnp.max(jnp.where(ours, after, 0.0)).astype(I32)
    counts = [jnp.max(after[c * 2 * rows:(c + 1) * 2 * rows]).astype(I32) for c in range(chips)]
    which = jnp.int32(len(plans) - 1)
    cap = pick_of(plans[-1], chip)
    for v in range(len(plans) - 2, -1, -1):
        fits = counts[0] <= plans[v][0] * BLOCK
        for c in range(1, chips):
            fits &= counts[c] <= plans[v][c] * BLOCK
        which = jnp.where(fits, v, which)
        cap = jnp.where(fits, pick_of(plans[v], chip), cap)
    cap_ref[0] = which

    groups = (cap * BLOCK + GROUP - 1) // GROUP
    first, last = low // GROUP, (high + GROUP - 1) // GROUP
    last = jnp.where(high > low, last, first)

    local = id_row[...]
    owned = (local >= 0) & (local < vocab_local)
    tile = local >> 3
    sub = iota((8, length), 0)
    digits = jnp.where(sub == 0, tile >> 6, jnp.where(sub == 1, tile & 63, jnp.where(sub == 2, local & 7, 1)))
    digits = jnp.where(owned & (sub < 4), digits, 0).astype(F32)

    for k in range(rows):
        turned[k * lanes:(k + 1) * lanes, :] = digits[:, k * lanes:(k + 1) * lanes].T.astype(BF16)

    def fill(kb):
        hot = onehot(code_ref[...] == chip * length + kb * lanes + iota((lanes, length), 0))
        found = dot(hot, turned[...])
        pick[pl.ds(pl.multiple_of(kb * lanes, lanes), lanes), :] = found
        across = found.T
        spread = lax.rem(kb * lanes + iota((1, lanes), 1), w_ref.shape[0])
        table[pl.ds(kb, 1), :] = jnp.where(across[3:4] > 0.5, (across[0:1] * 64.0 + across[1:2]).astype(I32), spread)
        to_smem(kb).start()

    def to_smem(kb):
        return pltpu.make_async_copy(table.at[pl.ds(kb, 1), :], table_s.at[pl.ds(kb, 1), :], table_sem.at[kb])

    loop(jnp.where(high > low, (high + lanes - 1) // lanes, 0), fill, low // lanes)

    def issue(g):
        per = lanes // GROUP
        line, offset, slot = g // per, lax.rem(g, per) * GROUP, lax.rem(g, RING)

        @pl.when((offset == 0) | (g == first))
        def _():
            to_smem(line).wait()
        for i in range(GROUP):
            pltpu.make_async_copy(w_ref.at[table_s[line, offset + i]], stage.at[slot, i], in_sem.at[slot]).start()

    loop(jnp.minimum(last, first + RING), issue, first)

    tile = target_ref.shape[1]
    for k in range(target_ref.shape[0]):
        target = jnp.broadcast_to(target_ref[k:k + 1, :].astype(F32), (tile, tile)).T
        column_ref[k * tile:(k + 1) * tile, :] = target[:, :1]

    def blank(g):
        part_ref[pl.ds(pl.multiple_of(g * GROUP, GROUP), GROUP), :] = jnp.zeros((GROUP, part_ref.shape[1]), BF16)

    loop(first, blank)
    loop(groups, blank, last)

    def step(g):
        slot = lax.rem(g, RING)
        pltpu.make_async_copy(w_ref.at[pl.ds(0, GROUP)], stage.at[slot], in_sem.at[slot]).wait()
        for k in range(GROUP // SELECT):
            here = pl.ds(pl.multiple_of(g * GROUP + k * SELECT, SELECT), SELECT)
            found = pick[here, :]
            row = jnp.where(found[:, 3:4] > 0.5, found[:, 2:3], -4096.0).astype(I32)
            sel = onehot(iota((SELECT, 8 * SELECT), 1) - 8 * iota((SELECT, 8 * SELECT), 0) == row)
            tiles = stage[slot, k * SELECT:(k + 1) * SELECT].reshape(8 * SELECT, part_ref.shape[1])
            part_ref[here, :] = dot(sel, tiles).astype(BF16)

        @pl.when(g + RING < last)
        def _():
            issue(g + RING)

    loop(last, step, first)


def cuts_of(ms):
    cuts = []
    for s in range(4):
        through_y, through_x = ms[s ^ 2], ms[s ^ 1]
        cuts.append(min(max((through_y + ms[s] - through_x + 1) // 2, 0), ms[s]))
    return cuts


def link_load(ms):
    cuts = cuts_of(ms)
    return max(max(ms[s ^ 2] + ms[s] - cuts[s], ms[s ^ 1] + cuts[s]) for s in range(4))


def exchange_kernel(ms, length, hid, part, code_ref, acc, inc, rows, split, send, inc_recv, recv, p_recv):
    cuts, total = cuts_of(ms), sum(ms)
    steps = -(-total // WINDOW)
    from_x = [ms[r ^ 1] + ms[r ^ 3] - cuts[r ^ 3] for r in range(4)]
    from_y = [ms[r ^ 2] + cuts[r ^ 3] for r in range(4)]
    both = [min(u, v) for u, v in zip(from_x, from_y)]
    longer = [int(v > u) for u, v in zip(from_x, from_y)]

    me = lax.axis_index("vocab")
    chip, core = me // 2, lax.rem(me, 2)
    x, y = lax.rem(chip, 2), chip // 2
    mate = {"vocab": me + 1 - 2 * core}
    x_dev = {"vocab": me + 2 - 4 * x}
    y_dev = {"vocab": me + 4 - 8 * y}
    x_chip, y_chip, d_chip = y * 2 + 1 - x, (1 - y) * 2 + x, (1 - y) * 2 + 1 - x
    mine, other = core * HALF, (1 - core) * HALF
    m, m_x, m_y, m_d = (pick_of(ms, c) for c in (chip, x_chip, y_chip, d_chip))
    cut_x, cut_y = pick_of(cuts, x_chip), pick_of(cuts, y_chip)
    shared, tail_side = pick_of(both, chip), pick_of(longer, chip)

    barrier = pltpu.get_barrier_semaphore()
    for dev in (mate, x_dev, y_dev):
        pl.semaphore_signal(barrier, inc=1, device_id=dev, device_id_type=MESH)

    pl.semaphore_wait(barrier, 3)

    def at(block, side):
        return rows.at[pl.ds(pl.multiple_of(block * BLOCK + side, HALF), HALF), :]

    def remote(src, dst, sent, received, dev):
        return pltpu.make_async_remote_copy(src_ref=src, dst_ref=dst, send_sem=sent, recv_sem=received,
                                            device_id=dev, device_id_type=MESH)

    def wait_for(n, sem):
        chunk = rows.at[pl.ds(0, n * HALF), :]
        remote(chunk, chunk, send.at[0], sem, mate).wait_recv()

    def inc_copy(i):
        return remote(part.at[pl.ds(pl.multiple_of(i * BLOCK + other, HALF), HALF), :],
                      inc.at[pl.ds(pl.multiple_of(i * HALF, HALF), HALF), :],
                      send.at[0], inc_recv.at[i], mate)

    def to_link(block, side, t, sent):
        there, dev = ((x_chip, x_dev), (y_chip, y_dev))[side]
        pair_up = pick_of(both, there)
        place = jnp.where(t < pair_up, 2 * t + side, pair_up + t)
        return remote(at(block, mine), at(pick_of(ms, there) + place, mine), send.at[sent], recv.at[place], dev)

    def pair(b):
        return remote(at(b, mine), at(b, mine), send.at[3], p_recv.at[b // WINDOW], mate)

    loop(m, lambda i: inc_copy(jnp.where(i == 0, 0, jnp.where(i == 1, m - 1, i - 1))).start())

    def merge(i):
        wait_for(1, inc_recv.at[i])
        src = pl.ds(pl.multiple_of(i * BLOCK + mine, HALF), HALF)
        rows[src, :] = part[src, :] + inc[pl.ds(pl.multiple_of(i * HALF, HALF), HALF), :]

    merge(0)
    merge(m - 1)
    to_link(0, 0, 0, 1).start()
    to_link(m - 1, 1, 0, 2).start()
    loop(m - 1, merge, 1)

    def send_own(t):
        to_link(t, 0, t, 1).start()
        to_link(m - 1 - t, 1, t, 2).start()

    loop(m, send_own, 1)
    loop(m, lambda i: pair(i).start())

    def start_value(i):
        start = jnp.where(code_ref[...] >= 0, 0.0, -jnp.inf)
        acc[pl.ds(pl.multiple_of(i * 8, 8), 8), :] = jnp.broadcast_to(start, (8, length))

    loop(acc.shape[0] // 8, start_value)
    if total < steps * WINDOW:
        rows[total * BLOCK:, :] = jnp.zeros((steps * WINDOW * BLOCK - total * BLOCK, rows.shape[1]), BF16)

    def source(p):
        paired = p < 2 * shared
        return jnp.where(paired, lax.rem(p + 2 * total, 2), tail_side), jnp.where(paired, p // 2, p - shared)

    def arrived(p):
        side, t = source(p)
        wait_for(1, recv.at[p])
        pair(m + p).start()

        @pl.when((side == 0) & (t < cut_x))
        def _():
            to_link(m + p, 1, m + t, 4).start()

        @pl.when((side == 1) & (t < m_y - cut_y))
        def _():
            to_link(m + p, 0, m + t, 4).start()

    def base(b):
        side, t = source(b - m)
        near = t < jnp.where(side == 0, m_x, m_y)
        of = jnp.where(near, jnp.where(side == 0, x_chip, y_chip), d_chip)
        i = jnp.where(side == 0, jnp.where(near, t, m_d - 1 - (t - m_x)), jnp.where(near, m_y - 1 - t, t - m_y))
        of, i = jnp.where(b < m, chip, of), jnp.where(b < m, b, i)
        return jnp.where(b < total, of * length + i * BLOCK, -length)

    width = WINDOW * BLOCK
    step_n = length // WINDOW
    left = total - (steps - 1) * WINDOW

    def window(w):
        if left == WINDOW:
            wait_for(WINDOW, p_recv.at[w])
        else:
            @pl.when(w < steps - 1)
            def _():
                wait_for(WINDOW, p_recv.at[w])

            @pl.when(w == steps - 1)
            def _():
                wait_for(left, p_recv.at[w])
        got = rows[pl.ds(pl.multiple_of(w * width, width), width), :]
        s = dot(hid[...], got, ((1,), (1,))) * INV_TEMP
        high = s.astype(BF16)
        rest = s - high.astype(F32)
        middle = rest.astype(BF16)
        split[:, :width] = high
        split[:, width:2 * width] = middle
        split[:, 2 * width:] = (rest - middle.astype(F32)).astype(BF16)
        slot = jnp.concatenate([base(w * WINDOW + k) + iota((BLOCK, step_n), 0) for k in range(WINDOW)], axis=0)

        def columns(c):
            cols = pl.ds(pl.multiple_of(c * step_n, step_n), step_n)
            hot = onehot(code_ref[:, cols] == slot)
            acc[:, cols] += dot(split[...], jnp.concatenate([hot, hot, hot], axis=0))

            @pl.when(c < 2)
            def _():
                start = (w + 1) * WINDOW - m + 2 * c
                loop(jnp.minimum(start + 2, total - m), arrived, jnp.maximum(start, 0))

        loop(WINDOW, columns)

    loop(WINDOW - m, arrived)
    loop(steps, window)

    def drain(q):
        amounts = (ms[q], ms[q], ms[q], total, cuts[q ^ 1] + ms[q ^ 2] - cuts[q ^ 2])
        for k, blocks in enumerate(amounts):
            if blocks:
                chunk = rows.at[pl.ds(0, blocks * HALF), :]
                remote(chunk, chunk, send.at[k], recv.at[0], mate).wait_send()

    if len(set(ms)) == 1 and len({cuts[q ^ 1] + ms[q ^ 2] - cuts[q ^ 2] for q in range(4)}) == 1:
        drain(0)
    else:
        for q in range(4):
            pl.when(chip == q)(functools.partial(drain, q))


def finish_kernel(s_ref, target_ref, prob_ref, logp_ref, prob, column, sem):
    rows, tile = prob.shape[0], logp_ref.shape[1]
    lane = iota((FINISH, prob.shape[1]), 1)

    def block(i):
        here = pl.ds(pl.multiple_of(i * FINISH, FINISH), FINISH)
        s = s_ref[here, :]
        top = jnp.max(s, axis=1, keepdims=True)
        e = jnp.exp(s - top)
        total = jnp.sum(e, axis=1, keepdims=True)
        prob[here, :] = e * (1.0 / total)
        picked = jnp.sum(jnp.where(lane == target_ref[here, :].astype(I32), s, 0.0), axis=1, keepdims=True)
        column[here, :] = picked - (top + jnp.log(total))
        pltpu.make_async_copy(prob.at[here, :], prob_ref.at[here, :], sem).start()

    def turn_out(i):
        value = column[pl.ds(pl.multiple_of(i * tile, tile), tile), :]
        logp_ref[pl.ds(i, 1), :] = jnp.broadcast_to(value, (tile, tile)).T[:1]

    loop(rows // FINISH, block)
    loop(rows // tile, turn_out)
    pltpu.make_async_copy(prob, prob_ref, sem).wait()


def solution(mesh):
    shards = mesh.shape["vocab"]
    chips = shards // 2
    hbm = pl.BlockSpec(memory_space=pl.ANY)
    vmem = pl.BlockSpec(memory_space=pltpu.VMEM)

    def device_step(hidden, w_head, allowed_ids, allowed_valid, target_pos):
        rows_dev, depth = hidden.shape
        length = allowed_ids.shape[0]
        most = length // BLOCK
        plans = sorted({p for p in PLANS if max(p) < most}, key=lambda p: (link_load(p), sum(p))) + [(most,) * chips]
        lanes = 128
        tile = 128
        part, code, column, which = pl.pallas_call(
            functools.partial(gather_kernel, chips, w_head.shape[0], plans),
            out_shape=(pltpu.VMEM((length, depth), BF16),
                       pltpu.VMEM((1, length), I32),
                       pltpu.VMEM((rows_dev, 1), F32),
                       jax.ShapeDtypeStruct((1,), I32)),
            in_specs=[pl.BlockSpec(memory_space=pltpu.HBM)] * 4,
            out_specs=(vmem, vmem, vmem, pl.BlockSpec(memory_space=pltpu.SMEM)),
            scratch_shapes=[
                pltpu.VMEM((length // lanes, lanes), I32),
                pltpu.VMEM((length // lanes, lanes), I32),
                pltpu.VMEM((rows_dev // tile, tile), I32),
                pltpu.VMEM((1, length), I32),
                pltpu.VMEM((length, 8), BF16),
                pltpu.VMEM((length // lanes, lanes), I32),
                pltpu.SMEM((length // lanes, lanes), I32),
                pltpu.VMEM((length, 8), F32),
                pltpu.VMEM((RING, GROUP, 8, depth), BF16),
                pltpu.SemaphoreType.DMA((3,)),
                pltpu.SemaphoreType.DMA((length // lanes,)),
                pltpu.SemaphoreType.DMA((RING,)),
            ],
            compiler_params=pltpu.CompilerParams(vmem_limit_bytes=28 * MIB),
            name="gather_rows",
        )(*(pltpu.with_memory_space_constraint(v, pltpu.HBM) for v in (allowed_ids.reshape(-1, lanes), allowed_valid.reshape(-1, lanes))), w_head.reshape(-1, 8, depth),
          pltpu.with_memory_space_constraint(target_pos.reshape(-1, tile), pltpu.HBM))

        finish = pl.pallas_call(
            finish_kernel,
            out_shape=(jax.ShapeDtypeStruct((rows_dev, length), F32),
                       jax.ShapeDtypeStruct((rows_dev // tile, tile), F32)),
            in_specs=[vmem, vmem],
            out_specs=(hbm, vmem),
            scratch_shapes=[pltpu.VMEM((rows_dev, length), F32), pltpu.VMEM((rows_dev, 1), F32), pltpu.SemaphoreType.DMA],
            compiler_params=pltpu.CompilerParams(vmem_limit_bytes=16 * MIB),
            name="finish",
        )

        def serve(ms, cid):
            total, steps = sum(ms), -(-sum(ms) // WINDOW)
            dma = lambda n: pltpu.SemaphoreType.DMA((n,))
            exchange = pl.pallas_call(
                functools.partial(exchange_kernel, ms, length),
                out_shape=pltpu.VMEM((rows_dev, length), F32),
                in_specs=[vmem, vmem, vmem],
                out_specs=vmem,
                scratch_shapes=[
                    pltpu.VMEM((max(ms) * HALF, depth), BF16),
                    pltpu.VMEM((steps * WINDOW * BLOCK, depth), BF16),
                    pltpu.VMEM((rows_dev, 3 * WINDOW * BLOCK), BF16),
                    dma(5), dma(max(ms)), dma(total - min(ms)), dma(steps),
                ],
                compiler_params=pltpu.CompilerParams(collective_id=cid, has_side_effects=True,
                                                     vmem_limit_bytes=(8 + total // 5 + max(ms) // 10) * MIB),
                name="exchange_" + "_".join(map(str, ms)),
            )
            return lambda hidden, part, code, target: finish(exchange(hidden, part, code), target)

        probs, logp = lax.switch(which[0], [serve(ms, k) for k, ms in enumerate(plans)],
                                 hidden, part, code, column)
        return probs, logp.reshape(rows_dev)

    row_spec = P(("rep", "vocab"))
    mat_spec = P(("rep", "vocab"), None)
    return jax.shard_map(device_step, mesh=mesh, in_specs=(mat_spec, P("vocab", None), P("rep"), P("rep"), row_spec),
                         out_specs=(mat_spec, row_spec), check_vma=False)


PLANS = [(k,) * 4 for k in (6, 7, 8, 9, 10, 11, 12, 14, 16)]
for heavy, others in ((15, 8), (11, 7), (10, 6)):
    PLANS += [tuple(heavy if c == h else others for c in range(4)) for h in range(4)]
```

```python
import functools

import jax
import jax.numpy as jnp
from jax import lax
from jax.experimental import pallas as pl
from jax.experimental.pallas import tpu as pltpu
from jax.sharding import PartitionSpec as P

INV_TEMP = 1.25
BLOCK = 64
HALF = BLOCK // 2
WINDOW = 4
GROUP = 128
SELECT = 32
RING = 5
FINISH = 128
MIB = 2 ** 20
MESH = pl.DeviceIdType.MESH
BF16, F32, I32 = jnp.bfloat16, jnp.float32, jnp.int32


def iota(shape, dim):
    return lax.broadcasted_iota(I32, shape, dim)


def onehot(mask):
    return jnp.where(mask, 1.0, 0.0).astype(BF16)


def dot(a, b, dims=((1,), (0,))):
    return lax.dot_general(a, b, (dims, ((), ())), preferred_element_type=F32)


def loop(n, f, start=0):
    def body(i, carry):
        f(i)
        return carry
    lax.fori_loop(start, n, body, 0)


def pick_of(table, index):
    value = jnp.int32(table[0])
    for k in range(1, len(table)):
        if table[k] != table[0]:
            value = jnp.where(index == k, table[k], value)
    return value


def gather_kernel(chips, vocab_local, plans, ids_hbm, valid_hbm, w_ref, target_hbm, part_ref, code_ref, column_ref, cap_ref,
                  ids_ref, valid_ref, target_ref, id_row, turned, table, table_s, pick, stage, load_sem, table_sem, in_sem):
    me = lax.axis_index("vocab")
    chip, devices = me // 2, 2 * chips
    loads = [pltpu.make_async_copy(ids_hbm, ids_ref, load_sem.at[0]),
             pltpu.make_async_copy(valid_hbm, valid_ref, load_sem.at[1]),
             pltpu.make_async_copy(target_hbm, target_ref, load_sem.at[2])]
    for load in loads:
        load.start()
    for load in loads:
        load.wait()
    rows, lanes = ids_ref.shape
    length = rows * lanes
    ids = ids_ref[...]
    valid = valid_ref[...] > 0
    owner = jnp.zeros_like(ids)
    for d in range(1, devices):
        owner += jnp.where(ids >= vocab_local * d, 1, 0)
    keep = [valid & (owner == d) for d in range(devices)]
    marks = jnp.concatenate([jnp.where(k, 1.0, 0.0) for k in keep], axis=0).astype(BF16)
    inside = dot(marks, onehot(iota((lanes, lanes), 0) <= iota((lanes, lanes), 1)))
    total = dot(marks, jnp.ones((lanes, lanes), BF16))
    n = devices * rows
    r, c_ = iota((n, n), 0), iota((n, n), 1)
    before = dot(onehot((r // (2 * rows) == c_ // (2 * rows)) & (c_ < r)), total.astype(BF16))
    rank = inside + before - 1.0
    code = jnp.full((rows, lanes), -1, I32)
    for d in range(devices):
        code = jnp.where(keep[d], d // 2 * length + rank[d * rows:(d + 1) * rows].astype(I32), code)
    own_id = jnp.where(valid, ids - me * vocab_local, -1)
    for k in range(rows):
        code_ref[:, k * lanes:(k + 1) * lanes] = code[k:k + 1]
        id_row[:, k * lanes:(k + 1) * lanes] = own_id[k:k + 1]
    after = before + total
    ours = iota((n, lanes), 0) // rows == me
    low = jnp.min(jnp.where(ours, before, 1e6)).astype(I32)
    high = jnp.max(jnp.where(ours, after, 0.0)).astype(I32)
    counts = [jnp.max(after[c * 2 * rows:(c + 1) * 2 * rows]).astype(I32) for c in range(chips)]
    which = jnp.int32(len(plans) - 1)
    cap = pick_of(plans[-1], chip)
    for v in range(len(plans) - 2, -1, -1):
        fits = counts[0] <= plans[v][0] * BLOCK
        for c in range(1, chips):
            fits &= counts[c] <= plans[v][c] * BLOCK
        which = jnp.where(fits, v, which)
        cap = jnp.where(fits, pick_of(plans[v], chip), cap)
    cap_ref[0] = which

    groups = (cap * BLOCK + GROUP - 1) // GROUP
    first, last = low // GROUP, (high + GROUP - 1) // GROUP
    last = jnp.where(high > low, last, first)

    local = id_row[...]
    owned = (local >= 0) & (local < vocab_local)
    tile = local >> 3
    sub = iota((8, length), 0)
    digits = jnp.where(sub == 0, tile >> 6, jnp.where(sub == 1, tile & 63, jnp.where(sub == 2, local & 7, 1)))
    digits = jnp.where(owned & (sub < 4), digits, 0).astype(F32)

    for k in range(rows):
        turned[k * lanes:(k + 1) * lanes, :] = digits[:, k * lanes:(k + 1) * lanes].T.astype(BF16)

    def fill(kb):
        hot = onehot(code_ref[...] == chip * length + kb * lanes + iota((lanes, length), 0))
        found = dot(hot, turned[...])
        pick[pl.ds(pl.multiple_of(kb * lanes, lanes), lanes), :] = found
        across = found.T
        spread = lax.rem(kb * lanes + iota((1, lanes), 1), w_ref.shape[0])
        table[pl.ds(kb, 1), :] = jnp.where(across[3:4] > 0.5, (across[0:1] * 64.0 + across[1:2]).astype(I32), spread)
        to_smem(kb).start()

    def to_smem(kb):
        return pltpu.make_async_copy(table.at[pl.ds(kb, 1), :], table_s.at[pl.ds(kb, 1), :], table_sem.at[kb])

    def each_run(g, act):
        for k in range(GROUP // SELECT):
            begin = g * GROUP + k * SELECT
            pl.when((begin < high) & (begin + SELECT > low))(functools.partial(act, k))

    def issue(g):
        slot = lax.rem(g, RING)
        to_smem(g).wait()

        def start(k):
            for i in range(k * SELECT, (k + 1) * SELECT):
                pltpu.make_async_copy(w_ref.at[table_s[g, i]], stage.at[slot, i], in_sem.at[slot]).start()

        each_run(g, start)

    def fill_and_issue(g):
        pl.when(g < last)(functools.partial(fill, g))
        pl.when((g > first) & (g <= first + RING))(functools.partial(issue, g - 1))

    loop(jnp.where(last > first, last + 1, first), fill_and_issue, first)

    tile = target_ref.shape[1]
    for k in range(target_ref.shape[0]):
        target = jnp.broadcast_to(target_ref[k:k + 1, :].astype(F32), (tile, tile)).T
        column_ref[k * tile:(k + 1) * tile, :] = target[:, :1]

    def blank(g):
        part_ref[pl.ds(pl.multiple_of(g * GROUP, GROUP), GROUP), :] = jnp.zeros((GROUP, part_ref.shape[1]), BF16)

    loop(first, blank)
    loop(groups, blank, last)

    def step(g):
        slot = lax.rem(g, RING)

        def finished(k):
            pltpu.make_async_copy(w_ref.at[pl.ds(0, SELECT)], stage.at[slot, pl.ds(0, SELECT)], in_sem.at[slot]).wait()

        each_run(g, finished)
        for k in range(GROUP // SELECT):
            here = pl.ds(pl.multiple_of(g * GROUP + k * SELECT, SELECT), SELECT)
            found = pick[here, :]
            owned = found[:, 3:4] > 0.5
            row = jnp.where(owned, found[:, 2:3], -4096.0).astype(I32)
            sel = onehot(iota((SELECT, 8 * SELECT), 1) - 8 * iota((SELECT, 8 * SELECT), 0) == row)
            tiles = stage[slot, k * SELECT:(k + 1) * SELECT].reshape(8 * SELECT, part_ref.shape[1])
            part_ref[here, :] = jnp.where(owned, dot(sel, tiles), 0.0).astype(BF16)

        @pl.when(g + RING < last)
        def _():
            issue(g + RING)

    loop(last, step, first)


def cuts_of(ms):
    cuts = []
    for s in range(4):
        through_y, through_x = ms[s ^ 2], ms[s ^ 1]
        cuts.append(min(max((through_y + ms[s] - through_x + 1) // 2, 0), ms[s]))
    return cuts


def link_load(ms):
    cuts = cuts_of(ms)
    return max(max(ms[s ^ 2] + ms[s] - cuts[s], ms[s ^ 1] + cuts[s]) for s in range(4))


def exchange_kernel(ms, length, hid, part, code_ref, acc, inc, rows, split, send, inc_recv, recv, p_recv):
    cuts, total = cuts_of(ms), sum(ms)
    steps = -(-total // WINDOW)
    from_x = [ms[r ^ 1] + ms[r ^ 3] - cuts[r ^ 3] for r in range(4)]
    from_y = [ms[r ^ 2] + cuts[r ^ 3] for r in range(4)]
    both = [min(u, v) for u, v in zip(from_x, from_y)]
    longer = [int(v > u) for u, v in zip(from_x, from_y)]

    me = lax.axis_index("vocab")
    chip, core = me // 2, lax.rem(me, 2)
    x, y = lax.rem(chip, 2), chip // 2
    mate = {"vocab": me + 1 - 2 * core}
    x_dev = {"vocab": me + 2 - 4 * x}
    y_dev = {"vocab": me + 4 - 8 * y}
    x_chip, y_chip, d_chip = y * 2 + 1 - x, (1 - y) * 2 + x, (1 - y) * 2 + 1 - x
    mine, other = core * HALF, (1 - core) * HALF
    m, m_x, m_y, m_d = (pick_of(ms, c) for c in (chip, x_chip, y_chip, d_chip))
    cut_x, cut_y = pick_of(cuts, x_chip), pick_of(cuts, y_chip)
    shared, tail_side = pick_of(both, chip), pick_of(longer, chip)

    barrier = pltpu.get_barrier_semaphore()
    for dev in (mate, x_dev, y_dev):
        pl.semaphore_signal(barrier, inc=1, device_id=dev, device_id_type=MESH)

    pl.semaphore_wait(barrier, 3)

    def at(block, side):
        return rows.at[pl.ds(pl.multiple_of(block * BLOCK + side, HALF), HALF), :]

    def remote(src, dst, sent, received, dev):
        return pltpu.make_async_remote_copy(src_ref=src, dst_ref=dst, send_sem=sent, recv_sem=received,
                                            device_id=dev, device_id_type=MESH)

    def wait_for(n, sem):
        chunk = rows.at[pl.ds(0, n * HALF), :]
        remote(chunk, chunk, send.at[0], sem, mate).wait_recv()

    def inc_copy(i):
        return remote(part.at[pl.ds(pl.multiple_of(i * BLOCK + other, HALF), HALF), :],
                      inc.at[pl.ds(pl.multiple_of(i * HALF, HALF), HALF), :],
                      send.at[0], inc_recv.at[i], mate)

    def to_link(block, side, t, sent):
        there, dev = ((x_chip, x_dev), (y_chip, y_dev))[side]
        pair_up = pick_of(both, there)
        place = jnp.where(t < pair_up, 2 * t + side, pair_up + t)
        return remote(at(block, mine), at(pick_of(ms, there) + place, mine), send.at[sent], recv.at[place], dev)

    def pair(b):
        return remote(at(b, mine), at(b, mine), send.at[3], p_recv.at[b // WINDOW], mate)

    loop(m, lambda i: inc_copy(jnp.where(i == 0, 0, jnp.where(i == 1, m - 1, i - 1))).start())

    def merge(i):
        wait_for(1, inc_recv.at[i])
        src = pl.ds(pl.multiple_of(i * BLOCK + mine, HALF), HALF)
        rows[src, :] = part[src, :] + inc[pl.ds(pl.multiple_of(i * HALF, HALF), HALF), :]

    merge(0)
    merge(m - 1)
    to_link(0, 0, 0, 1).start()
    to_link(m - 1, 1, 0, 2).start()
    loop(m - 1, merge, 1)

    def send_own(t):
        to_link(t, 0, t, 1).start()
        to_link(m - 1 - t, 1, t, 2).start()

    loop(m, send_own, 1)
    loop(m, lambda i: pair(i).start())

    def start_value(i):
        start = jnp.where(code_ref[...] >= 0, 0.0, -jnp.inf)
        acc[pl.ds(pl.multiple_of(i * 8, 8), 8), :] = jnp.broadcast_to(start, (8, length))

    loop(acc.shape[0] // 8, start_value)
    if total < steps * WINDOW:
        rows[total * BLOCK:, :] = jnp.zeros((steps * WINDOW * BLOCK - total * BLOCK, rows.shape[1]), BF16)

    def source(p):
        paired = p < 2 * shared
        return jnp.where(paired, lax.rem(p + 2 * total, 2), tail_side), jnp.where(paired, p // 2, p - shared)

    def arrived(p):
        side, t = source(p)
        wait_for(1, recv.at[p])
        pair(m + p).start()

        @pl.when((side == 0) & (t < cut_x))
        def _():
            to_link(m + p, 1, m + t, 4).start()

        @pl.when((side == 1) & (t < m_y - cut_y))
        def _():
            to_link(m + p, 0, m + t, 4).start()

    def base(b):
        side, t = source(b - m)
        near = t < jnp.where(side == 0, m_x, m_y)
        of = jnp.where(near, jnp.where(side == 0, x_chip, y_chip), d_chip)
        i = jnp.where(side == 0, jnp.where(near, t, m_d - 1 - (t - m_x)), jnp.where(near, m_y - 1 - t, t - m_y))
        of, i = jnp.where(b < m, chip, of), jnp.where(b < m, b, i)
        return jnp.where(b < total, of * length + i * BLOCK, -length)

    width = WINDOW * BLOCK
    step_n = length // WINDOW
    left = total - (steps - 1) * WINDOW

    def window(w):
        if left == WINDOW:
            wait_for(WINDOW, p_recv.at[w])
        else:
            @pl.when(w < steps - 1)
            def _():
                wait_for(WINDOW, p_recv.at[w])

            @pl.when(w == steps - 1)
            def _():
                wait_for(left, p_recv.at[w])
        got = rows[pl.ds(pl.multiple_of(w * width, width), width), :]
        s = dot(hid[...], got, ((1,), (1,))) * INV_TEMP
        high = s.astype(BF16)
        rest = s - high.astype(F32)
        middle = rest.astype(BF16)
        split[:, :width] = high
        split[:, width:2 * width] = middle
        split[:, 2 * width:] = (rest - middle.astype(F32)).astype(BF16)
        slot = jnp.concatenate([base(w * WINDOW + k) + iota((BLOCK, step_n), 0) for k in range(WINDOW)], axis=0)

        def columns(c):
            cols = pl.ds(pl.multiple_of(c * step_n, step_n), step_n)
            hot = onehot(code_ref[:, cols] == slot)
            acc[:, cols] += dot(split[...], jnp.concatenate([hot, hot, hot], axis=0))

            @pl.when(c < 2)
            def _():
                start = (w + 1) * WINDOW - m + 2 * c
                loop(jnp.minimum(start + 2, total - m), arrived, jnp.maximum(start, 0))

        loop(WINDOW, columns)

    loop(WINDOW - m, arrived)
    loop(steps, window)

    def drain(q):
        amounts = (ms[q], ms[q], ms[q], total, cuts[q ^ 1] + ms[q ^ 2] - cuts[q ^ 2])
        for k, blocks in enumerate(amounts):
            if blocks:
                chunk = rows.at[pl.ds(0, blocks * HALF), :]
                remote(chunk, chunk, send.at[k], recv.at[0], mate).wait_send()

    if len(set(ms)) == 1 and len({cuts[q ^ 1] + ms[q ^ 2] - cuts[q ^ 2] for q in range(4)}) == 1:
        drain(0)
    else:
        for q in range(4):
            pl.when(chip == q)(functools.partial(drain, q))


def finish_kernel(s_ref, target_ref, prob_ref, logp_ref, prob, column, sem):
    rows, tile = prob.shape[0], logp_ref.shape[1]
    lane = iota((FINISH, prob.shape[1]), 1)

    def block(i):
        here = pl.ds(pl.multiple_of(i * FINISH, FINISH), FINISH)
        s = s_ref[here, :]
        top = jnp.max(s, axis=1, keepdims=True)
        e = jnp.exp(s - top)
        total = jnp.sum(e, axis=1, keepdims=True)
        prob[here, :] = e * (1.0 / total)
        picked = jnp.sum(jnp.where(lane == target_ref[here, :].astype(I32), s, 0.0), axis=1, keepdims=True)
        column[here, :] = picked - (top + jnp.log(total))
        pltpu.make_async_copy(prob.at[here, :], prob_ref.at[here, :], sem).start()

    def turn_out(i):
        value = column[pl.ds(pl.multiple_of(i * tile, tile), tile), :]
        logp_ref[pl.ds(i, 1), :] = jnp.broadcast_to(value, (tile, tile)).T[:1]

    loop(rows // FINISH, block)
    loop(rows // tile, turn_out)
    pltpu.make_async_copy(prob, prob_ref, sem).wait()


def solution(mesh):
    shards = mesh.shape["vocab"]
    chips = shards // 2
    hbm = pl.BlockSpec(memory_space=pl.ANY)
    vmem = pl.BlockSpec(memory_space=pltpu.VMEM)

    def device_step(hidden, w_head, allowed_ids, allowed_valid, target_pos):
        rows_dev, depth = hidden.shape
        length = allowed_ids.shape[0]
        most = length // BLOCK
        plans = sorted({p for p in PLANS if max(p) < most}, key=lambda p: (link_load(p), sum(p))) + [(most,) * chips]
        lanes = 128
        tile = 128
        part, code, column, which = pl.pallas_call(
            functools.partial(gather_kernel, chips, w_head.shape[0], plans),
            out_shape=(pltpu.VMEM((length, depth), BF16),
                       pltpu.VMEM((1, length), I32),
                       pltpu.VMEM((rows_dev, 1), F32),
                       jax.ShapeDtypeStruct((1,), I32)),
            in_specs=[pl.BlockSpec(memory_space=pltpu.HBM)] * 4,
            out_specs=(vmem, vmem, vmem, pl.BlockSpec(memory_space=pltpu.SMEM)),
            scratch_shapes=[
                pltpu.VMEM((length // lanes, lanes), I32),
                pltpu.VMEM((length // lanes, lanes), I32),
                pltpu.VMEM((rows_dev // tile, tile), I32),
                pltpu.VMEM((1, length), I32),
                pltpu.VMEM((length, 8), BF16),
                pltpu.VMEM((length // lanes, lanes), I32),
                pltpu.SMEM((length // lanes, lanes), I32),
                pltpu.VMEM((length, 8), F32),
                pltpu.VMEM((RING, GROUP, 8, depth), BF16),
                pltpu.SemaphoreType.DMA((3,)),
                pltpu.SemaphoreType.DMA((length // lanes,)),
                pltpu.SemaphoreType.DMA((RING,)),
            ],
            compiler_params=pltpu.CompilerParams(vmem_limit_bytes=28 * MIB),
            name="gather_rows",
        )(*(pltpu.with_memory_space_constraint(v, pltpu.HBM) for v in (allowed_ids.reshape(-1, lanes), allowed_valid.reshape(-1, lanes))), w_head.reshape(-1, 8, depth),
          pltpu.with_memory_space_constraint(target_pos.reshape(-1, tile), pltpu.HBM))

        finish = pl.pallas_call(
            finish_kernel,
            out_shape=(jax.ShapeDtypeStruct((rows_dev, length), F32),
                       jax.ShapeDtypeStruct((rows_dev // tile, tile), F32)),
            in_specs=[vmem, vmem],
            out_specs=(hbm, vmem),
            scratch_shapes=[pltpu.VMEM((rows_dev, length), F32), pltpu.VMEM((rows_dev, 1), F32), pltpu.SemaphoreType.DMA],
            compiler_params=pltpu.CompilerParams(vmem_limit_bytes=16 * MIB),
            name="finish",
        )

        def serve(ms, cid):
            total, steps = sum(ms), -(-sum(ms) // WINDOW)
            dma = lambda n: pltpu.SemaphoreType.DMA((n,))
            exchange = pl.pallas_call(
                functools.partial(exchange_kernel, ms, length),
                out_shape=pltpu.VMEM((rows_dev, length), F32),
                in_specs=[vmem, vmem, vmem],
                out_specs=vmem,
                scratch_shapes=[
                    pltpu.VMEM((max(ms) * HALF, depth), BF16),
                    pltpu.VMEM((steps * WINDOW * BLOCK, depth), BF16),
                    pltpu.VMEM((rows_dev, 3 * WINDOW * BLOCK), BF16),
                    dma(5), dma(max(ms)), dma(total - min(ms)), dma(steps),
                ],
                compiler_params=pltpu.CompilerParams(collective_id=cid, has_side_effects=True,
                                                     vmem_limit_bytes=(8 + total // 5 + max(ms) // 10) * MIB),
                name="exchange_" + "_".join(map(str, ms)),
            )
            return lambda hidden, part, code, target: finish(exchange(hidden, part, code), target)

        probs, logp = lax.switch(which[0], [serve(ms, k) for k, ms in enumerate(plans)],
                                 hidden, part, code, column)
        return probs, logp.reshape(rows_dev)

    row_spec = P(("rep", "vocab"))
    mat_spec = P(("rep", "vocab"), None)
    return jax.shard_map(device_step, mesh=mesh, in_specs=(mat_spec, P("vocab", None), P("rep"), P("rep"), row_spec),
                         out_specs=(mat_spec, row_spec), check_vma=False)


PLANS = [(k,) * 4 for k in (6, 8, 9, 10, 11, 12, 14, 16)]
for heavy, others in ((14, 8), (12, 7), (10, 6)):
    PLANS += [tuple(heavy if c == h else others for c in range(4)) for h in range(4)]
```

```python
import functools

import jax
import jax.numpy as jnp
from jax import lax
from jax.experimental import pallas as pl
from jax.experimental.pallas import tpu as pltpu
from jax.sharding import PartitionSpec as P

INV_TEMP = 1.25
BLOCK = 64
HALF = BLOCK // 2
WINDOW = 4
GROUP = 128
SELECT = 32
RING = 5
FINISH = 128
MIB = 2 ** 20
MESH = pl.DeviceIdType.MESH
BF16, F32, I32 = jnp.bfloat16, jnp.float32, jnp.int32


def iota(shape, dim):
    return lax.broadcasted_iota(I32, shape, dim)


def onehot(mask):
    return jnp.where(mask, 1.0, 0.0).astype(BF16)


def dot(a, b, dims=((1,), (0,))):
    return lax.dot_general(a, b, (dims, ((), ())), preferred_element_type=F32)


def loop(n, f, start=0):
    def body(i, carry):
        f(i)
        return carry
    lax.fori_loop(start, n, body, 0)


def pick_of(table, index):
    value = jnp.int32(table[0])
    for k in range(1, len(table)):
        if table[k] != table[0]:
            value = jnp.where(index == k, table[k], value)
    return value


def gather_kernel(chips, vocab_local, plans, ids_hbm, valid_hbm, w_ref, target_hbm, part_ref, code_ref, column_ref, cap_ref,
                  ids_ref, valid_ref, target_ref, id_row, turned, table, table_s, pick, stage, load_sem, table_sem, in_sem):
    me = lax.axis_index("vocab")
    chip, devices = me // 2, 2 * chips
    loads = [pltpu.make_async_copy(ids_hbm, ids_ref, load_sem.at[0]),
             pltpu.make_async_copy(valid_hbm, valid_ref, load_sem.at[1]),
             pltpu.make_async_copy(target_hbm, target_ref, load_sem.at[2])]
    for load in loads:
        load.start()
    for load in loads:
        load.wait()
    rows, lanes = ids_ref.shape
    length = rows * lanes
    ids = ids_ref[...]
    valid = valid_ref[...] > 0
    owner = jnp.zeros_like(ids)
    for d in range(1, devices):
        owner += jnp.where(ids >= vocab_local * d, 1, 0)
    keep = [valid & (owner == d) for d in range(devices)]
    marks = jnp.concatenate([jnp.where(k, 1.0, 0.0) for k in keep], axis=0).astype(BF16)
    inside = dot(marks, onehot(iota((lanes, lanes), 0) <= iota((lanes, lanes), 1)))
    total = dot(marks, jnp.ones((lanes, lanes), BF16))
    n = devices * rows
    r, c_ = iota((n, n), 0), iota((n, n), 1)
    before = dot(onehot((r // (2 * rows) == c_ // (2 * rows)) & (c_ < r)), total.astype(BF16))
    rank = inside + before - 1.0
    code = jnp.full((rows, lanes), -1, I32)
    for d in range(devices):
        code = jnp.where(keep[d], d // 2 * length + rank[d * rows:(d + 1) * rows].astype(I32), code)
    own_id = jnp.where(valid, ids - me * vocab_local, -1)
    for k in range(rows):
        code_ref[:, k * lanes:(k + 1) * lanes] = code[k:k + 1]
        id_row[:, k * lanes:(k + 1) * lanes] = own_id[k:k + 1]
    after = before + total
    ours = iota((n, lanes), 0) // rows == me
    low = jnp.min(jnp.where(ours, before, 1e6)).astype(I32)
    high = jnp.max(jnp.where(ours, after, 0.0)).astype(I32)
    first, last = low // GROUP, (high + GROUP - 1) // GROUP
    last = jnp.where(high > low, last, first)

    local = id_row[...]
    owned = (local >= 0) & (local < vocab_local)
    tile = local >> 3
    sub = iota((8, length), 0)
    digits = jnp.where(sub == 0, tile >> 6, jnp.where(sub == 1, tile & 63, jnp.where(sub == 2, local & 7, 1)))
    digits = jnp.where(owned & (sub < 4), digits, 0).astype(F32)

    for k in range(rows):
        turned[k * lanes:(k + 1) * lanes, :] = digits[:, k * lanes:(k + 1) * lanes].T.astype(BF16)

    def fill(kb):
        hot = onehot(code_ref[...] == chip * length + kb * lanes + iota((lanes, length), 0))
        found = dot(hot, turned[...])
        pick[pl.ds(pl.multiple_of(kb * lanes, lanes), lanes), :] = found
        across = found.T
        spread = lax.rem(kb * lanes + iota((1, lanes), 1), w_ref.shape[0])
        table[pl.ds(kb, 1), :] = jnp.where(across[3:4] > 0.5, (across[0:1] * 64.0 + across[1:2]).astype(I32), spread)
        to_smem(kb).start()

    def to_smem(kb):
        return pltpu.make_async_copy(table.at[pl.ds(kb, 1), :], table_s.at[pl.ds(kb, 1), :], table_sem.at[kb])

    def each_run(g, act):
        for k in range(GROUP // SELECT):
            begin = g * GROUP + k * SELECT
            pl.when((begin < high) & (begin + SELECT > low))(functools.partial(act, k))

    def issue(g):
        slot = lax.rem(g, RING)
        to_smem(g).wait()

        def start(k):
            for i in range(k * SELECT, (k + 1) * SELECT):
                pltpu.make_async_copy(w_ref.at[table_s[g, i]], stage.at[slot, i], in_sem.at[slot]).start()

        each_run(g, start)

    def fill_and_issue(g):
        pl.when(g < last)(functools.partial(fill, g))
        pl.when((g > first) & (g <= first + RING))(functools.partial(issue, g - 1))

    loop(jnp.where(last > first, last + 1, first), fill_and_issue, first)

    counts = [jnp.max(after[c * 2 * rows:(c + 1) * 2 * rows]).astype(I32) for c in range(chips)]
    which = jnp.int32(len(plans) - 1)
    cap = pick_of(plans[-1], chip)
    for v in range(len(plans) - 2, -1, -1):
        fits = counts[0] <= plans[v][0] * BLOCK
        for c in range(1, chips):
            fits &= counts[c] <= plans[v][c] * BLOCK
        which = jnp.where(fits, v, which)
        cap = jnp.where(fits, pick_of(plans[v], chip), cap)
    cap_ref[0] = which

    groups = (cap * BLOCK + GROUP - 1) // GROUP
    tile = target_ref.shape[1]
    for k in range(target_ref.shape[0]):
        target = jnp.broadcast_to(target_ref[k:k + 1, :].astype(F32), (tile, tile)).T
        column_ref[k * tile:(k + 1) * tile, :] = target[:, :1]

    def blank(g):
        part_ref[pl.ds(pl.multiple_of(g * GROUP, GROUP), GROUP), :] = jnp.zeros((GROUP, part_ref.shape[1]), BF16)

    loop(first, blank)
    loop(groups, blank, last)

    def step(g):
        slot = lax.rem(g, RING)

        def finished(k):
            pltpu.make_async_copy(w_ref.at[pl.ds(0, SELECT)], stage.at[slot, pl.ds(0, SELECT)], in_sem.at[slot]).wait()

        each_run(g, finished)
        for k in range(GROUP // SELECT):
            here = pl.ds(pl.multiple_of(g * GROUP + k * SELECT, SELECT), SELECT)
            found = pick[here, :]
            owned = found[:, 3:4] > 0.5
            row = jnp.where(owned, found[:, 2:3], -4096.0).astype(I32)
            sel = onehot(iota((SELECT, 8 * SELECT), 1) - 8 * iota((SELECT, 8 * SELECT), 0) == row)
            tiles = stage[slot, k * SELECT:(k + 1) * SELECT].reshape(8 * SELECT, part_ref.shape[1])
            part_ref[here, :] = jnp.where(owned, dot(sel, tiles), 0.0).astype(BF16)

        @pl.when(g + RING < last)
        def _():
            issue(g + RING)

    loop(last, step, first)


def cuts_of(ms):
    cuts = []
    for s in range(4):
        through_y, through_x = ms[s ^ 2], ms[s ^ 1]
        cuts.append(min(max((through_y + ms[s] - through_x + 1) // 2, 0), ms[s]))
    return cuts


def link_load(ms):
    cuts = cuts_of(ms)
    return max(max(ms[s ^ 2] + ms[s] - cuts[s], ms[s ^ 1] + cuts[s]) for s in range(4))


def exchange_kernel(ms, length, hid, part, code_ref, acc, inc, rows, split, send, inc_recv, recv, p_recv):
    cuts, total = cuts_of(ms), sum(ms)
    steps = -(-total // WINDOW)
    from_x = [ms[r ^ 1] + ms[r ^ 3] - cuts[r ^ 3] for r in range(4)]
    from_y = [ms[r ^ 2] + cuts[r ^ 3] for r in range(4)]
    both = [min(u, v) for u, v in zip(from_x, from_y)]
    longer = [int(v > u) for u, v in zip(from_x, from_y)]

    me = lax.axis_index("vocab")
    chip, core = me // 2, lax.rem(me, 2)
    x, y = lax.rem(chip, 2), chip // 2
    mate = {"vocab": me + 1 - 2 * core}
    x_dev = {"vocab": me + 2 - 4 * x}
    y_dev = {"vocab": me + 4 - 8 * y}
    x_chip, y_chip, d_chip = y * 2 + 1 - x, (1 - y) * 2 + x, (1 - y) * 2 + 1 - x
    mine, other = core * HALF, (1 - core) * HALF
    m, m_x, m_y, m_d = (pick_of(ms, c) for c in (chip, x_chip, y_chip, d_chip))
    cut_x, cut_y = pick_of(cuts, x_chip), pick_of(cuts, y_chip)
    shared, tail_side = pick_of(both, chip), pick_of(longer, chip)

    barrier = pltpu.get_barrier_semaphore()
    for dev in (mate, x_dev, y_dev):
        pl.semaphore_signal(barrier, inc=1, device_id=dev, device_id_type=MESH)

    pl.semaphore_wait(barrier, 3)

    def at(block, side):
        return rows.at[pl.ds(pl.multiple_of(block * BLOCK + side, HALF), HALF), :]

    def remote(src, dst, sent, received, dev):
        return pltpu.make_async_remote_copy(src_ref=src, dst_ref=dst, send_sem=sent, recv_sem=received,
                                            device_id=dev, device_id_type=MESH)

    def wait_for(n, sem):
        chunk = rows.at[pl.ds(0, n * HALF), :]
        remote(chunk, chunk, send.at[0], sem, mate).wait_recv()

    def inc_copy(i):
        return remote(part.at[pl.ds(pl.multiple_of(i * BLOCK + other, HALF), HALF), :],
                      inc.at[pl.ds(pl.multiple_of(i * HALF, HALF), HALF), :],
                      send.at[0], inc_recv.at[i], mate)

    def to_link(block, side, t, sent):
        there, dev = ((x_chip, x_dev), (y_chip, y_dev))[side]
        pair_up = pick_of(both, there)
        place = jnp.where(t < pair_up, 2 * t + side, pair_up + t)
        return remote(at(block, mine), at(pick_of(ms, there) + place, mine), send.at[sent], recv.at[place], dev)

    def pair(b):
        return remote(at(b, mine), at(b, mine), send.at[3], p_recv.at[b // WINDOW], mate)

    loop(m, lambda i: inc_copy(jnp.where(i == 0, 0, jnp.where(i == 1, m - 1, i - 1))).start())

    def merge(i):
        wait_for(1, inc_recv.at[i])
        src = pl.ds(pl.multiple_of(i * BLOCK + mine, HALF), HALF)
        rows[src, :] = part[src, :] + inc[pl.ds(pl.multiple_of(i * HALF, HALF), HALF), :]

    merge(0)
    merge(m - 1)
    to_link(0, 0, 0, 1).start()
    to_link(m - 1, 1, 0, 2).start()
    loop(m - 1, merge, 1)

    def send_own(t):
        to_link(t, 0, t, 1).start()
        to_link(m - 1 - t, 1, t, 2).start()

    loop(m, send_own, 1)
    loop(m, lambda i: pair(i).start())

    def start_value(i):
        start = jnp.where(code_ref[...] >= 0, 0.0, -jnp.inf)
        acc[pl.ds(pl.multiple_of(i * 8, 8), 8), :] = jnp.broadcast_to(start, (8, length))

    loop(acc.shape[0] // 8, start_value)
    if total < steps * WINDOW:
        rows[total * BLOCK:, :] = jnp.zeros((steps * WINDOW * BLOCK - total * BLOCK, rows.shape[1]), BF16)

    def source(p):
        paired = p < 2 * shared
        return jnp.where(paired, lax.rem(p + 2 * total, 2), tail_side), jnp.where(paired, p // 2, p - shared)

    def arrived(p):
        side, t = source(p)
        wait_for(1, recv.at[p])
        pair(m + p).start()

        @pl.when((side == 0) & (t < cut_x))
        def _():
            to_link(m + p, 1, m + t, 4).start()

        @pl.when((side == 1) & (t < m_y - cut_y))
        def _():
            to_link(m + p, 0, m + t, 4).start()

    def base(b):
        side, t = source(b - m)
        near = t < jnp.where(side == 0, m_x, m_y)
        of = jnp.where(near, jnp.where(side == 0, x_chip, y_chip), d_chip)
        i = jnp.where(side == 0, jnp.where(near, t, m_d - 1 - (t - m_x)), jnp.where(near, m_y - 1 - t, t - m_y))
        of, i = jnp.where(b < m, chip, of), jnp.where(b < m, b, i)
        return jnp.where(b < total, of * length + i * BLOCK, -length)

    width = WINDOW * BLOCK
    step_n = length // WINDOW
    left = total - (steps - 1) * WINDOW

    def window(w):
        if left == WINDOW:
            wait_for(WINDOW, p_recv.at[w])
        else:
            @pl.when(w < steps - 1)
            def _():
                wait_for(WINDOW, p_recv.at[w])

            @pl.when(w == steps - 1)
            def _():
                wait_for(left, p_recv.at[w])
        got = rows[pl.ds(pl.multiple_of(w * width, width), width), :]
        s = dot(hid[...], got, ((1,), (1,))) * INV_TEMP
        high = s.astype(BF16)
        rest = s - high.astype(F32)
        middle = rest.astype(BF16)
        split[:, :width] = high
        split[:, width:2 * width] = middle
        split[:, 2 * width:] = (rest - middle.astype(F32)).astype(BF16)
        slot = jnp.concatenate([base(w * WINDOW + k) + iota((BLOCK, step_n), 0) for k in range(WINDOW)], axis=0)

        def columns(c):
            cols = pl.ds(pl.multiple_of(c * step_n, step_n), step_n)
            hot = onehot(code_ref[:, cols] == slot)
            acc[:, cols] += dot(split[...], jnp.concatenate([hot, hot, hot], axis=0))

            @pl.when(c < 2)
            def _():
                start = (w + 1) * WINDOW - m + 2 * c
                loop(jnp.minimum(start + 2, total - m), arrived, jnp.maximum(start, 0))

        loop(WINDOW, columns)

    loop(WINDOW - m, arrived)
    loop(steps, window)

    def drain(q):
        amounts = (ms[q], ms[q], ms[q], total, cuts[q ^ 1] + ms[q ^ 2] - cuts[q ^ 2])
        for k, blocks in enumerate(amounts):
            if blocks:
                chunk = rows.at[pl.ds(0, blocks * HALF), :]
                remote(chunk, chunk, send.at[k], recv.at[0], mate).wait_send()

    if len(set(ms)) == 1 and len({cuts[q ^ 1] + ms[q ^ 2] - cuts[q ^ 2] for q in range(4)}) == 1:
        drain(0)
    else:
        for q in range(4):
            pl.when(chip == q)(functools.partial(drain, q))


def finish_kernel(s_ref, target_ref, prob_ref, logp_ref, prob, column, sem):
    rows, tile = prob.shape[0], logp_ref.shape[1]
    lane = iota((FINISH, prob.shape[1]), 1)

    def block(i):
        here = pl.ds(pl.multiple_of(i * FINISH, FINISH), FINISH)
        s = s_ref[here, :]
        top = jnp.max(s, axis=1, keepdims=True)
        e = jnp.exp(s - top)
        total = jnp.sum(e, axis=1, keepdims=True)
        prob[here, :] = e * (1.0 / total)
        picked = jnp.sum(jnp.where(lane == target_ref[here, :].astype(I32), s, 0.0), axis=1, keepdims=True)
        column[here, :] = picked - (top + jnp.log(total))
        pltpu.make_async_copy(prob.at[here, :], prob_ref.at[here, :], sem).start()

    def turn_out(i):
        value = column[pl.ds(pl.multiple_of(i * tile, tile), tile), :]
        logp_ref[pl.ds(i, 1), :] = jnp.broadcast_to(value, (tile, tile)).T[:1]

    loop(rows // FINISH, block)
    loop(rows // tile, turn_out)
    pltpu.make_async_copy(prob, prob_ref, sem).wait()


def solution(mesh):
    shards = mesh.shape["vocab"]
    chips = shards // 2
    hbm = pl.BlockSpec(memory_space=pl.ANY)
    vmem = pl.BlockSpec(memory_space=pltpu.VMEM)

    def device_step(hidden, w_head, allowed_ids, allowed_valid, target_pos):
        rows_dev, depth = hidden.shape
        length = allowed_ids.shape[0]
        most = length // BLOCK
        plans = sorted({p for p in PLANS if max(p) < most}, key=lambda p: (link_load(p), sum(p))) + [(most,) * chips]
        lanes = 128
        tile = 128
        part, code, column, which = pl.pallas_call(
            functools.partial(gather_kernel, chips, w_head.shape[0], plans),
            out_shape=(pltpu.VMEM((length, depth), BF16),
                       pltpu.VMEM((1, length), I32),
                       pltpu.VMEM((rows_dev, 1), F32),
                       pltpu.SMEM((1,), I32)),
            in_specs=[pl.BlockSpec(memory_space=pltpu.HBM)] * 4,
            out_specs=(vmem, vmem, vmem, pl.BlockSpec(memory_space=pltpu.SMEM)),
            scratch_shapes=[
                pltpu.VMEM((length // lanes, lanes), I32),
                pltpu.VMEM((length // lanes, lanes), I32),
                pltpu.VMEM((rows_dev // tile, tile), I32),
                pltpu.VMEM((1, length), I32),
                pltpu.VMEM((length, 8), BF16),
                pltpu.VMEM((length // lanes, lanes), I32),
                pltpu.SMEM((length // lanes, lanes), I32),
                pltpu.VMEM((length, 8), F32),
                pltpu.VMEM((RING, GROUP, 8, depth), BF16),
                pltpu.SemaphoreType.DMA((3,)),
                pltpu.SemaphoreType.DMA((length // lanes,)),
                pltpu.SemaphoreType.DMA((RING,)),
            ],
            compiler_params=pltpu.CompilerParams(vmem_limit_bytes=28 * MIB),
            name="gather_rows",
        )(*(pltpu.with_memory_space_constraint(v, pltpu.HBM) for v in (allowed_ids.reshape(-1, lanes), allowed_valid.reshape(-1, lanes))), w_head.reshape(-1, 8, depth),
          pltpu.with_memory_space_constraint(target_pos.reshape(-1, tile), pltpu.HBM))

        finish = pl.pallas_call(
            finish_kernel,
            out_shape=(jax.ShapeDtypeStruct((rows_dev, length), F32),
                       jax.ShapeDtypeStruct((rows_dev // tile, tile), F32)),
            in_specs=[vmem, vmem],
            out_specs=(hbm, vmem),
            scratch_shapes=[pltpu.VMEM((rows_dev, length), F32), pltpu.VMEM((rows_dev, 1), F32), pltpu.SemaphoreType.DMA],
            compiler_params=pltpu.CompilerParams(vmem_limit_bytes=16 * MIB),
            name="finish",
        )

        def serve(ms, cid):
            total, steps = sum(ms), -(-sum(ms) // WINDOW)
            dma = lambda n: pltpu.SemaphoreType.DMA((n,))
            exchange = pl.pallas_call(
                functools.partial(exchange_kernel, ms, length),
                out_shape=pltpu.VMEM((rows_dev, length), F32),
                in_specs=[vmem, vmem, vmem],
                out_specs=vmem,
                scratch_shapes=[
                    pltpu.VMEM((max(ms) * HALF, depth), BF16),
                    pltpu.VMEM((steps * WINDOW * BLOCK, depth), BF16),
                    pltpu.VMEM((rows_dev, 3 * WINDOW * BLOCK), BF16),
                    dma(5), dma(max(ms)), dma(total - min(ms)), dma(steps),
                ],
                compiler_params=pltpu.CompilerParams(collective_id=cid, has_side_effects=True,
                                                     vmem_limit_bytes=(8 + total // 5 + max(ms) // 10) * MIB),
                name="exchange_" + "_".join(map(str, ms)),
            )
            return lambda hidden, part, code, target: finish(exchange(hidden, part, code), target)

        probs, logp = lax.switch(which[0], [serve(ms, k) for k, ms in enumerate(plans)],
                                 hidden, part, code, column)
        return probs, logp.reshape(rows_dev)

    row_spec = P(("rep", "vocab"))
    mat_spec = P(("rep", "vocab"), None)
    return jax.shard_map(device_step, mesh=mesh, in_specs=(mat_spec, P("vocab", None), P("rep"), P("rep"), row_spec),
                         out_specs=(mat_spec, row_spec), check_vma=False)


PLANS = [(k,) * 4 for k in (6, 8, 9, 10, 11, 12, 14, 16)]
for heavy, others in ((14, 8), (12, 7), (10, 6)):
    PLANS += [tuple(heavy if c == h else others for c in range(4)) for h in range(4)]
```

```python
import functools

import jax
import jax.numpy as jnp
from jax import lax
from jax.experimental import pallas as pl
from jax.experimental.pallas import tpu as pltpu
from jax.sharding import PartitionSpec as P

INV_TEMP = 1.25
BLOCK = 64
HALF = BLOCK // 2
WINDOW = 4
GROUP = 128
SELECT = 32
RING = 5
FINISH = 128
MIB = 2 ** 20
MESH = pl.DeviceIdType.MESH
BF16, F32, I32 = jnp.bfloat16, jnp.float32, jnp.int32


def iota(shape, dim):
    return lax.broadcasted_iota(I32, shape, dim)


def onehot(mask):
    return jnp.where(mask, 1.0, 0.0).astype(BF16)


def dot(a, b, dims=((1,), (0,))):
    return lax.dot_general(a, b, (dims, ((), ())), preferred_element_type=F32)


def loop(n, f, start=0):
    def body(i, carry):
        f(i)
        return carry
    lax.fori_loop(start, n, body, 0)


def pick_of(table, index):
    value = jnp.int32(table[0])
    for k in range(1, len(table)):
        if table[k] != table[0]:
            value = jnp.where(index == k, table[k], value)
    return value


def gather_kernel(chips, vocab_local, plans, ids_hbm, valid_hbm, w_ref, target_hbm, part_ref, code_ref, column_ref, cap_ref,
                  ids_ref, valid_ref, target_ref, id_row, turned, table, table_s, pick, stage, load_sem, table_sem, in_sem):
    me = lax.axis_index("vocab")
    chip, devices = me // 2, 2 * chips
    loads = [pltpu.make_async_copy(ids_hbm, ids_ref, load_sem.at[0]),
             pltpu.make_async_copy(valid_hbm, valid_ref, load_sem.at[1]),
             pltpu.make_async_copy(target_hbm, target_ref, load_sem.at[2])]
    for load in loads:
        load.start()
    for load in loads:
        load.wait()
    rows, lanes = ids_ref.shape
    length = rows * lanes
    ids = ids_ref[...]
    valid = valid_ref[...] > 0
    owner = jnp.zeros_like(ids)
    for d in range(1, devices):
        owner += jnp.where(ids >= vocab_local * d, 1, 0)
    keep = [valid & (owner == d) for d in range(devices)]
    marks = jnp.concatenate([jnp.where(k, 1.0, 0.0) for k in keep], axis=0).astype(BF16)
    inside = dot(marks, onehot(iota((lanes, lanes), 0) <= iota((lanes, lanes), 1)))
    total = dot(marks, jnp.ones((lanes, lanes), BF16))
    n = devices * rows
    r, c_ = iota((n, n), 0), iota((n, n), 1)
    before = dot(onehot((r // (2 * rows) == c_ // (2 * rows)) & (c_ < r)), total.astype(BF16))
    rank = inside + before - 1.0
    code = jnp.full((rows, lanes), -1, I32)
    for d in range(devices):
        code = jnp.where(keep[d], d // 2 * length + rank[d * rows:(d + 1) * rows].astype(I32), code)
    own_id = jnp.where(valid, ids - me * vocab_local, -1)
    for k in range(rows):
        code_ref[:, k * lanes:(k + 1) * lanes] = code[k:k + 1]
        id_row[:, k * lanes:(k + 1) * lanes] = own_id[k:k + 1]
    after = before + total
    ours = iota((n, lanes), 0) // rows == me
    low = jnp.min(jnp.where(ours, before, 1e6)).astype(I32)
    high = jnp.max(jnp.where(ours, after, 0.0)).astype(I32)
    first, last = low // GROUP, (high + GROUP - 1) // GROUP
    last = jnp.where(high > low, last, first)

    local = id_row[...]
    owned = (local >= 0) & (local < vocab_local)
    tile = local >> 3
    sub = iota((8, length), 0)
    digits = jnp.where(sub == 0, tile >> 6, jnp.where(sub == 1, tile & 63, jnp.where(sub == 2, local & 7, 1)))
    digits = jnp.where(owned & (sub < 4), digits, 0).astype(F32)

    for k in range(rows):
        turned[k * lanes:(k + 1) * lanes, :] = digits[:, k * lanes:(k + 1) * lanes].T.astype(BF16)

    def fill(kb):
        hot = onehot(code_ref[...] == chip * length + kb * lanes + iota((lanes, length), 0))
        found = dot(hot, turned[...])
        pick[pl.ds(pl.multiple_of(kb * lanes, lanes), lanes), :] = found
        across = found.T
        spread = lax.rem(kb * lanes + iota((1, lanes), 1), w_ref.shape[0])
        table[pl.ds(kb, 1), :] = jnp.where(across[3:4] > 0.5, (across[0:1] * 64.0 + across[1:2]).astype(I32), spread)
        to_smem(kb).start()

    def to_smem(kb):
        return pltpu.make_async_copy(table.at[pl.ds(kb, 1), :], table_s.at[pl.ds(kb, 1), :], table_sem.at[kb])

    def each_run(g, act):
        for k in range(GROUP // SELECT):
            begin = g * GROUP + k * SELECT
            pl.when((begin < high) & (begin + SELECT > low))(functools.partial(act, k))

    def issue(g):
        slot = lax.rem(g, RING)
        to_smem(g).wait()

        def start(k):
            for i in range(k * SELECT, (k + 1) * SELECT):
                pltpu.make_async_copy(w_ref.at[table_s[g, i]], stage.at[slot, i], in_sem.at[slot]).start()

        each_run(g, start)

    def fill_and_issue(g):
        pl.when(g < last)(functools.partial(fill, g))
        pl.when((g > first) & (g <= first + RING))(functools.partial(issue, g - 1))

    loop(jnp.where(last > first, last + 1, first), fill_and_issue, first)

    counts = [jnp.max(after[c * 2 * rows:(c + 1) * 2 * rows]).astype(I32) for c in range(chips)]
    which = jnp.int32(len(plans) - 1)
    cap = pick_of(plans[-1], chip)
    for v in range(len(plans) - 2, -1, -1):
        fits = counts[0] <= plans[v][0] * BLOCK
        for c in range(1, chips):
            fits &= counts[c] <= plans[v][c] * BLOCK
        which = jnp.where(fits, v, which)
        cap = jnp.where(fits, pick_of(plans[v], chip), cap)
    cap_ref[0] = which

    groups = (cap * BLOCK + GROUP - 1) // GROUP
    tile = target_ref.shape[1]
    for k in range(target_ref.shape[0]):
        target = jnp.broadcast_to(target_ref[k:k + 1, :].astype(F32), (tile, tile)).T
        column_ref[k * tile:(k + 1) * tile, :] = target[:, :1]

    def blank(g):
        part_ref[pl.ds(pl.multiple_of(g * GROUP, GROUP), GROUP), :] = jnp.zeros((GROUP, part_ref.shape[1]), BF16)

    loop(first, blank)
    loop(groups, blank, last)

    def step(g):
        slot = lax.rem(g, RING)

        def finished(k):
            pltpu.make_async_copy(w_ref.at[pl.ds(0, SELECT)], stage.at[slot, pl.ds(0, SELECT)], in_sem.at[slot]).wait()

        each_run(g, finished)
        for k in range(GROUP // SELECT):
            here = pl.ds(pl.multiple_of(g * GROUP + k * SELECT, SELECT), SELECT)
            found = pick[here, :]
            owned = found[:, 3:4] > 0.5
            row = jnp.where(owned, found[:, 2:3], -4096.0).astype(I32)
            sel = onehot(iota((SELECT, 8 * SELECT), 1) - 8 * iota((SELECT, 8 * SELECT), 0) == row)
            tiles = stage[slot, k * SELECT:(k + 1) * SELECT].reshape(8 * SELECT, part_ref.shape[1])
            part_ref[here, :] = jnp.where(owned, dot(sel, tiles), 0.0).astype(BF16)

        @pl.when(g + RING < last)
        def _():
            issue(g + RING)

    loop(last, step, first)


def cuts_of(ms):
    cuts = []
    for s in range(4):
        through_y, through_x = ms[s ^ 2], ms[s ^ 1]
        cuts.append(min(max((through_y + ms[s] - through_x + 1) // 2, 0), ms[s]))
    return cuts


def link_load(ms):
    cuts = cuts_of(ms)
    return max(max(ms[s ^ 2] + ms[s] - cuts[s], ms[s ^ 1] + cuts[s]) for s in range(4))


def exchange_kernel(ms, length, hid, part, code_ref, acc, inc, rows, split, send, inc_recv, recv, p_recv):
    cuts, total = cuts_of(ms), sum(ms)
    steps = -(-total // WINDOW)
    pad = steps * WINDOW - total
    from_x = [ms[r ^ 1] + ms[r ^ 3] - cuts[r ^ 3] for r in range(4)]
    from_y = [ms[r ^ 2] + cuts[r ^ 3] for r in range(4)]
    both = [min(u, v) for u, v in zip(from_x, from_y)]
    longer = [int(v > u) for u, v in zip(from_x, from_y)]

    me = lax.axis_index("vocab")
    chip, core = me // 2, lax.rem(me, 2)
    x, y = lax.rem(chip, 2), chip // 2
    mate = {"vocab": me + 1 - 2 * core}
    x_dev = {"vocab": me + 2 - 4 * x}
    y_dev = {"vocab": me + 4 - 8 * y}
    x_chip, y_chip, d_chip = y * 2 + 1 - x, (1 - y) * 2 + x, (1 - y) * 2 + 1 - x
    mine, other = core * HALF, (1 - core) * HALF
    m, m_x, m_y, m_d = (pick_of(ms, c) for c in (chip, x_chip, y_chip, d_chip))
    cut_x, cut_y = pick_of(cuts, x_chip), pick_of(cuts, y_chip)
    shared, tail_side = pick_of(both, chip), pick_of(longer, chip)

    barrier = pltpu.get_barrier_semaphore()
    for dev in (mate, x_dev, y_dev):
        pl.semaphore_signal(barrier, inc=1, device_id=dev, device_id_type=MESH)

    pl.semaphore_wait(barrier, 3)

    def at(block, side):
        return rows.at[pl.ds(pl.multiple_of((block + pad) * BLOCK + side, HALF), HALF), :]

    def remote(src, dst, sent, received, dev):
        return pltpu.make_async_remote_copy(src_ref=src, dst_ref=dst, send_sem=sent, recv_sem=received,
                                            device_id=dev, device_id_type=MESH)

    def wait_for(n, sem):
        chunk = rows.at[pl.ds(0, n * HALF), :]
        remote(chunk, chunk, send.at[0], sem, mate).wait_recv()

    def inc_copy(i):
        return remote(part.at[pl.ds(pl.multiple_of(i * BLOCK + other, HALF), HALF), :],
                      inc.at[pl.ds(pl.multiple_of(i * HALF, HALF), HALF), :],
                      send.at[0], inc_recv.at[i], mate)

    def to_link(block, side, t, sent):
        there, dev = ((x_chip, x_dev), (y_chip, y_dev))[side]
        pair_up = pick_of(both, there)
        place = jnp.where(t < pair_up, 2 * t + side, pair_up + t)
        return remote(at(block, mine), at(pick_of(ms, there) + place, mine), send.at[sent], recv.at[place], dev)

    def pair(b):
        return remote(at(b, mine), at(b, mine), send.at[3], p_recv.at[(b + pad) // WINDOW], mate)

    loop(m, lambda i: inc_copy(jnp.where(i == 0, 0, jnp.where(i == 1, m - 1, i - 1))).start())

    def merge(i):
        wait_for(1, inc_recv.at[i])
        src = pl.ds(pl.multiple_of(i * BLOCK + mine, HALF), HALF)
        dst = pl.ds(pl.multiple_of((i + pad) * BLOCK + mine, HALF), HALF)
        rows[dst, :] = part[src, :] + inc[pl.ds(pl.multiple_of(i * HALF, HALF), HALF), :]

    merge(0)
    merge(m - 1)
    to_link(0, 0, 0, 1).start()
    to_link(m - 1, 1, 0, 2).start()
    loop(m - 1, merge, 1)

    def send_own(t):
        to_link(t, 0, t, 1).start()
        to_link(m - 1 - t, 1, t, 2).start()

    loop(m, send_own, 1)
    loop(m, lambda i: pair(i).start())

    def start_value(i):
        start = jnp.where(code_ref[...] >= 0, 0.0, -jnp.inf)
        acc[pl.ds(pl.multiple_of(i * 8, 8), 8), :] = jnp.broadcast_to(start, (8, length))

    loop(acc.shape[0] // 8, start_value)
    if pad:
        rows[:pad * BLOCK, :] = jnp.zeros((pad * BLOCK, rows.shape[1]), BF16)

    def source(p):
        paired = p < 2 * shared
        return jnp.where(paired, lax.rem(p + 2 * total, 2), tail_side), jnp.where(paired, p // 2, p - shared)

    def arrived(p):
        side, t = source(p)
        wait_for(1, recv.at[p])
        pair(m + p).start()

        @pl.when((side == 0) & (t < cut_x))
        def _():
            to_link(m + p, 1, m + t, 4).start()

        @pl.when((side == 1) & (t < m_y - cut_y))
        def _():
            to_link(m + p, 0, m + t, 4).start()

    def base(b):
        side, t = source(b - m)
        near = t < jnp.where(side == 0, m_x, m_y)
        of = jnp.where(near, jnp.where(side == 0, x_chip, y_chip), d_chip)
        i = jnp.where(side == 0, jnp.where(near, t, m_d - 1 - (t - m_x)), jnp.where(near, m_y - 1 - t, t - m_y))
        of, i = jnp.where(b < m, chip, of), jnp.where(b < m, b, i)
        return jnp.where(b >= 0, of * length + i * BLOCK, -length)

    width = WINDOW * BLOCK
    step_n = length // WINDOW

    def window(w):
        if pad:
            @pl.when(w > 0)
            def _():
                wait_for(WINDOW, p_recv.at[w])

            @pl.when(w == 0)
            def _():
                wait_for(WINDOW - pad, p_recv.at[w])
        else:
            wait_for(WINDOW, p_recv.at[w])
        got = rows[pl.ds(pl.multiple_of(w * width, width), width), :]
        s = dot(hid[...], got, ((1,), (1,))) * INV_TEMP
        high = s.astype(BF16)
        rest = s - high.astype(F32)
        middle = rest.astype(BF16)
        split[:, :width] = high
        split[:, width:2 * width] = middle
        split[:, 2 * width:] = (rest - middle.astype(F32)).astype(BF16)
        slot = jnp.concatenate([base(w * WINDOW + k - pad) + iota((BLOCK, step_n), 0) for k in range(WINDOW)], axis=0)

        def columns(c):
            cols = pl.ds(pl.multiple_of(c * step_n, step_n), step_n)
            hot = onehot(code_ref[:, cols] == slot)
            acc[:, cols] += dot(split[...], jnp.concatenate([hot, hot, hot], axis=0))

            @pl.when(c < 2)
            def _():
                start = (w + 1) * WINDOW - pad - m + 2 * c
                loop(jnp.minimum(start + 2, total - m), arrived, jnp.maximum(start, 0))

        loop(WINDOW, columns)

    loop(WINDOW - pad - m, arrived)
    loop(steps, window)

    def drain(q):
        amounts = (ms[q], ms[q], ms[q], total, cuts[q ^ 1] + ms[q ^ 2] - cuts[q ^ 2])
        for k, blocks in enumerate(amounts):
            if blocks:
                chunk = rows.at[pl.ds(0, blocks * HALF), :]
                remote(chunk, chunk, send.at[k], recv.at[0], mate).wait_send()

    if len(set(ms)) == 1 and len({cuts[q ^ 1] + ms[q ^ 2] - cuts[q ^ 2] for q in range(4)}) == 1:
        drain(0)
    else:
        for q in range(4):
            pl.when(chip == q)(functools.partial(drain, q))


def finish_kernel(s_ref, target_ref, prob_ref, logp_ref, prob, column, sem):
    rows, tile = prob.shape[0], logp_ref.shape[1]
    lane = iota((FINISH, prob.shape[1]), 1)

    def block(i):
        here = pl.ds(pl.multiple_of(i * FINISH, FINISH), FINISH)
        s = s_ref[here, :]
        top = jnp.max(s, axis=1, keepdims=True)
        e = jnp.exp(s - top)
        total = jnp.sum(e, axis=1, keepdims=True)
        prob[here, :] = e * (1.0 / total)
        picked = jnp.sum(jnp.where(lane == target_ref[here, :].astype(I32), s, 0.0), axis=1, keepdims=True)
        column[here, :] = picked - (top + jnp.log(total))
        pltpu.make_async_copy(prob.at[here, :], prob_ref.at[here, :], sem).start()

    def turn_out(i):
        value = column[pl.ds(pl.multiple_of(i * tile, tile), tile), :]
        logp_ref[pl.ds(i, 1), :] = jnp.broadcast_to(value, (tile, tile)).T[:1]

    loop(rows // FINISH, block)
    loop(rows // tile, turn_out)
    pltpu.make_async_copy(prob, prob_ref, sem).wait()


def solution(mesh):
    shards = mesh.shape["vocab"]
    chips = shards // 2
    hbm = pl.BlockSpec(memory_space=pl.ANY)
    vmem = pl.BlockSpec(memory_space=pltpu.VMEM)

    def device_step(hidden, w_head, allowed_ids, allowed_valid, target_pos):
        rows_dev, depth = hidden.shape
        length = allowed_ids.shape[0]
        most = length // BLOCK
        plans = sorted({p for p in PLANS if max(p) < most}, key=lambda p: (link_load(p), sum(p))) + [(most,) * chips]
        lanes = 128
        tile = 128
        part, code, column, which = pl.pallas_call(
            functools.partial(gather_kernel, chips, w_head.shape[0], plans),
            out_shape=(pltpu.VMEM((length, depth), BF16),
                       pltpu.VMEM((1, length), I32),
                       pltpu.VMEM((rows_dev, 1), F32),
                       pltpu.SMEM((1,), I32)),
            in_specs=[pl.BlockSpec(memory_space=pltpu.HBM)] * 4,
            out_specs=(vmem, vmem, vmem, pl.BlockSpec(memory_space=pltpu.SMEM)),
            scratch_shapes=[
                pltpu.VMEM((length // lanes, lanes), I32),
                pltpu.VMEM((length // lanes, lanes), I32),
                pltpu.VMEM((rows_dev // tile, tile), I32),
                pltpu.VMEM((1, length), I32),
                pltpu.VMEM((length, 8), BF16),
                pltpu.VMEM((length // lanes, lanes), I32),
                pltpu.SMEM((length // lanes, lanes), I32),
                pltpu.VMEM((length, 8), F32),
                pltpu.VMEM((RING, GROUP, 8, depth), BF16),
                pltpu.SemaphoreType.DMA((3,)),
                pltpu.SemaphoreType.DMA((length // lanes,)),
                pltpu.SemaphoreType.DMA((RING,)),
            ],
            compiler_params=pltpu.CompilerParams(vmem_limit_bytes=28 * MIB),
            name="gather_rows",
        )(*(pltpu.with_memory_space_constraint(v, pltpu.HBM) for v in (allowed_ids.reshape(-1, lanes), allowed_valid.reshape(-1, lanes))), w_head.reshape(-1, 8, depth),
          pltpu.with_memory_space_constraint(target_pos.reshape(-1, tile), pltpu.HBM))

        finish = pl.pallas_call(
            finish_kernel,
            out_shape=(jax.ShapeDtypeStruct((rows_dev, length), F32),
                       jax.ShapeDtypeStruct((rows_dev // tile, tile), F32)),
            in_specs=[vmem, vmem],
            out_specs=(hbm, vmem),
            scratch_shapes=[pltpu.VMEM((rows_dev, length), F32), pltpu.VMEM((rows_dev, 1), F32), pltpu.SemaphoreType.DMA],
            compiler_params=pltpu.CompilerParams(vmem_limit_bytes=16 * MIB),
            name="finish",
        )

        def serve(ms, cid):
            total, steps = sum(ms), -(-sum(ms) // WINDOW)
            dma = lambda n: pltpu.SemaphoreType.DMA((n,))
            exchange = pl.pallas_call(
                functools.partial(exchange_kernel, ms, length),
                out_shape=pltpu.VMEM((rows_dev, length), F32),
                in_specs=[vmem, vmem, vmem],
                out_specs=vmem,
                scratch_shapes=[
                    pltpu.VMEM((max(ms) * HALF, depth), BF16),
                    pltpu.VMEM((steps * WINDOW * BLOCK, depth), BF16),
                    pltpu.VMEM((rows_dev, 3 * WINDOW * BLOCK), BF16),
                    dma(5), dma(max(ms)), dma(total - min(ms)), dma(steps),
                ],
                compiler_params=pltpu.CompilerParams(collective_id=cid, has_side_effects=True,
                                                     vmem_limit_bytes=(8 + total // 5 + max(ms) // 10) * MIB),
                name="exchange_" + "_".join(map(str, ms)),
            )
            return lambda hidden, part, code, target: finish(exchange(hidden, part, code), target)

        probs, logp = lax.switch(which[0], [serve(ms, k) for k, ms in enumerate(plans)],
                                 hidden, part, code, column)
        return probs, logp.reshape(rows_dev)

    row_spec = P(("rep", "vocab"))
    mat_spec = P(("rep", "vocab"), None)
    return jax.shard_map(device_step, mesh=mesh, in_specs=(mat_spec, P("vocab", None), P("rep"), P("rep"), row_spec),
                         out_specs=(mat_spec, row_spec), check_vma=False)


PLANS = [(k,) * 4 for k in (6, 8, 9, 10, 11, 12, 14, 16)]
for heavy, others in ((14, 8), (12, 7), (10, 6)):
    PLANS += [tuple(heavy if c == h else others for c in range(4)) for h in range(4)]
```

```python
import functools

import jax
import jax.numpy as jnp
from jax import lax
from jax.experimental import pallas as pl
from jax.experimental.pallas import tpu as pltpu
from jax.sharding import PartitionSpec as P

INV_TEMP = 1.25
BLOCK = 64
HALF = BLOCK // 2
WINDOW = 4
GROUP = 128
SELECT = 32
RING = 5
FINISH = 128
MIB = 2 ** 20
MESH = pl.DeviceIdType.MESH
BF16, F32, I32 = jnp.bfloat16, jnp.float32, jnp.int32
BF16_MAX = float(jnp.finfo(BF16).max)


def iota(shape, dim):
    return lax.broadcasted_iota(I32, shape, dim)


def onehot(mask):
    return jnp.where(mask, 1.0, 0.0).astype(BF16)


def dot(a, b, dims=((1,), (0,))):
    return lax.dot_general(a, b, (dims, ((), ())), preferred_element_type=F32)


def loop(n, f, start=0):
    def body(i, carry):
        f(i)
        return carry
    lax.fori_loop(start, n, body, 0)


def pick_of(table, index):
    value = jnp.int32(table[0])
    for k in range(1, len(table)):
        if table[k] != table[0]:
            value = jnp.where(index == k, table[k], value)
    return value


def gather_kernel(chips, vocab_local, plans, ids_hbm, valid_hbm, w_ref, target_hbm, part_ref, code_ref, column_ref, cap_ref,
                  ids_ref, valid_ref, target_ref, id_row, turned, table, table_s, pick, stage, load_sem, table_sem, in_sem):
    me = lax.axis_index("vocab")
    chip, devices = me // 2, 2 * chips
    loads = [pltpu.make_async_copy(ids_hbm, ids_ref, load_sem.at[0]),
             pltpu.make_async_copy(valid_hbm, valid_ref, load_sem.at[1]),
             pltpu.make_async_copy(target_hbm, target_ref, load_sem.at[2])]
    for load in loads:
        load.start()
    for load in loads:
        load.wait()
    rows, lanes = ids_ref.shape
    length = rows * lanes
    ids = ids_ref[...]
    valid = valid_ref[...] > 0
    owner = jnp.zeros_like(ids)
    for d in range(1, devices):
        owner += jnp.where(ids >= vocab_local * d, 1, 0)
    keep = [valid & (owner == d) for d in range(devices)]
    marks = jnp.concatenate([jnp.where(k, 1.0, 0.0) for k in keep], axis=0).astype(BF16)
    inside = dot(marks, onehot(iota((lanes, lanes), 0) <= iota((lanes, lanes), 1)))
    total = dot(marks, jnp.ones((lanes, lanes), BF16))
    n = devices * rows
    r, c_ = iota((n, n), 0), iota((n, n), 1)
    before = dot(onehot((r // (2 * rows) == c_ // (2 * rows)) & (c_ < r)), total.astype(BF16))
    rank = inside + before - 1.0
    code = jnp.full((rows, lanes), -1, I32)
    for d in range(devices):
        code = jnp.where(keep[d], d // 2 * length + rank[d * rows:(d + 1) * rows].astype(I32), code)
    own_id = jnp.where(valid, ids - me * vocab_local, -1)
    for k in range(rows):
        code_ref[:, k * lanes:(k + 1) * lanes] = code[k:k + 1]
        id_row[:, k * lanes:(k + 1) * lanes] = own_id[k:k + 1]
    after = before + total
    ours = iota((n, lanes), 0) // rows == me
    low = jnp.min(jnp.where(ours, before, 1e6)).astype(I32)
    high = jnp.max(jnp.where(ours, after, 0.0)).astype(I32)
    first, last = low // GROUP, (high + GROUP - 1) // GROUP
    last = jnp.where(high > low, last, first)

    local = id_row[...]
    owned = (local >= 0) & (local < vocab_local)
    tile = local >> 3
    sub = iota((8, length), 0)
    digits = jnp.where(sub == 0, tile >> 6, jnp.where(sub == 1, tile & 63, jnp.where(sub == 2, local & 7, 1)))
    digits = jnp.where(owned & (sub < 4), digits, 0).astype(F32)

    for k in range(rows):
        turned[k * lanes:(k + 1) * lanes, :] = digits[:, k * lanes:(k + 1) * lanes].T.astype(BF16)

    def fill(kb):
        hot = onehot(code_ref[...] == chip * length + kb * lanes + iota((lanes, length), 0))
        found = dot(hot, turned[...])
        pick[pl.ds(pl.multiple_of(kb * lanes, lanes), lanes), :] = found
        across = found.T
        spread = lax.rem(kb * lanes + iota((1, lanes), 1), w_ref.shape[0])
        table[pl.ds(kb, 1), :] = jnp.where(across[3:4] > 0.5, (across[0:1] * 64.0 + across[1:2]).astype(I32), spread)
        to_smem(kb).start()

    def to_smem(kb):
        return pltpu.make_async_copy(table.at[pl.ds(kb, 1), :], table_s.at[pl.ds(kb, 1), :], table_sem.at[kb])

    def each_run(g, act):
        for k in range(GROUP // SELECT):
            begin = g * GROUP + k * SELECT
            pl.when((begin < high) & (begin + SELECT > low))(functools.partial(act, k))

    def issue(g):
        slot = lax.rem(g, RING)
        to_smem(g).wait()

        def start(k):
            for i in range(k * SELECT, (k + 1) * SELECT):
                pltpu.make_async_copy(w_ref.at[table_s[g, i]], stage.at[slot, i], in_sem.at[slot]).start()

        each_run(g, start)

    def fill_and_issue(g):
        pl.when(g < last)(functools.partial(fill, g))
        pl.when((g > first) & (g <= first + RING))(functools.partial(issue, g - 1))

    loop(jnp.where(last > first, last + 1, first), fill_and_issue, first)

    counts = [jnp.max(after[c * 2 * rows:(c + 1) * 2 * rows]).astype(I32) for c in range(chips)]
    which = jnp.int32(len(plans) - 1)
    cap = pick_of(plans[-1], chip)
    for v in range(len(plans) - 2, -1, -1):
        fits = counts[0] <= plans[v][0] * BLOCK
        for c in range(1, chips):
            fits &= counts[c] <= plans[v][c] * BLOCK
        which = jnp.where(fits, v, which)
        cap = jnp.where(fits, pick_of(plans[v], chip), cap)
    cap_ref[0] = which

    groups = (cap * BLOCK + GROUP - 1) // GROUP
    tile = target_ref.shape[1]
    for k in range(target_ref.shape[0]):
        target = jnp.broadcast_to(target_ref[k:k + 1, :].astype(F32), (tile, tile)).T
        column_ref[k * tile:(k + 1) * tile, :] = target[:, :1]

    def blank(g):
        part_ref[pl.ds(pl.multiple_of(g * GROUP, GROUP), GROUP), :] = jnp.zeros((GROUP, part_ref.shape[1]), BF16)

    loop(first, blank)
    loop(groups, blank, last)

    def step(g):
        slot = lax.rem(g, RING)

        def finished(k):
            pltpu.make_async_copy(w_ref.at[pl.ds(0, SELECT)], stage.at[slot, pl.ds(0, SELECT)], in_sem.at[slot]).wait()

        each_run(g, finished)
        for k in range(GROUP // SELECT):
            here = pl.ds(pl.multiple_of(g * GROUP + k * SELECT, SELECT), SELECT)
            found = pick[here, :]
            owned = found[:, 3:4] > 0.5
            row = jnp.where(owned, found[:, 2:3], -4096.0).astype(I32)
            sel = onehot(iota((SELECT, 8 * SELECT), 1) - 8 * iota((SELECT, 8 * SELECT), 0) == row)
            tiles = stage[slot, k * SELECT:(k + 1) * SELECT].reshape(8 * SELECT, part_ref.shape[1])
            part_ref[here, :] = jnp.where(owned, dot(sel, tiles), 0.0).astype(BF16)

        @pl.when(g + RING < last)
        def _():
            issue(g + RING)

    loop(last, step, first)


def cuts_of(ms):
    cuts = []
    for s in range(4):
        through_y, through_x = ms[s ^ 2], ms[s ^ 1]
        cuts.append(min(max((through_y + ms[s] - through_x + 1) // 2, 0), ms[s]))
    return cuts


def link_load(ms):
    cuts = cuts_of(ms)
    return max(max(ms[s ^ 2] + ms[s] - cuts[s], ms[s ^ 1] + cuts[s]) for s in range(4))


def exchange_kernel(ms, length, hid, part, code_ref, acc, inc, rows, split, send, inc_recv, recv, p_recv):
    cuts, total = cuts_of(ms), sum(ms)
    steps = -(-total // WINDOW)
    pad = steps * WINDOW - total
    from_x = [ms[r ^ 1] + ms[r ^ 3] - cuts[r ^ 3] for r in range(4)]
    from_y = [ms[r ^ 2] + cuts[r ^ 3] for r in range(4)]
    both = [min(u, v) for u, v in zip(from_x, from_y)]
    longer = [int(v > u) for u, v in zip(from_x, from_y)]

    me = lax.axis_index("vocab")
    chip, core = me // 2, lax.rem(me, 2)
    x, y = lax.rem(chip, 2), chip // 2
    mate = {"vocab": me + 1 - 2 * core}
    x_dev = {"vocab": me + 2 - 4 * x}
    y_dev = {"vocab": me + 4 - 8 * y}
    x_chip, y_chip, d_chip = y * 2 + 1 - x, (1 - y) * 2 + x, (1 - y) * 2 + 1 - x
    mine, other = core * HALF, (1 - core) * HALF
    m, m_x, m_y, m_d = (pick_of(ms, c) for c in (chip, x_chip, y_chip, d_chip))
    cut_x, cut_y = pick_of(cuts, x_chip), pick_of(cuts, y_chip)
    shared, tail_side = pick_of(both, chip), pick_of(longer, chip)

    barrier = pltpu.get_barrier_semaphore()
    for dev in (mate, x_dev, y_dev):
        pl.semaphore_signal(barrier, inc=1, device_id=dev, device_id_type=MESH)

    pl.semaphore_wait(barrier, 3)

    def at(block, side):
        return rows.at[pl.ds(pl.multiple_of((block + pad) * BLOCK + side, HALF), HALF), :]

    def remote(src, dst, sent, received, dev):
        return pltpu.make_async_remote_copy(src_ref=src, dst_ref=dst, send_sem=sent, recv_sem=received,
                                            device_id=dev, device_id_type=MESH)

    def wait_for(n, sem):
        chunk = rows.at[pl.ds(0, n * HALF), :]
        remote(chunk, chunk, send.at[0], sem, mate).wait_recv()

    def inc_copy(i):
        return remote(part.at[pl.ds(pl.multiple_of(i * BLOCK + other, HALF), HALF), :],
                      inc.at[pl.ds(pl.multiple_of(i * HALF, HALF), HALF), :],
                      send.at[0], inc_recv.at[i], mate)

    def to_link(block, side, t, sent):
        there, dev = ((x_chip, x_dev), (y_chip, y_dev))[side]
        pair_up = pick_of(both, there)
        place = jnp.where(t < pair_up, 2 * t + side, pair_up + t)
        return remote(at(block, mine), at(pick_of(ms, there) + place, mine), send.at[sent], recv.at[place], dev)

    def pair(b):
        return remote(at(b, mine), at(b, mine), send.at[3], p_recv.at[(b + pad) // WINDOW], mate)

    loop(m, lambda i: inc_copy(jnp.where(i == 0, 0, jnp.where(i == 1, m - 1, i - 1))).start())

    def merge(i):
        wait_for(1, inc_recv.at[i])
        src = pl.ds(pl.multiple_of(i * BLOCK + mine, HALF), HALF)
        dst = pl.ds(pl.multiple_of((i + pad) * BLOCK + mine, HALF), HALF)
        rows[dst, :] = part[src, :] + inc[pl.ds(pl.multiple_of(i * HALF, HALF), HALF), :]

    merge(0)
    merge(m - 1)
    to_link(0, 0, 0, 1).start()
    to_link(m - 1, 1, 0, 2).start()
    loop(m - 1, merge, 1)

    def send_own(t):
        to_link(t, 0, t, 1).start()
        to_link(m - 1 - t, 1, t, 2).start()

    loop(m, send_own, 1)
    loop(m, lambda i: pair(i).start())

    def start_value(i):
        start = jnp.where(code_ref[...] >= 0, 0.0, -jnp.inf)
        acc[pl.ds(pl.multiple_of(i * 8, 8), 8), :] = jnp.broadcast_to(start, (8, length))

    loop(acc.shape[0] // 8, start_value)
    if pad:
        rows[:pad * BLOCK, :] = jnp.zeros((pad * BLOCK, rows.shape[1]), BF16)

    def source(p):
        paired = p < 2 * shared
        return jnp.where(paired, lax.rem(p + 2 * total, 2), tail_side), jnp.where(paired, p // 2, p - shared)

    def arrived(p):
        side, t = source(p)
        wait_for(1, recv.at[p])
        pair(m + p).start()

        @pl.when((side == 0) & (t < cut_x))
        def _():
            to_link(m + p, 1, m + t, 4).start()

        @pl.when((side == 1) & (t < m_y - cut_y))
        def _():
            to_link(m + p, 0, m + t, 4).start()

    def base(b):
        side, t = source(b - m)
        near = t < jnp.where(side == 0, m_x, m_y)
        of = jnp.where(near, jnp.where(side == 0, x_chip, y_chip), d_chip)
        i = jnp.where(side == 0, jnp.where(near, t, m_d - 1 - (t - m_x)), jnp.where(near, m_y - 1 - t, t - m_y))
        of, i = jnp.where(b < m, chip, of), jnp.where(b < m, b, i)
        return jnp.where(b >= 0, of * length + i * BLOCK, -length)

    width = WINDOW * BLOCK
    step_n = length // WINDOW

    def window(w):
        if pad:
            @pl.when(w > 0)
            def _():
                wait_for(WINDOW, p_recv.at[w])

            @pl.when(w == 0)
            def _():
                wait_for(WINDOW - pad, p_recv.at[w])
        else:
            wait_for(WINDOW, p_recv.at[w])
        got = rows[pl.ds(pl.multiple_of(w * width, width), width), :]
        s = dot(hid[...], got, ((1,), (1,))) * INV_TEMP
        high = jnp.clip(s, -BF16_MAX, BF16_MAX).astype(BF16)
        rest = s - high.astype(F32)
        middle = rest.astype(BF16)
        split[:, :width] = high
        split[:, width:2 * width] = middle
        split[:, 2 * width:] = (rest - middle.astype(F32)).astype(BF16)
        slot = jnp.concatenate([base(w * WINDOW + k - pad) + iota((BLOCK, step_n), 0) for k in range(WINDOW)], axis=0)

        def columns(c):
            cols = pl.ds(pl.multiple_of(c * step_n, step_n), step_n)
            hot = onehot(code_ref[:, cols] == slot)
            acc[:, cols] += dot(split[...], jnp.concatenate([hot, hot, hot], axis=0))

            @pl.when(c < 2)
            def _():
                start = (w + 1) * WINDOW - pad - m + 2 * c
                loop(jnp.minimum(start + 2, total - m), arrived, jnp.maximum(start, 0))

        loop(WINDOW, columns)

    loop(WINDOW - pad - m, arrived)
    loop(steps, window)

    def drain(q):
        amounts = (ms[q], ms[q], ms[q], total, cuts[q ^ 1] + ms[q ^ 2] - cuts[q ^ 2])
        for k, blocks in enumerate(amounts):
            if blocks:
                chunk = rows.at[pl.ds(0, blocks * HALF), :]
                remote(chunk, chunk, send.at[k], recv.at[0], mate).wait_send()

    if len(set(ms)) == 1 and len({cuts[q ^ 1] + ms[q ^ 2] - cuts[q ^ 2] for q in range(4)}) == 1:
        drain(0)
    else:
        for q in range(4):
            pl.when(chip == q)(functools.partial(drain, q))


def finish_kernel(s_ref, target_ref, prob_ref, logp_ref, prob, column, sem):
    rows, tile = prob.shape[0], logp_ref.shape[1]
    lane = iota((FINISH, prob.shape[1]), 1)

    def block(i):
        here = pl.ds(pl.multiple_of(i * FINISH, FINISH), FINISH)
        s = s_ref[here, :]
        top = jnp.max(s, axis=1, keepdims=True)
        e = jnp.exp(s - top)
        total = jnp.sum(e, axis=1, keepdims=True)
        prob[here, :] = e * (1.0 / total)
        picked = jnp.sum(jnp.where(lane == target_ref[here, :].astype(I32), s, 0.0), axis=1, keepdims=True)
        column[here, :] = picked - (top + jnp.log(total))
        pltpu.make_async_copy(prob.at[here, :], prob_ref.at[here, :], sem).start()

    def turn_out(i):
        value = column[pl.ds(pl.multiple_of(i * tile, tile), tile), :]
        logp_ref[pl.ds(i, 1), :] = jnp.broadcast_to(value, (tile, tile)).T[:1]

    loop(rows // FINISH, block)
    loop(rows // tile, turn_out)
    pltpu.make_async_copy(prob, prob_ref, sem).wait()


def solution(mesh):
    shards = mesh.shape["vocab"]
    chips = shards // 2
    hbm = pl.BlockSpec(memory_space=pl.ANY)
    vmem = pl.BlockSpec(memory_space=pltpu.VMEM)

    def device_step(hidden, w_head, allowed_ids, allowed_valid, target_pos):
        rows_dev, depth = hidden.shape
        length = allowed_ids.shape[0]
        most = length // BLOCK
        plans = sorted({p for p in PLANS if max(p) < most}, key=lambda p: (link_load(p), sum(p), p)) + [(most,) * chips]
        lanes = 128
        tile = 128
        part, code, column, which = pl.pallas_call(
            functools.partial(gather_kernel, chips, w_head.shape[0], plans),
            out_shape=(pltpu.VMEM((length, depth), BF16),
                       pltpu.VMEM((1, length), I32),
                       pltpu.VMEM((rows_dev, 1), F32),
                       pltpu.SMEM((1,), I32)),
            in_specs=[pl.BlockSpec(memory_space=pltpu.HBM)] * 4,
            out_specs=(vmem, vmem, vmem, pl.BlockSpec(memory_space=pltpu.SMEM)),
            scratch_shapes=[
                pltpu.VMEM((length // lanes, lanes), I32),
                pltpu.VMEM((length // lanes, lanes), I32),
                pltpu.VMEM((rows_dev // tile, tile), I32),
                pltpu.VMEM((1, length), I32),
                pltpu.VMEM((length, 8), BF16),
                pltpu.VMEM((length // lanes, lanes), I32),
                pltpu.SMEM((length // lanes, lanes), I32),
                pltpu.VMEM((length, 8), F32),
                pltpu.VMEM((RING, GROUP, 8, depth), BF16),
                pltpu.SemaphoreType.DMA((3,)),
                pltpu.SemaphoreType.DMA((length // lanes,)),
                pltpu.SemaphoreType.DMA((RING,)),
            ],
            compiler_params=pltpu.CompilerParams(vmem_limit_bytes=28 * MIB),
            name="gather_rows",
        )(*(pltpu.with_memory_space_constraint(v, pltpu.HBM) for v in (allowed_ids.reshape(-1, lanes), allowed_valid.reshape(-1, lanes))), w_head.reshape(-1, 8, depth),
          pltpu.with_memory_space_constraint(target_pos.reshape(-1, tile), pltpu.HBM))

        finish = pl.pallas_call(
            finish_kernel,
            out_shape=(jax.ShapeDtypeStruct((rows_dev, length), F32),
                       jax.ShapeDtypeStruct((rows_dev // tile, tile), F32)),
            in_specs=[vmem, vmem],
            out_specs=(hbm, vmem),
            scratch_shapes=[pltpu.VMEM((rows_dev, length), F32), pltpu.VMEM((rows_dev, 1), F32), pltpu.SemaphoreType.DMA],
            compiler_params=pltpu.CompilerParams(vmem_limit_bytes=16 * MIB),
            name="finish",
        )

        def serve(ms, cid):
            total, steps = sum(ms), -(-sum(ms) // WINDOW)
            dma = lambda n: pltpu.SemaphoreType.DMA((n,))
            exchange = pl.pallas_call(
                functools.partial(exchange_kernel, ms, length),
                out_shape=pltpu.VMEM((rows_dev, length), F32),
                in_specs=[vmem, vmem, vmem],
                out_specs=vmem,
                scratch_shapes=[
                    pltpu.VMEM((max(ms) * HALF, depth), BF16),
                    pltpu.VMEM((steps * WINDOW * BLOCK, depth), BF16),
                    pltpu.VMEM((rows_dev, 3 * WINDOW * BLOCK), BF16),
                    dma(5), dma(max(ms)), dma(total - min(ms)), dma(steps),
                ],
                compiler_params=pltpu.CompilerParams(collective_id=cid, has_side_effects=True,
                                                     vmem_limit_bytes=(8 + total // 5 + max(ms) // 10) * MIB),
                name="exchange_" + "_".join(map(str, ms)),
            )
            return lambda hidden, part, code, target: finish(exchange(hidden, part, code), target)

        probs, logp = lax.switch(which[0], [serve(ms, k) for k, ms in enumerate(plans)],
                                 hidden, part, code, column)
        return probs, logp.reshape(rows_dev)

    row_spec = P(("rep", "vocab"))
    mat_spec = P(("rep", "vocab"), None)
    return jax.shard_map(device_step, mesh=mesh, in_specs=(mat_spec, P("vocab", None), P("rep"), P("rep"), row_spec),
                         out_specs=(mat_spec, row_spec), check_vma=False)


PLANS = [(k,) * 4 for k in (6, 8, 9, 10, 11, 12, 14, 16)]
for heavy, others in ((14, 8), (12, 7), (10, 6)):
    PLANS += [tuple(heavy if c == h else others for c in range(4)) for h in range(4)]
```

```python
import functools

import jax
import jax.numpy as jnp
from jax import lax
from jax.experimental import pallas as pl
from jax.experimental.pallas import tpu as pltpu
from jax.sharding import PartitionSpec as P

INV_TEMP = 1.25
BLOCK = 64
HALF = BLOCK // 2
WINDOW = 4
GROUP = 128
SELECT = 32
RING = 5
FINISH = 128
MIB = 2 ** 20
MESH = pl.DeviceIdType.MESH
BF16, F32, I32 = jnp.bfloat16, jnp.float32, jnp.int32
BF16_MAX = float(jnp.finfo(BF16).max)


def iota(shape, dim):
    return lax.broadcasted_iota(I32, shape, dim)


def onehot(mask):
    return jnp.where(mask, 1.0, 0.0).astype(BF16)


def dot(a, b, dims=((1,), (0,))):
    return lax.dot_general(a, b, (dims, ((), ())), preferred_element_type=F32)


def loop(n, f, start=0):
    def body(i, carry):
        f(i)
        return carry
    lax.fori_loop(start, n, body, 0)


def pick_of(table, index):
    value = jnp.int32(table[0])
    for k in range(1, len(table)):
        if table[k] != table[0]:
            value = jnp.where(index == k, table[k], value)
    return value


def gather_kernel(chips, vocab_local, plans, ids_hbm, valid_hbm, w_ref, target_hbm, part_ref, code_ref, column_ref, cap_ref,
                  ids_ref, valid_ref, target_ref, id_row, turned, table, table_s, pick, stage, load_sem, table_sem, in_sem):
    me = lax.axis_index("vocab")
    chip, devices = me // 2, 2 * chips
    loads = [pltpu.make_async_copy(ids_hbm, ids_ref, load_sem.at[0]),
             pltpu.make_async_copy(valid_hbm, valid_ref, load_sem.at[1]),
             pltpu.make_async_copy(target_hbm, target_ref, load_sem.at[2])]
    for load in loads:
        load.start()
    for load in loads:
        load.wait()
    rows, lanes = ids_ref.shape
    length = rows * lanes
    ids = ids_ref[...]
    valid = valid_ref[...] > 0
    owner = jnp.zeros_like(ids)
    for d in range(1, devices):
        owner += jnp.where(ids >= vocab_local * d, 1, 0)
    keep = [valid & (owner == d) for d in range(devices)]
    marks = jnp.concatenate([jnp.where(k, 1.0, 0.0) for k in keep], axis=0).astype(BF16)
    inside = dot(marks, onehot(iota((lanes, lanes), 0) <= iota((lanes, lanes), 1)))
    total = dot(marks, jnp.ones((lanes, lanes), BF16))
    n = devices * rows
    r, c_ = iota((n, n), 0), iota((n, n), 1)
    before = dot(onehot((r // (2 * rows) == c_ // (2 * rows)) & (c_ < r)), total.astype(BF16))
    rank = inside + before - 1.0
    code = jnp.full((rows, lanes), -1, I32)
    for d in range(devices):
        code = jnp.where(keep[d], d // 2 * length + rank[d * rows:(d + 1) * rows].astype(I32), code)
    own_id = jnp.where(valid, ids - me * vocab_local, -1)
    for k in range(rows):
        code_ref[:, k * lanes:(k + 1) * lanes] = code[k:k + 1]
        id_row[:, k * lanes:(k + 1) * lanes] = own_id[k:k + 1]
    after = before + total
    ours = iota((n, lanes), 0) // rows == me
    low = jnp.min(jnp.where(ours, before, 1e6)).astype(I32)
    high = jnp.max(jnp.where(ours, after, 0.0)).astype(I32)
    first, last = low // GROUP, (high + GROUP - 1) // GROUP
    last = jnp.where(high > low, last, first)

    local = id_row[...]
    owned = (local >= 0) & (local < vocab_local)
    tile = local >> 3
    sub = iota((8, length), 0)
    digits = jnp.where(sub == 0, tile >> 6, jnp.where(sub == 1, tile & 63, jnp.where(sub == 2, local & 7, 1)))
    digits = jnp.where(owned & (sub < 4), digits, 0).astype(F32)

    for k in range(rows):
        turned[k * lanes:(k + 1) * lanes, :] = digits[:, k * lanes:(k + 1) * lanes].T.astype(BF16)

    def fill(kb):
        hot = onehot(code_ref[...] == chip * length + kb * lanes + iota((lanes, length), 0))
        found = dot(hot, turned[...])
        pick[pl.ds(pl.multiple_of(kb * lanes, lanes), lanes), :] = found
        across = found.T
        spread = lax.rem(kb * lanes + iota((1, lanes), 1), w_ref.shape[0])
        table[pl.ds(kb, 1), :] = jnp.where(across[3:4] > 0.5, (across[0:1] * 64.0 + across[1:2]).astype(I32), spread)
        to_smem(kb).start()

    def to_smem(kb):
        return pltpu.make_async_copy(table.at[pl.ds(kb, 1), :], table_s.at[pl.ds(kb, 1), :], table_sem.at[kb])

    def each_run(g, act):
        for k in range(GROUP // SELECT):
            begin = g * GROUP + k * SELECT
            pl.when((begin < high) & (begin + SELECT > low))(functools.partial(act, k))

    def issue(g):
        slot = lax.rem(g, RING)
        to_smem(g).wait()

        def start(k):
            for i in range(k * SELECT, (k + 1) * SELECT):
                pltpu.make_async_copy(w_ref.at[table_s[g, i]], stage.at[slot, i], in_sem.at[slot]).start()

        each_run(g, start)

    def fill_and_issue(g):
        pl.when(g < last)(functools.partial(fill, g))
        pl.when((g > first) & (g <= first + RING))(functools.partial(issue, g - 1))

    loop(jnp.where(last > first, last + 1, first), fill_and_issue, first)

    counts = [jnp.max(after[c * 2 * rows:(c + 1) * 2 * rows]).astype(I32) for c in range(chips)]
    which = jnp.int32(len(plans) - 1)
    cap = pick_of(plans[-1], chip)
    for v in range(len(plans) - 2, -1, -1):
        fits = counts[0] <= plans[v][0] * BLOCK
        for c in range(1, chips):
            fits &= counts[c] <= plans[v][c] * BLOCK
        which = jnp.where(fits, v, which)
        cap = jnp.where(fits, pick_of(plans[v], chip), cap)
    cap_ref[0] = which

    groups = (cap * BLOCK + GROUP - 1) // GROUP
    tile = target_ref.shape[1]
    for k in range(target_ref.shape[0]):
        target = jnp.broadcast_to(target_ref[k:k + 1, :].astype(F32), (tile, tile)).T
        column_ref[k * tile:(k + 1) * tile, :] = target[:, :1]

    def blank(g):
        part_ref[pl.ds(pl.multiple_of(g * GROUP, GROUP), GROUP), :] = jnp.zeros((GROUP, part_ref.shape[1]), BF16)

    loop(first, blank)
    loop(groups, blank, last)

    def step(g):
        slot = lax.rem(g, RING)

        def finished(k):
            pltpu.make_async_copy(w_ref.at[pl.ds(0, SELECT)], stage.at[slot, pl.ds(0, SELECT)], in_sem.at[slot]).wait()

        each_run(g, finished)
        for k in range(GROUP // SELECT):
            here = pl.ds(pl.multiple_of(g * GROUP + k * SELECT, SELECT), SELECT)
            found = pick[here, :]
            owned = found[:, 3:4] > 0.5
            row = jnp.where(owned, found[:, 2:3], -4096.0).astype(I32)
            sel = onehot(iota((SELECT, 8 * SELECT), 1) - 8 * iota((SELECT, 8 * SELECT), 0) == row)
            tiles = stage[slot, k * SELECT:(k + 1) * SELECT].reshape(8 * SELECT, part_ref.shape[1])
            part_ref[here, :] = jnp.where(owned, dot(sel, tiles), 0.0).astype(BF16)

        @pl.when(g + RING < last)
        def _():
            issue(g + RING)

    loop(last, step, first)


def cuts_of(ms):
    cuts = []
    for s in range(4):
        through_y, through_x = ms[s ^ 2], ms[s ^ 1]
        cuts.append(min(max((through_y + ms[s] - through_x + 1) // 2, 0), ms[s]))
    return cuts


def link_load(ms):
    cuts = cuts_of(ms)
    return max(max(ms[s ^ 2] + ms[s] - cuts[s], ms[s ^ 1] + cuts[s]) for s in range(4))


def exchange_kernel(ms, length, hid, part, code_ref, acc, inc, rows, split, send, inc_recv, recv, p_recv):
    cuts, total = cuts_of(ms), sum(ms)
    steps = -(-total // WINDOW)
    pad = steps * WINDOW - total
    from_x = [ms[r ^ 1] + ms[r ^ 3] - cuts[r ^ 3] for r in range(4)]
    from_y = [ms[r ^ 2] + cuts[r ^ 3] for r in range(4)]
    both = [min(u, v) for u, v in zip(from_x, from_y)]
    longer = [int(v > u) for u, v in zip(from_x, from_y)]

    me = lax.axis_index("vocab")
    chip, core = me // 2, lax.rem(me, 2)
    x, y = lax.rem(chip, 2), chip // 2
    mate = {"vocab": me + 1 - 2 * core}
    x_dev = {"vocab": me + 2 - 4 * x}
    y_dev = {"vocab": me + 4 - 8 * y}
    x_chip, y_chip, d_chip = y * 2 + 1 - x, (1 - y) * 2 + x, (1 - y) * 2 + 1 - x
    mine, other = core * HALF, (1 - core) * HALF
    m, m_x, m_y, m_d = (pick_of(ms, c) for c in (chip, x_chip, y_chip, d_chip))
    cut_x, cut_y = pick_of(cuts, x_chip), pick_of(cuts, y_chip)
    shared, tail_side = pick_of(both, chip), pick_of(longer, chip)

    barrier = pltpu.get_barrier_semaphore()
    for dev in (mate, x_dev, y_dev):
        pl.semaphore_signal(barrier, inc=1, device_id=dev, device_id_type=MESH)

    pl.semaphore_wait(barrier, 3)

    def at(block, side):
        return rows.at[pl.ds(pl.multiple_of((block + pad) * BLOCK + side, HALF), HALF), :]

    def remote(src, dst, sent, received, dev):
        return pltpu.make_async_remote_copy(src_ref=src, dst_ref=dst, send_sem=sent, recv_sem=received,
                                            device_id=dev, device_id_type=MESH)

    def wait_for(n, sem):
        chunk = rows.at[pl.ds(0, n * HALF), :]
        remote(chunk, chunk, send.at[0], sem, mate).wait_recv()

    def inc_copy(i):
        return remote(part.at[pl.ds(pl.multiple_of(i * BLOCK + other, HALF), HALF), :],
                      inc.at[pl.ds(pl.multiple_of(i * HALF, HALF), HALF), :],
                      send.at[0], inc_recv.at[i], mate)

    def to_link(block, side, t, sent):
        there, dev = ((x_chip, x_dev), (y_chip, y_dev))[side]
        pair_up = pick_of(both, there)
        place = jnp.where(t < pair_up, 2 * t + side, pair_up + t)
        return remote(at(block, mine), at(pick_of(ms, there) + place, mine), send.at[sent], recv.at[place], dev)

    def pair(b):
        return remote(at(b, mine), at(b, mine), send.at[3], p_recv.at[(b + pad) // WINDOW], mate)

    loop(m, lambda i: inc_copy(jnp.where(i == 0, 0, jnp.where(i == 1, m - 1, i - 1))).start())

    def start_value(i):
        start = jnp.where(code_ref[...] >= 0, 0.0, -jnp.inf)
        acc[pl.ds(pl.multiple_of(i * 8, 8), 8), :] = jnp.broadcast_to(start, (8, length))

    loop(acc.shape[0] // 8, start_value)
    if pad:
        rows[:pad * BLOCK, :] = jnp.zeros((pad * BLOCK, rows.shape[1]), BF16)

    def merge(i):
        wait_for(1, inc_recv.at[i])
        src = pl.ds(pl.multiple_of(i * BLOCK + mine, HALF), HALF)
        dst = pl.ds(pl.multiple_of((i + pad) * BLOCK + mine, HALF), HALF)
        rows[dst, :] = part[src, :] + inc[pl.ds(pl.multiple_of(i * HALF, HALF), HALF), :]

    merge(0)
    merge(m - 1)
    to_link(0, 0, 0, 1).start()
    to_link(m - 1, 1, 0, 2).start()
    loop(m - 1, merge, 1)

    def send_own(t):
        to_link(t, 0, t, 1).start()
        to_link(m - 1 - t, 1, t, 2).start()

    loop(m, send_own, 1)
    loop(m, lambda i: pair(i).start())

    def source(p):
        paired = p < 2 * shared
        return jnp.where(paired, lax.rem(p + 2 * total, 2), tail_side), jnp.where(paired, p // 2, p - shared)

    def arrived(p):
        side, t = source(p)
        wait_for(1, recv.at[p])
        pair(m + p).start()

        @pl.when((side == 0) & (t < cut_x))
        def _():
            to_link(m + p, 1, m + t, 4).start()

        @pl.when((side == 1) & (t < m_y - cut_y))
        def _():
            to_link(m + p, 0, m + t, 4).start()

    def base(b):
        side, t = source(b - m)
        near = t < jnp.where(side == 0, m_x, m_y)
        of = jnp.where(near, jnp.where(side == 0, x_chip, y_chip), d_chip)
        i = jnp.where(side == 0, jnp.where(near, t, m_d - 1 - (t - m_x)), jnp.where(near, m_y - 1 - t, t - m_y))
        of, i = jnp.where(b < m, chip, of), jnp.where(b < m, b, i)
        return jnp.where(b >= 0, of * length + i * BLOCK, -length)

    width = WINDOW * BLOCK
    step_n = length // WINDOW

    def window(w):
        if pad:
            @pl.when(w > 0)
            def _():
                wait_for(WINDOW, p_recv.at[w])

            @pl.when(w == 0)
            def _():
                wait_for(WINDOW - pad, p_recv.at[w])
        else:
            wait_for(WINDOW, p_recv.at[w])
        got = rows[pl.ds(pl.multiple_of(w * width, width), width), :]
        s = dot(hid[...], got, ((1,), (1,))) * INV_TEMP
        high = jnp.clip(s, -BF16_MAX, BF16_MAX).astype(BF16)
        rest = s - high.astype(F32)
        middle = rest.astype(BF16)
        split[:, :width] = high
        split[:, width:2 * width] = middle
        split[:, 2 * width:] = (rest - middle.astype(F32)).astype(BF16)
        slot = jnp.concatenate([base(w * WINDOW + k - pad) + iota((BLOCK, step_n), 0) for k in range(WINDOW)], axis=0)

        def columns(c):
            cols = pl.ds(pl.multiple_of(c * step_n, step_n), step_n)
            hot = onehot(code_ref[:, cols] == slot)
            acc[:, cols] += dot(split[...], jnp.concatenate([hot, hot, hot], axis=0))

            @pl.when(c < 2)
            def _():
                start = (w + 1) * WINDOW - pad - m + 2 * c
                loop(jnp.minimum(start + 2, total - m), arrived, jnp.maximum(start, 0))

        loop(WINDOW, columns)

    loop(WINDOW - pad - m, arrived)
    loop(steps, window)

    def drain(q):
        amounts = (ms[q], ms[q], ms[q], total, cuts[q ^ 1] + ms[q ^ 2] - cuts[q ^ 2])
        for k, blocks in enumerate(amounts):
            if blocks:
                chunk = rows.at[pl.ds(0, blocks * HALF), :]
                remote(chunk, chunk, send.at[k], recv.at[0], mate).wait_send()

    if len(set(ms)) == 1 and len({cuts[q ^ 1] + ms[q ^ 2] - cuts[q ^ 2] for q in range(4)}) == 1:
        drain(0)
    else:
        for q in range(4):
            pl.when(chip == q)(functools.partial(drain, q))


def finish_kernel(s_ref, target_ref, prob_ref, logp_ref, prob, column, sem):
    rows, tile = prob.shape[0], logp_ref.shape[1]
    lane = iota((FINISH, prob.shape[1]), 1)

    def block(i):
        here = pl.ds(pl.multiple_of(i * FINISH, FINISH), FINISH)
        s = s_ref[here, :]
        top = jnp.max(s, axis=1, keepdims=True)
        e = jnp.exp(s - top)
        total = jnp.sum(e, axis=1, keepdims=True)
        prob[here, :] = e * (1.0 / total)
        picked = jnp.sum(jnp.where(lane == target_ref[here, :].astype(I32), s, 0.0), axis=1, keepdims=True)
        column[here, :] = picked - (top + jnp.log(total))
        pltpu.make_async_copy(prob.at[here, :], prob_ref.at[here, :], sem).start()

    def turn_out(i):
        value = column[pl.ds(pl.multiple_of(i * tile, tile), tile), :]
        logp_ref[pl.ds(i, 1), :] = jnp.broadcast_to(value, (tile, tile)).T[:1]

    loop(rows // FINISH, block)
    loop(rows // tile, turn_out)
    pltpu.make_async_copy(prob, prob_ref, sem).wait()


def solution(mesh):
    shards = mesh.shape["vocab"]
    chips = shards // 2
    hbm = pl.BlockSpec(memory_space=pl.ANY)
    vmem = pl.BlockSpec(memory_space=pltpu.VMEM)

    def device_step(hidden, w_head, allowed_ids, allowed_valid, target_pos):
        rows_dev, depth = hidden.shape
        length = allowed_ids.shape[0]
        most = length // BLOCK
        plans = sorted({p for p in PLANS if max(p) < most}, key=lambda p: (link_load(p), sum(p), p)) + [(most,) * chips]
        lanes = 128
        tile = 128
        part, code, column, which = pl.pallas_call(
            functools.partial(gather_kernel, chips, w_head.shape[0], plans),
            out_shape=(pltpu.VMEM((length, depth), BF16),
                       pltpu.VMEM((1, length), I32),
                       pltpu.VMEM((rows_dev, 1), F32),
                       pltpu.SMEM((1,), I32)),
            in_specs=[pl.BlockSpec(memory_space=pltpu.HBM)] * 4,
            out_specs=(vmem, vmem, vmem, pl.BlockSpec(memory_space=pltpu.SMEM)),
            scratch_shapes=[
                pltpu.VMEM((length // lanes, lanes), I32),
                pltpu.VMEM((length // lanes, lanes), I32),
                pltpu.VMEM((rows_dev // tile, tile), I32),
                pltpu.VMEM((1, length), I32),
                pltpu.VMEM((length, 8), BF16),
                pltpu.VMEM((length // lanes, lanes), I32),
                pltpu.SMEM((length // lanes, lanes), I32),
                pltpu.VMEM((length, 8), F32),
                pltpu.VMEM((RING, GROUP, 8, depth), BF16),
                pltpu.SemaphoreType.DMA((3,)),
                pltpu.SemaphoreType.DMA((length // lanes,)),
                pltpu.SemaphoreType.DMA((RING,)),
            ],
            compiler_params=pltpu.CompilerParams(vmem_limit_bytes=28 * MIB),
            name="gather_rows",
        )(*(pltpu.with_memory_space_constraint(v, pltpu.HBM) for v in (allowed_ids.reshape(-1, lanes), allowed_valid.reshape(-1, lanes))), w_head.reshape(-1, 8, depth),
          pltpu.with_memory_space_constraint(target_pos.reshape(-1, tile), pltpu.HBM))

        finish = pl.pallas_call(
            finish_kernel,
            out_shape=(jax.ShapeDtypeStruct((rows_dev, length), F32),
                       jax.ShapeDtypeStruct((rows_dev // tile, tile), F32)),
            in_specs=[vmem, vmem],
            out_specs=(hbm, vmem),
            scratch_shapes=[pltpu.VMEM((rows_dev, length), F32), pltpu.VMEM((rows_dev, 1), F32), pltpu.SemaphoreType.DMA],
            compiler_params=pltpu.CompilerParams(vmem_limit_bytes=16 * MIB),
            name="finish",
        )

        def serve(ms, cid):
            total, steps = sum(ms), -(-sum(ms) // WINDOW)
            dma = lambda n: pltpu.SemaphoreType.DMA((n,))
            exchange = pl.pallas_call(
                functools.partial(exchange_kernel, ms, length),
                out_shape=pltpu.VMEM((rows_dev, length), F32),
                in_specs=[vmem, vmem, vmem],
                out_specs=vmem,
                scratch_shapes=[
                    pltpu.VMEM((max(ms) * HALF, depth), BF16),
                    pltpu.VMEM((steps * WINDOW * BLOCK, depth), BF16),
                    pltpu.VMEM((rows_dev, 3 * WINDOW * BLOCK), BF16),
                    dma(5), dma(max(ms)), dma(total - min(ms)), dma(steps),
                ],
                compiler_params=pltpu.CompilerParams(collective_id=cid, has_side_effects=True,
                                                     vmem_limit_bytes=(8 + total // 5 + max(ms) // 10) * MIB),
                name="exchange_" + "_".join(map(str, ms)),
            )
            return lambda hidden, part, code, target: finish(exchange(hidden, part, code), target)

        probs, logp = lax.switch(which[0], [serve(ms, k) for k, ms in enumerate(plans)],
                                 hidden, part, code, column)
        return probs, logp.reshape(rows_dev)

    row_spec = P(("rep", "vocab"))
    mat_spec = P(("rep", "vocab"), None)
    return jax.shard_map(device_step, mesh=mesh, in_specs=(mat_spec, P("vocab", None), P("rep"), P("rep"), row_spec),
                         out_specs=(mat_spec, row_spec), check_vma=False)


PLANS = [(k,) * 4 for k in (6, 8, 9, 10, 11, 12, 14, 16)]
for heavy, others in ((14, 8), (12, 7), (10, 6)):
    PLANS += [tuple(heavy if c == h else others for c in range(4)) for h in range(4)]
```

```python
import functools

import jax
import jax.numpy as jnp
from jax import lax
from jax.experimental import pallas as pl
from jax.experimental.pallas import tpu as pltpu
from jax.sharding import PartitionSpec as P

INV_TEMP = 1.25
BLOCK = 64
HALF = BLOCK // 2
WINDOW = 4
GROUP = 128
SELECT = 32
RING = 5
FINISH = 128
MIB = 2 ** 20
MESH = pl.DeviceIdType.MESH
BF16, F32, I32 = jnp.bfloat16, jnp.float32, jnp.int32
BF16_MAX = float(jnp.finfo(BF16).max)


def iota(shape, dim):
    return lax.broadcasted_iota(I32, shape, dim)


def onehot(mask):
    return jnp.where(mask, 1.0, 0.0).astype(BF16)


def dot(a, b, dims=((1,), (0,))):
    return lax.dot_general(a, b, (dims, ((), ())), preferred_element_type=F32)


def loop(n, f, start=0):
    def body(i, carry):
        f(i)
        return carry
    lax.fori_loop(start, n, body, 0)


def pick_of(table, index):
    value = jnp.int32(table[0])
    for k in range(1, len(table)):
        if table[k] != table[0]:
            value = jnp.where(index == k, table[k], value)
    return value


def gather_kernel(chips, vocab_local, plans, ids_hbm, valid_hbm, w_ref, target_hbm, part_ref, code_ref, column_ref, cap_ref,
                  ids_ref, valid_ref, target_ref, id_row, turned, table, table_s, pick, stage, load_sem, table_sem, in_sem):
    me = lax.axis_index("vocab")
    chip, devices = me // 2, 2 * chips
    loads = [pltpu.make_async_copy(ids_hbm, ids_ref, load_sem.at[0]),
             pltpu.make_async_copy(valid_hbm, valid_ref, load_sem.at[1]),
             pltpu.make_async_copy(target_hbm, target_ref, load_sem.at[2])]
    for load in loads:
        load.start()
    for load in loads:
        load.wait()
    rows, lanes = ids_ref.shape
    length = rows * lanes
    ids = ids_ref[...]
    valid = valid_ref[...] > 0
    owner = jnp.zeros_like(ids)
    for d in range(1, devices):
        owner += jnp.where(ids >= vocab_local * d, 1, 0)
    keep = [valid & (owner == d) for d in range(devices)]
    marks = jnp.concatenate([jnp.where(k, 1.0, 0.0) for k in keep], axis=0).astype(BF16)
    inside = dot(marks, onehot(iota((lanes, lanes), 0) <= iota((lanes, lanes), 1)))
    total = dot(marks, jnp.ones((lanes, lanes), BF16))
    n = devices * rows
    r, c_ = iota((n, n), 0), iota((n, n), 1)
    before = dot(onehot((r // (2 * rows) == c_ // (2 * rows)) & (c_ < r)), total.astype(BF16))
    rank = inside + before - 1.0
    code = jnp.full((rows, lanes), -1, I32)
    for d in range(devices):
        code = jnp.where(keep[d], d // 2 * length + rank[d * rows:(d + 1) * rows].astype(I32), code)
    own_id = jnp.where(valid, ids - me * vocab_local, -1)
    for k in range(rows):
        code_ref[:, k * lanes:(k + 1) * lanes] = code[k:k + 1]
        id_row[:, k * lanes:(k + 1) * lanes] = own_id[k:k + 1]
    after = before + total
    ours = iota((n, lanes), 0) // rows == me
    low = jnp.min(jnp.where(ours, before, 1e6)).astype(I32)
    high = jnp.max(jnp.where(ours, after, 0.0)).astype(I32)
    first, last = low // GROUP, (high + GROUP - 1) // GROUP
    last = jnp.where(high > low, last, first)

    local = id_row[...]
    owned = (local >= 0) & (local < vocab_local)
    tile = local >> 3
    sub = iota((8, length), 0)
    digits = jnp.where(sub == 0, tile >> 6, jnp.where(sub == 1, tile & 63, jnp.where(sub == 2, local & 7, 1)))
    digits = jnp.where(owned & (sub < 4), digits, 0).astype(F32)

    for k in range(rows):
        turned[k * lanes:(k + 1) * lanes, :] = digits[:, k * lanes:(k + 1) * lanes].T.astype(BF16)

    def fill(kb):
        hot = onehot(code_ref[...] == chip * length + kb * lanes + iota((lanes, length), 0))
        found = dot(hot, turned[...])
        pick[pl.ds(pl.multiple_of(kb * lanes, lanes), lanes), :] = found
        across = found.T
        spread = lax.rem(kb * lanes + iota((1, lanes), 1), w_ref.shape[0])
        table[pl.ds(kb, 1), :] = jnp.where(across[3:4] > 0.5, (across[0:1] * 64.0 + across[1:2]).astype(I32), spread)
        to_smem(kb).start()

    def to_smem(kb):
        return pltpu.make_async_copy(table.at[pl.ds(kb, 1), :], table_s.at[pl.ds(kb, 1), :], table_sem.at[kb])

    def each_run(g, act):
        for k in range(GROUP // SELECT):
            begin = g * GROUP + k * SELECT
            pl.when((begin < high) & (begin + SELECT > low))(functools.partial(act, k))

    def issue(g):
        slot = lax.rem(g, RING)
        to_smem(g).wait()

        def start(k):
            for i in range(k * SELECT, (k + 1) * SELECT):
                pltpu.make_async_copy(w_ref.at[table_s[g, i]], stage.at[slot, i], in_sem.at[slot]).start()

        each_run(g, start)

    def fill_and_issue(g):
        pl.when(g < last)(functools.partial(fill, g))
        pl.when((g > first) & (g <= first + RING))(functools.partial(issue, g - 1))

    loop(jnp.where(last > first, last + 1, first), fill_and_issue, first)

    counts = [jnp.max(after[c * 2 * rows:(c + 1) * 2 * rows]).astype(I32) for c in range(chips)]
    which = jnp.int32(len(plans) - 1)
    cap = pick_of(plans[-1], chip)
    for v in range(len(plans) - 2, -1, -1):
        fits = counts[0] <= plans[v][0] * BLOCK
        for c in range(1, chips):
            fits &= counts[c] <= plans[v][c] * BLOCK
        which = jnp.where(fits, v, which)
        cap = jnp.where(fits, pick_of(plans[v], chip), cap)
    cap_ref[0] = which

    groups = (cap * BLOCK + GROUP - 1) // GROUP
    tile = target_ref.shape[1]
    for k in range(target_ref.shape[0]):
        target = jnp.broadcast_to(target_ref[k:k + 1, :].astype(F32), (tile, tile)).T
        column_ref[k * tile:(k + 1) * tile, :] = target[:, :1]

    def blank(g):
        part_ref[pl.ds(pl.multiple_of(g * GROUP, GROUP), GROUP), :] = jnp.zeros((GROUP, part_ref.shape[1]), BF16)

    loop(first, blank)
    loop(groups, blank, last)

    def step(g):
        slot = lax.rem(g, RING)

        def finished(k):
            pltpu.make_async_copy(w_ref.at[pl.ds(0, SELECT)], stage.at[slot, pl.ds(0, SELECT)], in_sem.at[slot]).wait()

        each_run(g, finished)
        for k in range(GROUP // SELECT):
            here = pl.ds(pl.multiple_of(g * GROUP + k * SELECT, SELECT), SELECT)
            found = pick[here, :]
            owned = found[:, 3:4] > 0.5
            row = jnp.where(owned, found[:, 2:3], -4096.0).astype(I32)
            sel = onehot(iota((SELECT, 8 * SELECT), 1) - 8 * iota((SELECT, 8 * SELECT), 0) == row)
            tiles = stage[slot, k * SELECT:(k + 1) * SELECT].reshape(8 * SELECT, part_ref.shape[1])
            part_ref[here, :] = jnp.where(owned, dot(sel, tiles), 0.0).astype(BF16)

        @pl.when(g + RING < last)
        def _():
            issue(g + RING)

    loop(last, step, first)


def cuts_of(ms):
    cuts = []
    for s in range(4):
        through_y, through_x = ms[s ^ 2], ms[s ^ 1]
        cuts.append(min(max((through_y + ms[s] - through_x + 1) // 2, 0), ms[s]))
    return cuts


def link_load(ms):
    cuts = cuts_of(ms)
    return max(max(ms[s ^ 2] + ms[s] - cuts[s], ms[s ^ 1] + cuts[s]) for s in range(4))


def exchange_kernel(ms, length, hid, part, code_ref, acc, inc, rows, split, send, inc_recv, recv, p_recv):
    cuts, total = cuts_of(ms), sum(ms)
    steps = -(-total // WINDOW)
    pad = steps * WINDOW - total
    from_x = [ms[r ^ 1] + ms[r ^ 3] - cuts[r ^ 3] for r in range(4)]
    from_y = [ms[r ^ 2] + cuts[r ^ 3] for r in range(4)]
    both = [min(u, v) for u, v in zip(from_x, from_y)]
    longer = [int(v > u) for u, v in zip(from_x, from_y)]

    me = lax.axis_index("vocab")
    chip, core = me // 2, lax.rem(me, 2)
    x, y = lax.rem(chip, 2), chip // 2
    mate = {"vocab": me + 1 - 2 * core}
    x_dev = {"vocab": me + 2 - 4 * x}
    y_dev = {"vocab": me + 4 - 8 * y}
    x_chip, y_chip, d_chip = y * 2 + 1 - x, (1 - y) * 2 + x, (1 - y) * 2 + 1 - x
    mine, other = core * HALF, (1 - core) * HALF
    m, m_x, m_y, m_d = (pick_of(ms, c) for c in (chip, x_chip, y_chip, d_chip))
    cut_x, cut_y = pick_of(cuts, x_chip), pick_of(cuts, y_chip)
    shared, tail_side = pick_of(both, chip), pick_of(longer, chip)

    barrier = pltpu.get_barrier_semaphore()
    for dev in (mate, x_dev, y_dev):
        pl.semaphore_signal(barrier, inc=1, device_id=dev, device_id_type=MESH)

    pl.semaphore_wait(barrier, 3)

    def at(block, side):
        return rows.at[pl.ds(pl.multiple_of((block + pad) * BLOCK + side, HALF), HALF), :]

    def remote(src, dst, sent, received, dev):
        return pltpu.make_async_remote_copy(src_ref=src, dst_ref=dst, send_sem=sent, recv_sem=received,
                                            device_id=dev, device_id_type=MESH)

    def wait_for(n, sem):
        chunk = rows.at[pl.ds(0, n * HALF), :]
        remote(chunk, chunk, send.at[0], sem, mate).wait_recv()

    def inc_copy(i):
        return remote(part.at[pl.ds(pl.multiple_of(i * BLOCK + other, HALF), HALF), :],
                      inc.at[pl.ds(pl.multiple_of(i * HALF, HALF), HALF), :],
                      send.at[0], inc_recv.at[i], mate)

    def to_link(block, side, t, sent):
        there, dev = ((x_chip, x_dev), (y_chip, y_dev))[side]
        pair_up = pick_of(both, there)
        place = jnp.where(t < pair_up, 2 * t + side, pair_up + t)
        return remote(at(block, mine), at(pick_of(ms, there) + place, mine), send.at[sent], recv.at[place], dev)

    def pair(b):
        return remote(at(b, mine), at(b, mine), send.at[3], p_recv.at[(b + pad) // WINDOW], mate)

    loop(m, lambda i: inc_copy(jnp.where(i == 0, 0, jnp.where(i == 1, m - 1, i - 1))).start())

    def merge(i):
        wait_for(1, inc_recv.at[i])
        src = pl.ds(pl.multiple_of(i * BLOCK + mine, HALF), HALF)
        dst = pl.ds(pl.multiple_of((i + pad) * BLOCK + mine, HALF), HALF)
        rows[dst, :] = part[src, :] + inc[pl.ds(pl.multiple_of(i * HALF, HALF), HALF), :]

    merge(0)
    merge(m - 1)
    to_link(0, 0, 0, 1).start()
    to_link(m - 1, 1, 0, 2).start()
    loop(m - 1, merge, 1)

    def send_own(t):
        to_link(t, 0, t, 1).start()
        to_link(m - 1 - t, 1, t, 2).start()

    loop(m, send_own, 1)
    loop(m, lambda i: pair(i).start())

    def start_value(i):
        start = jnp.where(code_ref[...] >= 0, 0.0, -jnp.inf)
        acc[pl.ds(pl.multiple_of(i * 32, 32), 32), :] = jnp.broadcast_to(start, (32, length))

    loop(acc.shape[0] // 32, start_value)
    if pad:
        rows[:pad * BLOCK, :] = jnp.zeros((pad * BLOCK, rows.shape[1]), BF16)

    def source(p):
        paired = p < 2 * shared
        return jnp.where(paired, lax.rem(p + 2 * total, 2), tail_side), jnp.where(paired, p // 2, p - shared)

    def arrived(p):
        side, t = source(p)
        wait_for(1, recv.at[p])
        pair(m + p).start()

        @pl.when((side == 0) & (t < cut_x))
        def _():
            to_link(m + p, 1, m + t, 4).start()

        @pl.when((side == 1) & (t < m_y - cut_y))
        def _():
            to_link(m + p, 0, m + t, 4).start()

    def base(b):
        side, t = source(b - m)
        near = t < jnp.where(side == 0, m_x, m_y)
        of = jnp.where(near, jnp.where(side == 0, x_chip, y_chip), d_chip)
        i = jnp.where(side == 0, jnp.where(near, t, m_d - 1 - (t - m_x)), jnp.where(near, m_y - 1 - t, t - m_y))
        of, i = jnp.where(b < m, chip, of), jnp.where(b < m, b, i)
        return jnp.where(b >= 0, of * length + i * BLOCK, -length)

    width = WINDOW * BLOCK
    step_n = length // WINDOW

    def window(w):
        if pad:
            @pl.when(w > 0)
            def _():
                wait_for(WINDOW, p_recv.at[w])

            @pl.when(w == 0)
            def _():
                wait_for(WINDOW - pad, p_recv.at[w])
        else:
            wait_for(WINDOW, p_recv.at[w])
        got = rows[pl.ds(pl.multiple_of(w * width, width), width), :]
        s = dot(hid[...], got, ((1,), (1,))) * INV_TEMP
        high = jnp.clip(s, -BF16_MAX, BF16_MAX).astype(BF16)
        rest = s - high.astype(F32)
        middle = rest.astype(BF16)
        split[:, :width] = high
        split[:, width:2 * width] = middle
        split[:, 2 * width:] = (rest - middle.astype(F32)).astype(BF16)
        slot = jnp.concatenate([base(w * WINDOW + k - pad) + iota((BLOCK, step_n), 0) for k in range(WINDOW)], axis=0)

        def columns(c):
            cols = pl.ds(pl.multiple_of(c * step_n, step_n), step_n)
            hot = onehot(code_ref[:, cols] == slot)
            acc[:, cols] += dot(split[...], jnp.concatenate([hot, hot, hot], axis=0))

            @pl.when(c < 2)
            def _():
                start = (w + 1) * WINDOW - pad - m + 2 * c
                loop(jnp.minimum(start + 2, total - m), arrived, jnp.maximum(start, 0))

        loop(WINDOW, columns)

    loop(WINDOW - pad - m, arrived)
    loop(steps, window)

    def drain(q):
        amounts = (ms[q], ms[q], ms[q], total, cuts[q ^ 1] + ms[q ^ 2] - cuts[q ^ 2])
        for k, blocks in enumerate(amounts):
            if blocks:
                chunk = rows.at[pl.ds(0, blocks * HALF), :]
                remote(chunk, chunk, send.at[k], recv.at[0], mate).wait_send()

    if len(set(ms)) == 1 and len({cuts[q ^ 1] + ms[q ^ 2] - cuts[q ^ 2] for q in range(4)}) == 1:
        drain(0)
    else:
        for q in range(4):
            pl.when(chip == q)(functools.partial(drain, q))


def finish_kernel(s_ref, target_ref, prob_ref, logp_ref, prob, column, sem):
    rows, tile = prob.shape[0], logp_ref.shape[1]
    lane = iota((FINISH, prob.shape[1]), 1)

    def block(i):
        here = pl.ds(pl.multiple_of(i * FINISH, FINISH), FINISH)
        s = s_ref[here, :]
        top = jnp.max(s, axis=1, keepdims=True)
        e = jnp.exp(s - top)
        total = jnp.sum(e, axis=1, keepdims=True)
        prob[here, :] = e * (1.0 / total)
        picked = jnp.sum(jnp.where(lane == target_ref[here, :].astype(I32), s, 0.0), axis=1, keepdims=True)
        column[here, :] = picked - (top + jnp.log(total))
        pltpu.make_async_copy(prob.at[here, :], prob_ref.at[here, :], sem).start()

    def turn_out(i):
        value = column[pl.ds(pl.multiple_of(i * tile, tile), tile), :]
        logp_ref[pl.ds(i, 1), :] = jnp.broadcast_to(value, (tile, tile)).T[:1]

    loop(rows // FINISH, block)
    loop(rows // tile, turn_out)
    pltpu.make_async_copy(prob, prob_ref, sem).wait()


def solution(mesh):
    shards = mesh.shape["vocab"]
    chips = shards // 2
    hbm = pl.BlockSpec(memory_space=pl.ANY)
    vmem = pl.BlockSpec(memory_space=pltpu.VMEM)

    def device_step(hidden, w_head, allowed_ids, allowed_valid, target_pos):
        rows_dev, depth = hidden.shape
        length = allowed_ids.shape[0]
        most = length // BLOCK
        plans = sorted({p for p in PLANS if max(p) < most}, key=lambda p: (link_load(p), sum(p), p)) + [(most,) * chips]
        lanes = 128
        tile = 128
        part, code, column, which = pl.pallas_call(
            functools.partial(gather_kernel, chips, w_head.shape[0], plans),
            out_shape=(pltpu.VMEM((length, depth), BF16),
                       pltpu.VMEM((1, length), I32),
                       pltpu.VMEM((rows_dev, 1), F32),
                       pltpu.SMEM((1,), I32)),
            in_specs=[pl.BlockSpec(memory_space=pltpu.HBM)] * 4,
            out_specs=(vmem, vmem, vmem, pl.BlockSpec(memory_space=pltpu.SMEM)),
            scratch_shapes=[
                pltpu.VMEM((length // lanes, lanes), I32),
                pltpu.VMEM((length // lanes, lanes), I32),
                pltpu.VMEM((rows_dev // tile, tile), I32),
                pltpu.VMEM((1, length), I32),
                pltpu.VMEM((length, 8), BF16),
                pltpu.VMEM((length // lanes, lanes), I32),
                pltpu.SMEM((length // lanes, lanes), I32),
                pltpu.VMEM((length, 8), F32),
                pltpu.VMEM((RING, GROUP, 8, depth), BF16),
                pltpu.SemaphoreType.DMA((3,)),
                pltpu.SemaphoreType.DMA((length // lanes,)),
                pltpu.SemaphoreType.DMA((RING,)),
            ],
            compiler_params=pltpu.CompilerParams(vmem_limit_bytes=28 * MIB),
            name="gather_rows",
        )(*(pltpu.with_memory_space_constraint(v, pltpu.HBM) for v in (allowed_ids.reshape(-1, lanes), allowed_valid.reshape(-1, lanes))), w_head.reshape(-1, 8, depth),
          pltpu.with_memory_space_constraint(target_pos.reshape(-1, tile), pltpu.HBM))

        finish = pl.pallas_call(
            finish_kernel,
            out_shape=(jax.ShapeDtypeStruct((rows_dev, length), F32),
                       jax.ShapeDtypeStruct((rows_dev // tile, tile), F32)),
            in_specs=[vmem, vmem],
            out_specs=(hbm, vmem),
            scratch_shapes=[pltpu.VMEM((rows_dev, length), F32), pltpu.VMEM((rows_dev, 1), F32), pltpu.SemaphoreType.DMA],
            compiler_params=pltpu.CompilerParams(vmem_limit_bytes=16 * MIB),
            name="finish",
        )

        def serve(ms, cid):
            total, steps = sum(ms), -(-sum(ms) // WINDOW)
            dma = lambda n: pltpu.SemaphoreType.DMA((n,))
            exchange = pl.pallas_call(
                functools.partial(exchange_kernel, ms, length),
                out_shape=pltpu.VMEM((rows_dev, length), F32),
                in_specs=[vmem, vmem, vmem],
                out_specs=vmem,
                scratch_shapes=[
                    pltpu.VMEM((max(ms) * HALF, depth), BF16),
                    pltpu.VMEM((steps * WINDOW * BLOCK, depth), BF16),
                    pltpu.VMEM((rows_dev, 3 * WINDOW * BLOCK), BF16),
                    dma(5), dma(max(ms)), dma(total - min(ms)), dma(steps),
                ],
                compiler_params=pltpu.CompilerParams(collective_id=cid, has_side_effects=True,
                                                     vmem_limit_bytes=(8 + total // 5 + max(ms) // 10) * MIB),
                name="exchange_" + "_".join(map(str, ms)),
            )
            return lambda hidden, part, code, target: finish(exchange(hidden, part, code), target)

        probs, logp = lax.switch(which[0], [serve(ms, k) for k, ms in enumerate(plans)],
                                 hidden, part, code, column)
        return probs, logp.reshape(rows_dev)

    row_spec = P(("rep", "vocab"))
    mat_spec = P(("rep", "vocab"), None)
    return jax.shard_map(device_step, mesh=mesh, in_specs=(mat_spec, P("vocab", None), P("rep"), P("rep"), row_spec),
                         out_specs=(mat_spec, row_spec), check_vma=False)


PLANS = [(k,) * 4 for k in (6, 8, 9, 10, 11, 12, 14, 16)]
for heavy, others in ((14, 8), (12, 7), (10, 6)):
    PLANS += [tuple(heavy if c == h else others for c in range(4)) for h in range(4)]
```
